32 devices in a mesh: sample: 2 (over x), sy: 4 (over y, core), sz: 4 (over z).
Axes of the slice: x: 2, y: 2, z: 4, core: 2. Of those that a mesh axis runs over, the one named last changes fastest.
Arguments:
- volume: bfloat16 [2, 32, 16, 32, 128], P('sample', None, 'sz', 'sy'), may hold values from -22.5 to 22.5
- amax_history: float32 [4, 16], replicated, may hold values from 0.48 to 2.5
- conv_first: bfloat16 [27, 32, 32], replicated, may hold values from -0.21875 to 0.21875
- conv_second: bfloat16 [27, 32, 32], replicated, may hold values from -0.21875 to 0.21875
- conv_third: bfloat16 [27, 64, 32], P(None, 'sy'), may hold values from -0.21875 to 0.21875
- conv_fourth: bfloat16 [27, 64, 64], P(None, 'sy'), may hold values from -0.15625 to 0.15625
- gain_fine: float32 [2, 32], replicated, may hold values from 0.5 to 1.5
- shift_fine: float32 [2, 32], replicated, may hold values from -0.5 to 0.5
- gain_coarse: float32 [2, 64], P(None, 'sy'), may hold values from 0.5 to 1.5
- shift_coarse: float32 [2, 64], P(None, 'sy'), may hold values from -0.5 to 0.5
Outputs:
- skip_features: bfloat16 [2, 32, 16, 32, 128], P('sample', None, 'sz', 'sy')
- coarse_features: bfloat16 [2, 64, 8, 1024], P('sample', 'sy', 'sz')
- amax_now: float32 [4], replicated
The draws below stay inside these ranges and needn't reach their ends.
All inputs are finite; a program needn't handle non-finite values.
Results may differ from the reference program's by a relative error of at most 0.012.
Values may be sent and summed in bfloat16 or wider, within the bound.
No kernel may reach another device: no remote copies, remote signals or barrier semaphores. Data moves between devices by JAX's collectives and lax.ppermute only.
A program may use at most 128 MiB of HBM per device.

```python
import jax
import jax.numpy as jnp
from jax import lax

C1 = 32
C2 = 64
NX = 128
HIST = 16
LAYERS = 4
SAMPLES = 2
NY = 32
NZ = 16


def draw_volume(key, part):
    shape_all = (SAMPLES, C1, NZ, NY, NX)
    sample_pos = lax.broadcasted_iota(jnp.float32, shape_all, 0) / max(SAMPLES - 1, 1)
    z_pos = lax.broadcasted_iota(jnp.float32, shape_all, 2) / NZ
    y_pos = lax.broadcasted_iota(jnp.float32, shape_all, 3) / NY
    scaling = (0.6 + 1.2 * sample_pos) * (0.5 + z_pos + y_pos)
    noise_part = jnp.clip(jax.random.normal(key, shape_all, jnp.float32), -5.0, 5.0)
    return (noise_part * scaling).astype(jnp.bfloat16)


def draw_amax_history(key, part):
    level_key = jax.random.fold_in(key, 11)
    entry_key = jax.random.fold_in(key, 12)
    level_log = jax.random.uniform(level_key, (LAYERS, 1), jnp.float32, jnp.log(0.8), jnp.log(2.5))
    entries = jax.random.uniform(entry_key, (LAYERS, HIST), jnp.float32, 0.6, 1.0)
    return jnp.exp(level_log) * entries


def level_of(stream_key, dims, cuts, least, largest):
    def one(position, shards_of):
        steps = jax.random.uniform(jax.random.fold_in(jax.random.fold_in(stream_key, 6), position), (shards_of,), jnp.float32, least / len(cuts), largest / len(cuts))
        return jnp.repeat(jnp.exp(steps), dims[position] // shards_of).reshape((-1,) + (1,) * (len(dims) - position - 1))

    factor_of = one(*cuts[0])
    for cut in cuts[1:]:
        factor_of = factor_of * one(*cut)
    return factor_of


def gaussian(own_key, shape, scale, most, cuts=(), held_as=jnp.bfloat16):
    values = scale * jax.random.normal(own_key, shape, jnp.float32)
    if cuts:
        values = values * level_of(own_key, shape, cuts, -0.22, 0.18)
    return jnp.clip(values, -most, most).astype(held_as)


def setup_inputs(seed: int = 0) -> dict:
    seeds = jax.random.split(jax.random.key(seed), 11)
    volume = draw_volume(jax.random.fold_in(seeds[10], 71), 0)
    amax_history = draw_amax_history(jax.random.fold_in(seeds[10], 71), 0)
    conv_first = gaussian(seeds[2], (27, C1, C1), (27 * C1) ** -0.5, 0.21875)
    conv_second = gaussian(seeds[3], (27, C1, C1), (27 * C1) ** -0.5, 0.21875)
    conv_third = gaussian(seeds[4], (27, C2, C1), (27 * C1) ** -0.5, 0.21875, ((1, 4),))
    conv_fourth = gaussian(seeds[5], (27, C2, C2), (27 * C2) ** -0.5, 0.15625, ((1, 4),))
    gain_fine = jnp.clip(1.0 + 0.1 * jax.random.normal(seeds[6], (2, C1), jnp.float32), 0.5, 1.5)
    shift_fine = jnp.clip(jax.random.uniform(seeds[7], (2, C1), jnp.float32, -0.5, 0.5), -0.5, 0.5)
    gain_coarse = jnp.clip(1.0 + 0.1 * jax.random.normal(seeds[8], (2, C2), jnp.float32), 0.5, 1.5)
    shift_coarse = jnp.clip(jax.random.uniform(seeds[9], (2, C2), jnp.float32, -0.5, 0.5) * level_of(seeds[9], (2, C2), ((1, 4),), -0.4, 0.0), -0.5, 0.5)
    return {"volume": volume, "amax_history": amax_history, "conv_first": conv_first, "conv_second": conv_second, "conv_third": conv_third, "conv_fourth": conv_fourth, "gain_fine": gain_fine, "shift_fine": shift_fine, "gain_coarse": gain_coarse, "shift_coarse": shift_coarse}


norm_eps = 1e-05
leak_slope = 0.01

def convolve(values, weight):
    out_chan = weight.shape[1]
    in_chan = weight.shape[2]
    kernel = jnp.transpose(weight.reshape(3, 3, 3, out_chan, in_chan), (3, 4, 0, 1, 2))
    result = lax.conv_general_dilated(values.astype(jnp.float32)[None], kernel.astype(jnp.float32), (1, 1, 1), 'SAME', dimension_numbers=('NCDHW', 'OIDHW', 'NCDHW'), precision=lax.Precision.HIGHEST)
    return result[0]

def activate(values, gains, offset):
    cell_count = values[0].size
    flat_rows = values.reshape(values.shape[0], -1)
    chan_mean = lax.optimization_barrier(jnp.sum(flat_rows, axis=1)) / cell_count
    spread = lax.optimization_barrier(jnp.sum(flat_rows * flat_rows, axis=1)) / cell_count - chan_mean * chan_mean
    scaling = lax.rsqrt(spread + norm_eps) * gains
    normed = (values - chan_mean[:, None, None, None]) * scaling[:, None, None, None] + offset[:, None, None, None]
    return jnp.where(normed >= 0, normed, leak_slope * normed).astype(jnp.bfloat16)

def limited(values, bound):
    return jnp.clip(values.astype(jnp.float32), -bound, bound).astype(jnp.bfloat16)

def pool_max(values):
    chans, depth_cells, height_cells, width_cells = values.shape
    blocks = values.reshape(chans, depth_cells // 2, 2, height_cells // 2, 2, width_cells // 2, 2)
    return lax.optimization_barrier(jnp.max(blocks, axis=(2, 4, 6)))

def reference(volume, amax_history, conv_first, conv_second, conv_third, conv_fourth, gain_fine, shift_fine, gain_coarse, shift_coarse):
    bounds = lax.optimization_barrier(jnp.max(amax_history, axis=1))

    def single(volume_one):
        first = activate(convolve(limited(volume_one, bounds[0]), conv_first), gain_fine[0], shift_fine[0])
        skip_out = activate(convolve(limited(first, bounds[1]), conv_second), gain_fine[1], shift_fine[1])
        pooled = pool_max(skip_out)
        coarse = activate(convolve(limited(pooled, bounds[2]), conv_third), gain_coarse[0], shift_coarse[0])
        coarse_out = activate(convolve(limited(coarse, bounds[3]), conv_fourth), gain_coarse[1], shift_coarse[1])
        peak_list = jnp.stack([jnp.max(jnp.abs(member.astype(jnp.float32))) for member in (volume_one, first, pooled, coarse)])
        return (skip_out, coarse_out.reshape(coarse_out.shape[0], coarse_out.shape[1], -1), peak_list)
    skip_all, coarse_all, peak_all = lax.map(single, volume)
    return (skip_all, coarse_all, lax.optimization_barrier(jnp.max(peak_all, axis=0)))
```

```python
import jax
import jax.numpy as jnp
from jax import lax
from jax.experimental import pallas as pl
from jax.experimental.pallas import tpu as pltpu
from jax.sharding import PartitionSpec as P

norm_eps = 1e-05
leak_slope = 0.01
f32 = jnp.float32
bf16 = jnp.bfloat16
LANES = 128
HALO = 2
PEAK_AT = 64
GAIN_AT = 80
SHIFT_AT = 96


def near(axis):
    count = lax.axis_size(axis)
    first = [(i, i ^ 1) for i in range(count)]
    second = [(i, min(max(((i + 1) ^ 1) - 1, 0), count - 1)) for i in range(count)]
    return first, second


def column(row, channels, start):
    lanes = lax.broadcasted_iota(jnp.int32, (channels, row.shape[1]), 1)
    chans = lax.broadcasted_iota(jnp.int32, (channels, row.shape[1]), 0)
    return jnp.sum(jnp.where(lanes == chans + start, row, 0.0), axis=1, keepdims=True)


def as_row(col, start):
    channels = col.shape[0]
    lanes = lax.broadcasted_iota(jnp.int32, (channels, LANES), 1)
    chans = lax.broadcasted_iota(jnp.int32, (channels, LANES), 0)
    return jnp.sum(jnp.where(lanes == chans + start, col, 0.0), axis=0, keepdims=True)


def at_lane(value, lane):
    lanes = lax.broadcasted_iota(jnp.int32, (1, LANES), 1)
    return jnp.where(lanes == lane, value, 0.0)


def affine(total, square, cells, gains, offset):
    mean = total / cells
    spread = square / cells - mean * mean
    scale = lax.rsqrt(spread + norm_eps) * gains
    return scale, offset - mean * scale


def activated(values, scale, offset):
    normed = values * scale + offset
    return jnp.where(normed >= 0, normed, leak_slope * normed).astype(bf16)


def peak_of(values):
    return jnp.max(jnp.max(values, axis=1, keepdims=True), axis=0, keepdims=True)


def bounded(values, bound):
    return jnp.minimum(jnp.maximum(values.astype(f32), -bound), bound).astype(bf16)


def bound_of(hist_ref, level):
    return jnp.max(hist_ref[level : level + 1, :], axis=1, keepdims=True)


def tap_sum(left, middle, right, period):
    lane = lax.broadcasted_iota(jnp.int32, middle.shape, 1) % period
    up = pltpu.roll(left, 1, 1)
    down = pltpu.roll(right, LANES - 1, 1)
    return middle + jnp.where(lane == 0, 0.0, up) + jnp.where(lane == period - 1, 0.0, down)


def prep_kernel(vol_ref, hist_ref, cells_ref, first_ref, second_ref, peak_ref, wide_ref):
    channels, depth, height, width = vol_ref.shape[1:]
    rows = depth * height
    wide = vol_ref[0].astype(f32).reshape(channels * rows, width)
    wide_ref[...] = wide
    peak_ref[...] = jnp.broadcast_to(peak_of(jnp.abs(wide)), (1, LANES))
    bound = bound_of(hist_ref, 0)
    for r in range(rows):
        cells_ref[r // height, r % height] = bounded(
            wide_ref[pl.ds(r, channels, stride=rows), :], bound
        )
    even = lax.axis_index("sz") % 2 == 0
    start_first = jnp.where(even, depth - HALO, 0)
    start_second = jnp.where(even, 0, depth - HALO)
    first_ref[...] = cells_ref[pl.ds(start_first, HALO)]
    second_ref[...] = cells_ref[pl.ds(start_second, HALO)]


def sides(axis, first, second):
    at = lax.axis_index(axis)
    count = lax.axis_size(axis)
    even = at % 2 == 0
    blank = jnp.zeros_like(first)
    below = jnp.where(at == 0, blank, jnp.where(even, second, first))
    above = jnp.where(at == count - 1, blank, jnp.where(even, first, second))
    return below, above


def deep_kernel(cells_ref, got_first_ref, got_second_ref, deep_ref, first_ref, second_ref):
    depth, height = cells_ref.shape[:2]
    below, above = sides("sz", got_first_ref[...], got_second_ref[...])
    deep_ref[0:HALO] = below
    deep_ref[HALO : HALO + depth] = cells_ref[...]
    deep_ref[HALO + depth :] = above
    even = lax.axis_index("sy") % 2 == 0
    start_first = jnp.where(even, height - HALO, 0)
    start_second = jnp.where(even, 0, height - HALO)
    first_ref[...] = deep_ref[:, pl.ds(start_first, HALO)]
    second_ref[...] = deep_ref[:, pl.ds(start_second, HALO)]


def conv_rows(cells_ref, weight, z, y, out_chan):
    window = jnp.concatenate(
        [
            jnp.concatenate(
                [cells_ref[z + dz, y + dy], cells_ref[z + dz, y + 1 + dy]], axis=1
            )
            for dz in range(3)
            for dy in range(3)
        ],
        axis=0,
    )
    taps = jnp.dot(weight, window, preferred_element_type=f32)
    outs = []
    for half in range(2):
        part = taps[:, half * LANES : (half + 1) * LANES]
        outs.append(
            tap_sum(
                part[:out_chan], part[out_chan : 2 * out_chan], part[2 * out_chan :], LANES
            )
        )
    return outs


def first_kernel(
    deep_ref, got_first_ref, got_second_ref, weight_ref, peak_ref, raw_ref, row_ref, cells_ref
):
    depth, height = raw_ref.shape[:2]
    channels = raw_ref.shape[2]
    inner = deep_ref.shape[1]
    below, above = sides("sy", got_first_ref[...], got_second_ref[...])
    cells_ref[:, 0:HALO] = below
    cells_ref[:, HALO : HALO + inner] = deep_ref[...]
    cells_ref[:, HALO + inner :] = above
    weight = weight_ref[...]

    def plane(z, sums):
        total, square = sums
        own = jnp.where((z >= 1) & (z < depth - 1), 1.0, 0.0).astype(f32)
        for y in range(0, height, 2):
            outs = conv_rows(cells_ref, weight, z, y, channels)
            for half in range(2):
                raw_ref[z, y + half] = outs[half]
                if 1 <= y + half < height - 1:
                    mine = outs[half] * own
                    total = total + mine
                    square = square + mine * mine
        return total, square

    blank = jnp.zeros((channels, LANES), f32)
    total, square = lax.fori_loop(0, depth, plane, (blank, blank))
    row = as_row(jnp.sum(total, axis=1, keepdims=True), 0)
    row = row + as_row(jnp.sum(square, axis=1, keepdims=True), channels)
    row = row + at_lane(peak_ref[...], PEAK_AT)
    row_ref[...] = jnp.broadcast_to(row[None], row_ref.shape)


def second_kernel(cell_count):
    def kernel(
        raw_ref,
        rows_ref,
        weight_ref,
        hist_ref,
        gain_ref,
        shift_ref,
        gain_coarse_ref,
        shift_coarse_ref,
        out_ref,
        load_ref,
        hidden_ref,
        pool_ref,
    ):
        wide_depth, wide_height, channels, width = raw_ref.shape
        depth, height = out_ref.shape[:2]
        rows = rows_ref[...]
        merged = jnp.sum(rows, axis=0)
        peak_vol = jnp.max(rows, axis=0)
        scale, offset = affine(
            column(merged, channels, 0),
            column(merged, channels, channels),
            cell_count,
            column(gain_ref[0:1, :], channels, 0),
            column(shift_ref[0:1, :], channels, 0),
        )
        bound = bound_of(hist_ref, 1)
        at_z = lax.axis_index("sz")
        at_y = lax.axis_index("sy")
        last_z = lax.axis_size("sz") - 1
        last_y = lax.axis_size("sy") - 1

        def plane(z, peak):
            inside_z = ((z > 0) | (at_z > 0)) & ((z < wide_depth - 1) | (at_z < last_z))
            own = jnp.where((z >= 1) & (z < wide_depth - 1), 1.0, 0.0).astype(f32)
            for y in range(wide_height):
                inside = inside_z
                if y == 0:
                    inside = inside & (at_y > 0)
                if y == wide_height - 1:
                    inside = inside & (at_y < last_y)
                hidden = activated(raw_ref[z, y], scale, offset).astype(f32)
                if 1 <= y < wide_height - 1:
                    peak = jnp.maximum(peak, jnp.abs(hidden) * own)
                clipped = jnp.minimum(jnp.maximum(hidden, -bound), bound)
                hidden_ref[z, y] = jnp.where(inside, clipped, 0.0).astype(bf16)
            return peak

        blank = jnp.zeros((channels, width), f32)
        peak = lax.fori_loop(0, wide_depth, plane, blank)
        weight = weight_ref[...]
        sign = jnp.where(column(gain_ref[1:2, :], channels, 0) >= 0, 1.0, -1.0).astype(f32)
        half_height = height // 2

        def pair(zp, sums):
            total, square = sums
            for yp in range(half_height):
                best = None
                for dz in range(2):
                    outs = conv_rows(hidden_ref, weight, 2 * zp + dz, 2 * yp, channels)
                    for half in range(2):
                        out_ref[2 * zp + dz, 2 * yp + half] = outs[half]
                        total = total + outs[half]
                        square = square + outs[half] * outs[half]
                        signed = outs[half] * sign
                        best = signed if best is None else jnp.maximum(best, signed)
                best = jnp.maximum(best, pltpu.roll(best, LANES - 1, 1)) * sign
                pool_ref[zp, yp] = best.astype(bf16)
            return total, square

        total, square = lax.fori_loop(0, depth // 2, pair, (blank, blank))
        pick = jnp.where(
            lax.broadcasted_iota(jnp.int32, (2 * LANES, LANES), 0)
            == 2 * lax.broadcasted_iota(jnp.int32, (2 * LANES, LANES), 1),
            1.0,
            0.0,
        ).astype(bf16)
        for zp in range(depth // 2):
            for yq in range(half_height // 2):
                both = jnp.concatenate([pool_ref[zp, 2 * yq], pool_ref[zp, 2 * yq + 1]], axis=1)
                load_ref[
                    zp * channels : (zp + 1) * channels, yq * LANES : (yq + 1) * LANES
                ] = jnp.dot(both, pick, preferred_element_type=f32).astype(bf16)
        mine = gain_coarse_ref.shape[1]
        row = as_row(jnp.sum(total, axis=1, keepdims=True), 0)
        row = row + as_row(jnp.sum(square, axis=1, keepdims=True), channels)
        row = row + at_lane(peak_vol, PEAK_AT)
        row = row + at_lane(peak_of(peak), PEAK_AT + 1)
        row = row + as_row(column(gain_coarse_ref[0:1, :], mine, 0), GAIN_AT)
        row = row + as_row(column(shift_coarse_ref[0:1, :], mine, 0), SHIFT_AT)
        high = row.astype(bf16).astype(f32)
        middle = (row - high).astype(bf16).astype(f32)
        low = row - high - middle
        level = lax.broadcasted_iota(jnp.int32, (16, LANES), 0)
        parts = jnp.where(
            level == 0, high, jnp.where(level == 1, middle, jnp.where(level == 2, low, 0.0))
        )
        body = (depth // 2) * channels
        load_ref[body:, 0:LANES] = parts.astype(bf16)
        load_ref[body:, LANES:] = jnp.zeros((16, load_ref.shape[1] - LANES), bf16)

    return kernel


def spread_rows(cells, store):
    count = cells.shape[1] // LANES
    parts = [cells[:, j * LANES : (j + 1) * LANES] for j in range(count)]
    turned = [pltpu.roll(part, LANES // 2, 1) for part in parts]
    lower = lax.broadcasted_iota(jnp.int32, parts[0].shape, 1) < LANES // 2
    blank = jnp.zeros_like(parts[0])
    for j in range(count):
        before = turned[j - 1] if j > 0 else blank
        after = turned[j + 1] if j + 1 < count else blank
        store(0, j, jnp.where(lower, before, turned[j]))
        store(1, j, parts[j])
        store(2, j, jnp.where(lower, turned[j], after))


def coarse_kernel(fine_cells, coarse_cells, load_rows, piece):
    def kernel(
        all_ref,
        hist_ref,
        gain_ref,
        shift_ref,
        gain_coarse_ref,
        shift_coarse_ref,
        weight_ref,
        out_ref,
        peak_ref,
        affine_ref,
        cells_ref,
        raw_ref,
        hidden_ref,
        last_ref,
    ):
        y_groups = all_ref.shape[0]
        z_groups = lax.axis_size("sz")
        span = all_ref.shape[2]
        planes = raw_ref.shape[0]
        channels = gain_ref.shape[1]
        chan_own = gain_coarse_ref.shape[1]
        chan_all = raw_ref.shape[1]
        flat = raw_ref.shape[2]
        row_len = LANES // 2
        body = load_rows - 16
        z_own = body // channels
        at_z = lax.axis_index("sz")
        totals = jnp.zeros((16, LANES), f32)
        tops = jnp.zeros((1, LANES), f32)
        gain_rows = []
        for s in range(y_groups):
            for k in range(z_groups):
                parts = all_ref[s, k * load_rows + body : (k + 1) * load_rows, 0:LANES].astype(f32)
                one = jnp.sum(parts, axis=0, keepdims=True)
                totals = totals + parts
                tops = jnp.maximum(tops, one)
                if k == 0:
                    gain_rows.append(one)
        merged = jnp.sum(totals, axis=0, keepdims=True)
        scale, offset = affine(
            column(merged, channels, 0),
            column(merged, channels, channels),
            fine_cells,
            column(gain_ref[1:2, :], channels, 0),
            column(shift_ref[1:2, :], channels, 0),
        )
        lanes = lax.broadcasted_iota(jnp.int32, (channels, LANES), 1)
        affine_ref[...] = jnp.where(lanes == 0, scale, jnp.where(lanes == 1, offset, 0.0))
        bound = bound_of(hist_ref, 2)
        peak_pool = jnp.zeros((channels, span), f32)
        for s in range(y_groups):
            for k in range(z_groups):
                for zp in range(z_own):
                    at = k * load_rows + zp * channels
                    value = activated(all_ref[s, at : at + channels, :].astype(f32), scale, offset)
                    value = value.astype(f32)
                    peak_pool = jnp.maximum(peak_pool, jnp.abs(value))
                    clipped = jnp.minimum(jnp.maximum(value, -bound), bound)
                    raw_ref[(at_z ^ k) * z_own + zp, 0:channels, s * span : (s + 1) * span] = clipped
        cells_ref[0] = jnp.zeros(cells_ref.shape[1:], bf16)
        cells_ref[planes + 1] = jnp.zeros(cells_ref.shape[1:], bf16)

        def spread_pool(z, carry):
            def store(dy, j, value):
                cells_ref[
                    z + 1, dy * channels : (dy + 1) * channels, j * LANES : (j + 1) * LANES
                ] = value.astype(bf16)

            spread_rows(raw_ref[z, 0:channels, :], store)
            return carry

        lax.fori_loop(0, planes, spread_pool, 0)
        near_weight = jnp.concatenate(
            [
                all_ref[s, z_groups * load_rows : z_groups * load_rows + piece, :]
                for s in range(y_groups)
            ],
            axis=0,
        )
        far_weight = jnp.concatenate(
            [
                all_ref[s, z_groups * load_rows + piece :, 0 : 9 * channels - span]
                for s in range(y_groups)
            ],
            axis=0,
        )

        def third(z, sums):
            totals, squares = list(sums[0]), list(sums[1])
            for t in range(flat // span):
                window = jnp.concatenate(
                    [cells_ref[z + dz, :, t * span : (t + 1) * span] for dz in range(3)], axis=0
                )
                taps = jnp.dot(near_weight, window[:span], preferred_element_type=f32)
                taps = taps + jnp.dot(far_weight, window[span:], preferred_element_type=f32)
                for s in range(y_groups):
                    for half in range(span // LANES):
                        at = s * piece
                        part = taps[at : at + piece, half * LANES : (half + 1) * LANES]
                        out = tap_sum(
                            part[:chan_own],
                            part[chan_own : 2 * chan_own],
                            part[2 * chan_own :],
                            row_len,
                        )
                        start = t * span + half * LANES
                        raw_ref[
                            z, s * chan_own : (s + 1) * chan_own, start : start + LANES
                        ] = out
                        totals[s] = totals[s] + out
                        squares[s] = squares[s] + out * out
            return tuple(totals), tuple(squares)

        blank = jnp.zeros((chan_own, LANES), f32)
        zero = tuple(blank for _ in range(y_groups))
        totals, squares = lax.fori_loop(0, planes, third, (zero, zero))
        pairs = [
            affine(
                jnp.sum(totals[s], axis=1, keepdims=True),
                jnp.sum(squares[s], axis=1, keepdims=True),
                coarse_cells,
                column(gain_rows[s], chan_own, GAIN_AT),
                column(gain_rows[s], chan_own, SHIFT_AT),
            )
            for s in range(y_groups)
        ]
        scale = jnp.concatenate([one[0] for one in pairs], axis=0)
        offset = jnp.concatenate([one[1] for one in pairs], axis=0)
        bound = bound_of(hist_ref, 3)
        hidden_ref[0] = jnp.zeros(hidden_ref.shape[1:], bf16)
        hidden_ref[planes + 1] = jnp.zeros(hidden_ref.shape[1:], bf16)

        def spread_hidden(z, peak):
            value = activated(raw_ref[z], scale, offset).astype(f32)
            for j in range(flat // LANES):
                peak = jnp.maximum(peak, jnp.abs(value[:, j * LANES : (j + 1) * LANES]))
            clipped = jnp.minimum(jnp.maximum(value, -bound), bound)

            def store(dy, j, part):
                hidden_ref[
                    z + 1, dy * chan_all : (dy + 1) * chan_all, j * LANES : (j + 1) * LANES
                ] = part.astype(bf16)

            spread_rows(clipped, store)
            return peak

        peak_coarse = lax.fori_loop(
            0, planes, spread_hidden, jnp.zeros((chan_all, LANES), f32)
        )
        weight = weight_ref[...]

        def fourth(z, sums):
            total, square = sums
            for t in range(flat // span):
                window = jnp.concatenate(
                    [hidden_ref[z + dz, :, t * span : (t + 1) * span] for dz in range(3)], axis=0
                )
                taps = jnp.dot(weight, window, preferred_element_type=f32)
                for half in range(span // LANES):
                    part = taps[:, half * LANES : (half + 1) * LANES]
                    out = tap_sum(
                        part[:chan_own],
                        part[chan_own : 2 * chan_own],
                        part[2 * chan_own :],
                        row_len,
                    )
                    start = t * span + half * LANES
                    last_ref[z, :, start : start + LANES] = out
                    total = total + out
                    square = square + out * out
            return total, square

        total, square = lax.fori_loop(0, planes, fourth, (blank, blank))
        scale, offset = affine(
            jnp.sum(total, axis=1, keepdims=True),
            jnp.sum(square, axis=1, keepdims=True),
            coarse_cells,
            column(gain_coarse_ref[1:2, :], chan_own, 0),
            column(shift_coarse_ref[1:2, :], chan_own, 0),
        )
        for i in range(z_own):
            out_ref[i] = activated(last_ref[at_z * z_own + i], scale, offset)
        row = at_lane(jnp.max(tops[:, PEAK_AT : PEAK_AT + 1], axis=1, keepdims=True), 0)
        row = row + at_lane(jnp.max(tops[:, PEAK_AT + 1 : PEAK_AT + 2], axis=1, keepdims=True), 1)
        row = row + at_lane(peak_of(peak_pool), 2)
        row = row + at_lane(peak_of(peak_coarse), 3)
        peak_ref[...] = row

    return kernel


def skip_kernel(raw_ref, affine_ref, out_ref, wide_ref):
    depth, height, channels, width = raw_ref.shape
    rows = depth * height
    scale = affine_ref[:, 0:1]
    offset = affine_ref[:, 1:2]
    for r in range(rows):
        wide_ref[pl.ds(r, channels, stride=rows), :] = activated(
            raw_ref[r // height, r % height], scale, offset
        ).astype(f32)
    out_ref[0] = wide_ref[...].reshape(channels, depth, height, width).astype(bf16)


def tap_matrix(weight):
    taps, out_chan, in_chan = weight.shape
    split = weight.reshape(taps // 3, 3, out_chan, in_chan)
    return jnp.transpose(split, (1, 2, 0, 3)).reshape(3 * out_chan, (taps // 3) * in_chan)


def shape(dims, dtype):
    return jax.ShapeDtypeStruct(dims, dtype)


def per_device(
    volume,
    amax_history,
    conv_first,
    conv_second,
    conv_third,
    conv_fourth,
    gain_fine,
    shift_fine,
    gain_coarse,
    shift_coarse,
):
    channels, depth, height, width = volume.shape[1:]
    z_groups = lax.axis_size("sz")
    y_groups = lax.axis_size("sy")
    samples = lax.axis_size("sample")
    fine_cells = float(depth * z_groups * height * y_groups * width)
    coarse_cells = fine_cells / 8
    chan_own = conv_third.shape[1]
    chan_all = conv_fourth.shape[2]
    span = (height // 2) * (width // 2)
    planes = (depth // 2) * z_groups
    flat = span * y_groups
    group = z_groups * y_groups
    load_rows = (depth // 2) * channels + 16

    cells, first, second, peak = pl.pallas_call(
        prep_kernel,
        out_shape=(
            shape((depth, height, channels, width), bf16),
            shape((HALO, height, channels, width), bf16),
            shape((HALO, height, channels, width), bf16),
            shape((1, LANES), f32),
        ),
        scratch_shapes=[pltpu.VMEM((channels * depth * height, width), f32)],
        name="prep",
    )(volume, amax_history)
    pair_first, pair_second = near("sz")
    first = lax.ppermute(first, "sz", pair_first)
    second = lax.ppermute(second, "sz", pair_second)
    deep_depth = depth + 2 * HALO
    deep, first, second = pl.pallas_call(
        deep_kernel,
        out_shape=(
            shape((deep_depth, height, channels, width), bf16),
            shape((deep_depth, HALO, channels, width), bf16),
            shape((deep_depth, HALO, channels, width), bf16),
        ),
        name="deep",
    )(cells, first, second)
    pair_first, pair_second = near("sy")
    first = lax.ppermute(first, "sy", pair_first)
    second = lax.ppermute(second, "sy", pair_second)
    raw_first, row = pl.pallas_call(
        first_kernel,
        out_shape=(
            shape((depth + 2, height + 2, channels, width), f32),
            shape((group, 1, LANES), f32),
        ),
        scratch_shapes=[pltpu.VMEM((deep_depth, height + 2 * HALO, channels, width), bf16)],
        name="first",
    )(deep, first, second, tap_matrix(conv_first), peak)
    rows = lax.all_to_all(row, ("sy", "sz"), 0, 0, tiled=True)
    raw_second, load = pl.pallas_call(
        second_kernel(fine_cells),
        out_shape=(
            shape((depth, height, channels, width), f32),
            shape((load_rows, span), bf16),
        ),
        scratch_shapes=[
            pltpu.VMEM((depth + 2, height + 2, channels, width), bf16),
            pltpu.VMEM((depth // 2, height // 2, channels, width), bf16),
        ],
        name="second",
    )(
        raw_first,
        rows,
        tap_matrix(conv_second),
        amax_history,
        gain_fine,
        shift_fine,
        gain_coarse,
        shift_coarse,
    )
    loads = [load]
    for k in range(1, z_groups):
        loads.append(lax.ppermute(load, "sz", [(i, i ^ k) for i in range(z_groups)]))
    third = tap_matrix(conv_third)
    piece = third.shape[0]
    loads.append(third[:, :span])
    loads.append(jnp.pad(third[:, span:], ((0, 0), (0, 2 * span - third.shape[1]))))
    gathered = lax.all_gather(jnp.concatenate(loads, axis=0), "sy", axis=0)
    coarse, peaks, fine_affine = pl.pallas_call(
        coarse_kernel(fine_cells, coarse_cells, load_rows, piece),
        out_shape=(
            shape((depth // 2, chan_own, flat), bf16),
            shape((1, LANES), f32),
            shape((channels, LANES), f32),
        ),
        scratch_shapes=[
            pltpu.VMEM((planes + 2, 3 * channels, flat), bf16),
            pltpu.VMEM((planes, chan_all, flat), f32),
            pltpu.VMEM((planes + 2, 3 * chan_all, flat), bf16),
            pltpu.VMEM((planes, chan_own, flat), f32),
        ],
        name="coarse",
    )(
        gathered,
        amax_history,
        gain_fine,
        shift_fine,
        gain_coarse,
        shift_coarse,
        tap_matrix(conv_fourth),
    )
    if samples <= 4:
        others = [
            lax.ppermute(peaks, "sample", [(i, (i + k) % samples) for i in range(samples)])
            for k in range(1, samples)
        ]
        for other in others:
            peaks = jnp.maximum(peaks, other)
    else:
        peaks = lax.pmax(peaks, "sample")
    skip = pl.pallas_call(
        skip_kernel,
        out_shape=shape((1, channels, depth, height, width), bf16),
        scratch_shapes=[pltpu.VMEM((channels * depth * height, width), f32)],
        name="skip",
    )(raw_second, fine_affine)
    levels = amax_history.shape[0]
    return skip, jnp.transpose(coarse, (1, 0, 2))[None], peaks[0, :levels]


def solution(mesh):
    return jax.shard_map(
        per_device,
        mesh=mesh,
        in_specs=(
            P("sample", None, "sz", "sy", None),
            P(),
            P(),
            P(),
            P(None, "sy", None),
            P(None, "sy", None),
            P(),
            P(),
            P(None, "sy"),
            P(None, "sy"),
        ),
        out_specs=(P("sample", None, "sz", "sy", None), P("sample", "sy", "sz", None), P()),
        check_vma=False,
    )
```

```python
import jax
import jax.numpy as jnp
from jax import lax
from jax.experimental import pallas as pl
from jax.experimental.pallas import tpu as pltpu
from jax.sharding import PartitionSpec as P

norm_eps = 1e-05
leak_slope = 0.01
f32 = jnp.float32
bf16 = jnp.bfloat16
LANES = 128
HALO = 2
PEAK_AT = 64
CODE_AT = 66
GAIN_AT = 80
SHIFT_AT = 96
CODE_SPAN = 83.0


def near(axis):
    count = lax.axis_size(axis)
    first = [(i, i ^ 1) for i in range(count)]
    second = [(i, min(max(((i + 1) ^ 1) - 1, 0), count - 1)) for i in range(count)]
    return first, second


def column(row, channels, start):
    lanes = lax.broadcasted_iota(jnp.int32, (channels, row.shape[1]), 1)
    chans = lax.broadcasted_iota(jnp.int32, (channels, row.shape[1]), 0)
    return jnp.sum(jnp.where(lanes == chans + start, row, 0.0), axis=1, keepdims=True)


def as_row(col, start):
    channels = col.shape[0]
    lanes = lax.broadcasted_iota(jnp.int32, (channels, LANES), 1)
    chans = lax.broadcasted_iota(jnp.int32, (channels, LANES), 0)
    return jnp.sum(jnp.where(lanes == chans + start, col, 0.0), axis=0, keepdims=True)


def at_lane(value, lane):
    lanes = lax.broadcasted_iota(jnp.int32, (1, LANES), 1)
    return jnp.where(lanes == lane, value, 0.0)


def affine(total, square, cells, gains, offset):
    mean = total / cells
    spread = square / cells - mean * mean
    scale = lax.rsqrt(spread + norm_eps) * gains
    return scale, offset - mean * scale


def activated(values, scale, offset):
    normed = values * scale + offset
    return jnp.maximum(normed, leak_slope * normed).astype(bf16)


def peak_of(values):
    values = values.astype(f32)
    return jnp.max(jnp.max(values, axis=1, keepdims=True), axis=0, keepdims=True)


def bounded(values, bound):
    return jnp.minimum(jnp.maximum(values, -bound), bound)


def bound_of(hist_ref, level):
    return jnp.max(hist_ref[level : level + 1, :], axis=1, keepdims=True).astype(bf16)


def matrix_of(weight, taps_ref):
    taps, out_chan, in_chan = weight.shape
    for dx in range(3):
        taps_ref[dx * out_chan : (dx + 1) * out_chan, :] = jnp.concatenate(
            [weight[3 * j + dx] for j in range(taps // 3)], axis=1
        )


def matrix_kernel(
    peak_ref, first_ref, second_ref, third_ref, fourth_ref, m1_ref, m2_ref, m3_ref, m4_ref, wide_ref
):
    matrix_of(first_ref, m1_ref)
    matrix_of(second_ref, m2_ref)
    matrix_of(fourth_ref, m4_ref)
    matrix_of(third_ref, wide_ref)
    rows, span = m3_ref.shape[0] // 2, m3_ref.shape[1]
    rest = wide_ref.shape[1] - span
    m3_ref[:rows, :] = wide_ref[:, :span]
    m3_ref[rows:, :] = jnp.concatenate(
        [wide_ref[:, span:], jnp.zeros((rows, span - rest), bf16)], axis=1
    )


def tap_sum(left, middle, right, period):
    lane = lax.broadcasted_iota(jnp.int32, middle.shape, 1) % period
    up = pltpu.roll(left, 1, 1)
    down = pltpu.roll(right, LANES - 1, 1)
    return middle + jnp.where(lane == 0, 0.0, up) + jnp.where(lane == period - 1, 0.0, down)


def prep_kernel(vol_ref, hist_ref, cells_ref, first_ref, second_ref, peak_ref, wide_ref):
    channels, depth, height, width = vol_ref.shape[1:]
    rows = depth * height
    wide = vol_ref[0].astype(f32).reshape(channels * rows, width)
    wide_ref[...] = wide
    peak_ref[...] = jnp.broadcast_to(peak_of(jnp.abs(wide)), (1, LANES))
    bound = bound_of(hist_ref, 0)
    for r in range(rows):
        cells_ref[r // height, r % height] = bounded(
            wide_ref[pl.ds(r, channels, stride=rows), :].astype(bf16), bound
        )
    even = lax.axis_index("sz") % 2 == 0
    start_first = jnp.where(even, depth - HALO, 0)
    start_second = jnp.where(even, 0, depth - HALO)
    first_ref[...] = cells_ref[pl.ds(start_first, HALO)]
    second_ref[...] = cells_ref[pl.ds(start_second, HALO)]


def sides(axis, first, second):
    at = lax.axis_index(axis)
    count = lax.axis_size(axis)
    even = at % 2 == 0
    blank = jnp.zeros_like(first)
    below = jnp.where(at == 0, blank, jnp.where(even, second, first))
    above = jnp.where(at == count - 1, blank, jnp.where(even, first, second))
    return below, above


def deep_kernel(
    cells_ref, got_first_ref, got_second_ref, matrix_ref, first_ref, second_ref, done
):
    depth, height = cells_ref.shape[:2]
    even = lax.axis_index("sy") % 2 == 0
    starts = (jnp.where(even, height - HALO, 0), jnp.where(even, 0, height - HALO))
    odd_z = lax.axis_index("sz") % 2
    places = (odd_z * 0 + (1 - odd_z) * (HALO + depth), odd_z * (HALO + depth))
    copies = []
    for side, (start, out_ref) in enumerate(zip(starts, (first_ref, second_ref))):
        rows = pl.ds(start, HALO)
        jobs = (
            (got_first_ref.at[:, rows], out_ref.at[pl.ds(places[0], HALO)]),
            (got_second_ref.at[:, rows], out_ref.at[pl.ds(places[1], HALO)]),
            (cells_ref.at[:, rows], out_ref.at[HALO : HALO + depth]),
        )
        for which, (source, target) in enumerate(jobs):
            copies.append(pltpu.make_async_copy(source, target, done.at[3 * side + which]))
    for copy in copies:
        copy.start()
    for copy in copies:
        copy.wait()


def conv_rows(cells_ref, weight, z, y, out_chan):
    window = jnp.concatenate(
        [
            jnp.concatenate(
                [cells_ref[z + dz, y + dy], cells_ref[z + dz, y + 1 + dy]], axis=1
            )
            for dz in range(3)
            for dy in range(3)
        ],
        axis=0,
    )
    taps = jnp.dot(weight, window, preferred_element_type=f32)
    outs = []
    for half in range(2):
        part = taps[:, half * LANES : (half + 1) * LANES]
        outs.append(
            tap_sum(
                part[:out_chan], part[out_chan : 2 * out_chan], part[2 * out_chan :], LANES
            )
        )
    return outs


def first_kernel(
    own_ref,
    z_first_ref,
    z_second_ref,
    y_first_ref,
    y_second_ref,
    weight_ref,
    peak_ref,
    raw_ref,
    row_ref,
    cells_ref,
):
    depth, height = raw_ref.shape[:2]
    channels = raw_ref.shape[2]
    own_depth, own_height = own_ref.shape[:2]
    below, above = sides("sz", z_first_ref[...], z_second_ref[...])
    rows = slice(HALO, HALO + own_height)
    cells_ref[0:HALO, rows] = below
    cells_ref[HALO : HALO + own_depth, rows] = own_ref[...]
    cells_ref[HALO + own_depth :, rows] = above
    below, above = sides("sy", y_first_ref[...], y_second_ref[...])
    cells_ref[:, 0:HALO] = below
    cells_ref[:, HALO + own_height :] = above

    @pl.when(lax.axis_index("sz") == 0)
    def _():
        for edge in (slice(0, HALO), slice(HALO + own_height, 2 * HALO + own_height)):
            cells_ref[0:HALO, edge] = jnp.zeros((HALO, HALO) + own_ref.shape[2:], bf16)

    @pl.when(lax.axis_index("sz") == lax.axis_size("sz") - 1)
    def _():
        for edge in (slice(0, HALO), slice(HALO + own_height, 2 * HALO + own_height)):
            cells_ref[HALO + own_depth :, edge] = jnp.zeros(
                (HALO, HALO) + own_ref.shape[2:], bf16
            )

    weight = weight_ref[...]

    def plane(z, sums):
        total, square = sums
        own = jnp.where((z >= 1) & (z < depth - 1), 1.0, 0.0).astype(f32)
        for y in range(0, height, 2):
            outs = conv_rows(cells_ref, weight, z, y, channels)
            for half in range(2):
                raw_ref[z, y + half] = outs[half]
                if 1 <= y + half < height - 1:
                    mine = outs[half] * own
                    total = total + mine
                    square = square + mine * mine
        return total, square

    blank = jnp.zeros((channels, LANES), f32)
    total, square = lax.fori_loop(0, depth, plane, (blank, blank))
    row = as_row(jnp.sum(total, axis=1, keepdims=True), 0)
    row = row + as_row(jnp.sum(square, axis=1, keepdims=True), channels)
    row = row + at_lane(peak_ref[...], PEAK_AT)
    row_ref[...] = jnp.broadcast_to(row[None], row_ref.shape)


def second_kernel(cell_count):
    def kernel(
        raw_ref,
        rows_ref,
        weight_ref,
        hist_ref,
        gain_ref,
        shift_ref,
        gain_coarse_ref,
        shift_coarse_ref,
        out_ref,
        load_ref,
        hidden_ref,
        pool_ref,
    ):
        wide_depth, wide_height, channels, width = raw_ref.shape
        depth, height = out_ref.shape[:2]
        rows = rows_ref[...]
        merged = jnp.sum(rows, axis=0)
        peak_vol = jnp.max(rows, axis=0)
        scale, offset = affine(
            column(merged, channels, 0),
            column(merged, channels, channels),
            cell_count,
            column(gain_ref[0:1, :], channels, 0),
            column(shift_ref[0:1, :], channels, 0),
        )
        bound = bound_of(hist_ref, 1)
        at_z = lax.axis_index("sz")
        at_y = lax.axis_index("sy")
        last_z = lax.axis_size("sz") - 1
        last_y = lax.axis_size("sy") - 1

        def plane(z, peak):
            inside_z = ((z > 0) | (at_z > 0)) & ((z < wide_depth - 1) | (at_z < last_z))
            own = jnp.where((z >= 1) & (z < wide_depth - 1), 1.0, 0.0).astype(bf16)
            for y in range(wide_height):
                inside = inside_z
                if y == 0:
                    inside = inside & (at_y > 0)
                if y == wide_height - 1:
                    inside = inside & (at_y < last_y)
                hidden = activated(raw_ref[z, y], scale, offset)
                if 1 <= y < wide_height - 1:
                    peak = jnp.maximum(peak, jnp.abs(hidden) * own)
                inside = jnp.where(inside, 1.0, 0.0).astype(bf16)
                hidden_ref[z, y] = bounded(hidden, bound) * inside
            return peak

        blank = jnp.zeros((channels, width), f32)
        peak = lax.fori_loop(0, wide_depth, plane, jnp.zeros((channels, width), bf16))
        weight = weight_ref[...]
        sign = jnp.where(column(gain_ref[1:2, :], channels, 0) >= 0, 1.0, -1.0).astype(f32)
        half_height = height // 2

        def pair(zp, sums):
            total, square, least, most = sums
            for yp in range(half_height):
                best = None
                for dz in range(2):
                    outs = conv_rows(hidden_ref, weight, 2 * zp + dz, 2 * yp, channels)
                    for half in range(2):
                        out_ref[2 * zp + dz, 2 * yp + half] = outs[half]
                        total = total + outs[half]
                        square = square + outs[half] * outs[half]
                        signed = outs[half] * sign
                        best = signed if best is None else jnp.maximum(best, signed)
                best = jnp.maximum(best, pltpu.roll(best, LANES - 1, 1)) * sign
                pool_ref[zp, yp] = best
                least = jnp.minimum(least, best)
                most = jnp.maximum(most, best)
            return total, square, least, most

        total, square, least, most = lax.fori_loop(
            0, depth // 2, pair, (blank, blank, blank + 1e30, blank - 1e30)
        )
        most, least = peak_of(most), -peak_of(-least)
        center = 0.5 * (most + least)
        reach = jnp.maximum(0.5 * (most - least), 1e-30)
        rate = CODE_SPAN / reach
        pick = jnp.where(
            lax.broadcasted_iota(jnp.int32, (2 * LANES, LANES), 0)
            == 2 * lax.broadcasted_iota(jnp.int32, (2 * LANES, LANES), 1),
            1.0,
            0.0,
        ).astype(bf16)
        for zp in range(depth // 2):
            for yq in range(half_height // 2):
                both = jnp.concatenate([pool_ref[zp, 2 * yq], pool_ref[zp, 2 * yq + 1]], axis=1)
                both = jnp.exp((both - center) * rate).astype(bf16)
                load_ref[
                    zp * channels : (zp + 1) * channels, yq * LANES : (yq + 1) * LANES
                ] = jnp.dot(both, pick, preferred_element_type=f32).astype(bf16)
        mine = gain_coarse_ref.shape[1]
        row = as_row(jnp.sum(total, axis=1, keepdims=True), 0)
        row = row + as_row(jnp.sum(square, axis=1, keepdims=True), channels)
        row = row + at_lane(peak_vol, PEAK_AT)
        row = row + at_lane(peak_of(peak), PEAK_AT + 1)
        row = row + at_lane(center, CODE_AT)
        row = row + at_lane(reach / CODE_SPAN, CODE_AT + 1)
        row = row + as_row(column(gain_coarse_ref[0:1, :], mine, 0), GAIN_AT)
        row = row + as_row(column(shift_coarse_ref[0:1, :], mine, 0), SHIFT_AT)
        high = row.astype(bf16).astype(f32)
        middle = (row - high).astype(bf16).astype(f32)
        low = row - high - middle
        level = lax.broadcasted_iota(jnp.int32, (16, LANES), 0)
        parts = jnp.where(
            level == 0, high, jnp.where(level == 1, middle, jnp.where(level == 2, low, 0.0))
        )
        body = (depth // 2) * channels
        load_ref[body:, 0:LANES] = parts.astype(bf16)
        load_ref[body:, LANES:] = jnp.zeros((16, load_ref.shape[1] - LANES), bf16)

    return kernel


def spread_rows(cells, store):
    count = cells.shape[1] // LANES
    parts = [cells[:, j * LANES : (j + 1) * LANES] for j in range(count)]
    turned = [pltpu.roll(part, LANES // 2, 1) for part in parts]
    lower = lax.broadcasted_iota(jnp.int32, parts[0].shape, 1) < LANES // 2
    blank = jnp.zeros_like(parts[0])
    for j in range(count):
        before = turned[j - 1] if j > 0 else blank
        after = turned[j + 1] if j + 1 < count else blank
        store(0, j, jnp.where(lower, before, turned[j]))
        store(1, j, parts[j])
        store(2, j, jnp.where(lower, turned[j], after))


def third_kernel(fine_cells, coarse_cells, load_rows, piece):
    def kernel(
        all_ref,
        hist_ref,
        gain_ref,
        shift_ref,
        out_ref,
        peak_ref,
        affine_ref,
        pool_ref,
        cells_ref,
        raw_ref,
    ):
        y_groups = all_ref.shape[0]
        z_groups = lax.axis_size("sz")
        span = all_ref.shape[2]
        planes, chan_all, flat = raw_ref.shape
        channels = gain_ref.shape[1]
        chan_own = piece // 3
        row_len = LANES // 2
        body = load_rows - 16
        z_own = body // channels
        at_z = lax.axis_index("sz")
        totals = jnp.zeros((16, LANES), f32)
        tops = jnp.zeros((1, LANES), f32)
        rows = {}
        for s in range(y_groups):
            for k in range(z_groups):
                parts = all_ref[s, k * load_rows + body : (k + 1) * load_rows, 0:LANES].astype(f32)
                totals = totals + parts
                rows[s, k] = jnp.sum(parts, axis=0, keepdims=True)
                tops = jnp.maximum(tops, rows[s, k])
        merged = jnp.sum(totals, axis=0, keepdims=True)
        scale, offset = affine(
            column(merged, channels, 0),
            column(merged, channels, channels),
            fine_cells,
            column(gain_ref[1:2, :], channels, 0),
            column(shift_ref[1:2, :], channels, 0),
        )
        lanes = lax.broadcasted_iota(jnp.int32, (channels, LANES), 1)
        affine_ref[...] = jnp.where(lanes == 0, scale, jnp.where(lanes == 1, offset, 0.0))
        bound = bound_of(hist_ref, 2)
        peak_pool = jnp.zeros((channels, span), bf16)
        for s in range(y_groups):
            for k in range(z_groups):
                center = rows[s, k][:, CODE_AT : CODE_AT + 1]
                reach = rows[s, k][:, CODE_AT + 1 : CODE_AT + 2]
                rate = scale * reach
                start = scale * center + offset
                for zp in range(z_own):
                    at = k * load_rows + zp * channels
                    code = jnp.log(all_ref[s, at : at + channels, :].astype(f32))
                    value = activated(code, rate, start)
                    peak_pool = jnp.maximum(peak_pool, jnp.abs(value))
                    pool_ref[(at_z ^ k) * z_own + zp, :, s * span : (s + 1) * span] = bounded(
                        value, bound
                    )
        cells_ref[0] = jnp.zeros(cells_ref.shape[1:], bf16)
        cells_ref[planes + 1] = jnp.zeros(cells_ref.shape[1:], bf16)

        def spread_pool(z, carry):
            def store(dy, j, value):
                cells_ref[
                    z + 1, dy * channels : (dy + 1) * channels, j * LANES : (j + 1) * LANES
                ] = value

            spread_rows(pool_ref[z], store)
            return carry

        lax.fori_loop(0, planes, spread_pool, 0)
        weights = z_groups * load_rows
        near_weight = jnp.concatenate(
            [all_ref[s, weights : weights + piece, :] for s in range(y_groups)], axis=0
        )
        far_weight = jnp.concatenate(
            [all_ref[s, weights + piece :, 0 : 9 * channels - span] for s in range(y_groups)],
            axis=0,
        )

        def third(z, sums):
            totals, squares = list(sums[0]), list(sums[1])
            for t in range(flat // span):
                window = jnp.concatenate(
                    [cells_ref[z + dz, :, t * span : (t + 1) * span] for dz in range(3)], axis=0
                )
                taps = jnp.dot(near_weight, window[:span], preferred_element_type=f32)
                taps = taps + jnp.dot(far_weight, window[span:], preferred_element_type=f32)
                for s in range(y_groups):
                    for half in range(span // LANES):
                        at = s * piece
                        part = taps[at : at + piece, half * LANES : (half + 1) * LANES]
                        out = tap_sum(
                            part[:chan_own],
                            part[chan_own : 2 * chan_own],
                            part[2 * chan_own :],
                            row_len,
                        )
                        start = t * span + half * LANES
                        raw_ref[
                            z, s * chan_own : (s + 1) * chan_own, start : start + LANES
                        ] = out
                        totals[s] = totals[s] + out
                        squares[s] = squares[s] + out * out
            return tuple(totals), tuple(squares)

        blank = jnp.zeros((chan_own, LANES), f32)
        zero = tuple(blank for _ in range(y_groups))
        totals, squares = lax.fori_loop(0, planes, third, (zero, zero))
        pairs = [
            affine(
                jnp.sum(totals[s], axis=1, keepdims=True),
                jnp.sum(squares[s], axis=1, keepdims=True),
                coarse_cells,
                column(rows[s, 0], chan_own, GAIN_AT),
                column(rows[s, 0], chan_own, SHIFT_AT),
            )
            for s in range(y_groups)
        ]
        scale = jnp.concatenate([one[0] for one in pairs], axis=0)
        offset = jnp.concatenate([one[1] for one in pairs], axis=0)
        bound = bound_of(hist_ref, 3)

        def normed(z, peak):
            for j in range(flat // LANES):
                lanes = slice(j * LANES, (j + 1) * LANES)
                value = activated(raw_ref[z, :, lanes], scale, offset)
                peak = jnp.maximum(peak, jnp.abs(value))
                out_ref[z, :, lanes] = bounded(value, bound)
            return peak

        peak_coarse = lax.fori_loop(0, planes, normed, jnp.zeros((chan_all, LANES), bf16))
        row = at_lane(tops[:, PEAK_AT : PEAK_AT + 1], 0)
        row = row + at_lane(tops[:, PEAK_AT + 1 : PEAK_AT + 2], 1)
        row = row + at_lane(peak_of(peak_pool), 2)
        row = row + at_lane(peak_of(peak_coarse), 3)
        peak_ref[...] = row

    return kernel


def fourth_kernel(coarse_cells):
    def kernel(
        cells_ref,
        weight_ref,
        gain_ref,
        shift_ref,
        raw_ref,
        affine_ref,
        out_ref,
        skip_ref,
        hidden_ref,
        last_ref,
        wide_ref,
    ):
        planes, chan_all, flat = cells_ref.shape
        chan_own, z_own = out_ref.shape[1:3]
        span = 2 * LANES
        row_len = LANES // 2
        hidden_ref[0] = jnp.zeros(hidden_ref.shape[1:], bf16)
        hidden_ref[planes + 1] = jnp.zeros(hidden_ref.shape[1:], bf16)

        def spread_hidden(z, carry):
            def store(dy, j, part):
                hidden_ref[
                    z + 1, dy * chan_all : (dy + 1) * chan_all, j * LANES : (j + 1) * LANES
                ] = part

            spread_rows(cells_ref[z], store)
            return carry

        lax.fori_loop(0, planes, spread_hidden, 0)
        weight = weight_ref[...]

        def fourth(z, sums):
            total, square = sums
            for t in range(flat // span):
                window = jnp.concatenate(
                    [hidden_ref[z + dz, :, t * span : (t + 1) * span] for dz in range(3)], axis=0
                )
                taps = jnp.dot(weight, window, preferred_element_type=f32)
                for half in range(span // LANES):
                    part = taps[:, half * LANES : (half + 1) * LANES]
                    out = tap_sum(
                        part[:chan_own],
                        part[chan_own : 2 * chan_own],
                        part[2 * chan_own :],
                        row_len,
                    )
                    start = t * span + half * LANES
                    last_ref[z, :, start : start + LANES] = out
                    total = total + out
                    square = square + out * out
            return total, square

        blank = jnp.zeros((chan_own, LANES), f32)
        total, square = lax.fori_loop(0, planes, fourth, (blank, blank))
        scale, offset = affine(
            jnp.sum(total, axis=1, keepdims=True),
            jnp.sum(square, axis=1, keepdims=True),
            coarse_cells,
            column(gain_ref[1:2, :], chan_own, 0),
            column(shift_ref[1:2, :], chan_own, 0),
        )
        at_z = lax.axis_index("sz")
        own = [
            activated(last_ref[at_z * z_own + i], scale, offset).astype(f32) for i in range(z_own)
        ]
        for c in range(chan_own):
            out_ref[0, c] = jnp.concatenate([one[c : c + 1] for one in own], axis=0).astype(bf16)
        depth, height, channels, width = raw_ref.shape
        rows = depth * height
        scale = affine_ref[:, 0:1]
        offset = affine_ref[:, 1:2]
        for r in range(rows):
            wide_ref[pl.ds(r, channels, stride=rows), :] = activated(
                raw_ref[r // height, r % height], scale, offset
            ).astype(f32)
        skip_ref[0] = wide_ref[...].reshape(channels, depth, height, width).astype(bf16)

    return kernel


def shape(dims, dtype):
    return jax.ShapeDtypeStruct(dims, dtype)


def per_device(
    volume,
    amax_history,
    conv_first,
    conv_second,
    conv_third,
    conv_fourth,
    gain_fine,
    shift_fine,
    gain_coarse,
    shift_coarse,
):
    channels, depth, height, width = volume.shape[1:]
    z_groups = lax.axis_size("sz")
    y_groups = lax.axis_size("sy")
    samples = lax.axis_size("sample")
    fine_cells = float(depth * z_groups * height * y_groups * width)
    coarse_cells = fine_cells / 8
    chan_own = conv_third.shape[1]
    chan_all = conv_fourth.shape[2]
    span = (height // 2) * (width // 2)
    planes = (depth // 2) * z_groups
    flat = span * y_groups
    group = z_groups * y_groups
    load_rows = (depth // 2) * channels + 16

    cells, first, second, peak = pl.pallas_call(
        prep_kernel,
        out_shape=(
            shape((depth, height, channels, width), bf16),
            shape((HALO, height, channels, width), bf16),
            shape((HALO, height, channels, width), bf16),
            shape((1, LANES), f32),
        ),
        scratch_shapes=[pltpu.VMEM((channels * depth * height, width), f32)],
        name="prep",
    )(volume, amax_history)
    third_rows = 3 * chan_own
    m1, m2, m3, m4 = pl.pallas_call(
        matrix_kernel,
        out_shape=(
            shape((3 * channels, 9 * channels), bf16),
            shape((3 * channels, 9 * channels), bf16),
            shape((2 * third_rows, span), bf16),
            shape((third_rows, 9 * chan_all), bf16),
        ),
        scratch_shapes=[pltpu.VMEM((third_rows, 9 * channels), bf16)],
        name="matrices",
    )(peak, conv_first, conv_second, conv_third, conv_fourth)
    pair_first, pair_second = near("sz")
    z_first = lax.ppermute(first, "sz", pair_first)
    z_second = lax.ppermute(second, "sz", pair_second)
    deep_depth = depth + 2 * HALO
    anywhere = pl.BlockSpec(memory_space=pl.ANY)
    first, second = pl.pallas_call(
        deep_kernel,
        in_specs=[anywhere] * 4,
        out_specs=(anywhere, anywhere),
        out_shape=(
            shape((deep_depth, HALO, channels, width), bf16),
            shape((deep_depth, HALO, channels, width), bf16),
        ),
        scratch_shapes=[pltpu.SemaphoreType.DMA((6,))],
        name="deep",
    )(cells, z_first, z_second, m1)
    pair_first, pair_second = near("sy")
    y_first = lax.ppermute(first, "sy", pair_first)
    y_second = lax.ppermute(second, "sy", pair_second)
    raw_first, row = pl.pallas_call(
        first_kernel,
        out_shape=(
            shape((depth + 2, height + 2, channels, width), f32),
            shape((group, 1, LANES), f32),
        ),
        scratch_shapes=[pltpu.VMEM((deep_depth, height + 2 * HALO, channels, width), bf16)],
        name="first",
    )(cells, z_first, z_second, y_first, y_second, m1, peak)
    rows = lax.all_to_all(row, ("sy", "sz"), 0, 0, tiled=True)
    raw_second, load = pl.pallas_call(
        second_kernel(fine_cells),
        out_shape=(
            shape((depth, height, channels, width), f32),
            shape((load_rows, span), bf16),
        ),
        scratch_shapes=[
            pltpu.VMEM((depth + 2, height + 2, channels, width), bf16),
            pltpu.VMEM((depth // 2, height // 2, channels, width), f32),
        ],
        name="second",
    )(raw_first, rows, m2, amax_history, gain_fine, shift_fine, gain_coarse, shift_coarse)
    loads = [load]
    for k in range(1, z_groups):
        loads.append(lax.ppermute(load, "sz", [(i, i ^ k) for i in range(z_groups)]))
    loads.append(m3)
    gathered = lax.all_gather(jnp.concatenate(loads, axis=0), "sy", axis=0)
    hidden, peaks, fine_affine = pl.pallas_call(
        third_kernel(fine_cells, coarse_cells, load_rows, third_rows),
        out_shape=(
            shape((planes, chan_all, flat), bf16),
            shape((1, LANES), f32),
            shape((channels, LANES), f32),
        ),
        scratch_shapes=[
            pltpu.VMEM((planes, channels, flat), bf16),
            pltpu.VMEM((planes + 2, 3 * channels, flat), bf16),
            pltpu.VMEM((planes, chan_all, flat), f32),
        ],
        name="third",
    )(gathered, amax_history, gain_fine, shift_fine)
    if samples <= 4:
        others = [
            lax.ppermute(peaks, "sample", [(i, (i + k) % samples) for i in range(samples)])
            for k in range(1, samples)
        ]
    else:
        others = [lax.pmax(peaks, "sample")]
    coarse, skip = pl.pallas_call(
        fourth_kernel(coarse_cells),
        out_shape=(
            shape((1, chan_own, depth // 2, flat), bf16),
            shape((1, channels, depth, height, width), bf16),
        ),
        scratch_shapes=[
            pltpu.VMEM((planes + 2, 3 * chan_all, flat), bf16),
            pltpu.VMEM((planes, chan_own, flat), f32),
            pltpu.VMEM((channels * depth * height, width), f32),
        ],
        name="fourth",
    )(hidden, m4, gain_coarse, shift_coarse, raw_second, fine_affine)
    for other in others:
        peaks = jnp.maximum(peaks, other)
    levels = amax_history.shape[0]
    return skip, coarse, peaks[0, :levels]


def solution(mesh):
    return jax.shard_map(
        per_device,
        mesh=mesh,
        in_specs=(
            P("sample", None, "sz", "sy", None),
            P(),
            P(),
            P(),
            P(None, "sy", None),
            P(None, "sy", None),
            P(),
            P(),
            P(None, "sy"),
            P(None, "sy"),
        ),
        out_specs=(P("sample", None, "sz", "sy", None), P("sample", "sy", "sz", None), P()),
        check_vma=False,
    )
```

```python
import jax
import jax.numpy as jnp
from jax import lax
from jax.experimental import pallas as pl
from jax.experimental.pallas import tpu as pltpu
from jax.sharding import PartitionSpec as P

norm_eps = 1e-05
leak_slope = 0.01
f32 = jnp.float32
bf16 = jnp.bfloat16
LANES = 128
HALO = 2
PEAK_AT = 64
CODE_AT = 66
GAIN_AT = 80
SHIFT_AT = 96
CODE_SPAN = 83.0


def near(axis):
    count = lax.axis_size(axis)
    first = [(i, i ^ 1) for i in range(count)]
    second = [(i, min(max(((i + 1) ^ 1) - 1, 0), count - 1)) for i in range(count)]
    return first, second


def column(row, channels, start):
    lanes = lax.broadcasted_iota(jnp.int32, (channels, row.shape[1]), 1)
    chans = lax.broadcasted_iota(jnp.int32, (channels, row.shape[1]), 0)
    return jnp.sum(jnp.where(lanes == chans + start, row, 0.0), axis=1, keepdims=True)


def as_row(col, start):
    channels = col.shape[0]
    lanes = lax.broadcasted_iota(jnp.int32, (channels, LANES), 1)
    chans = lax.broadcasted_iota(jnp.int32, (channels, LANES), 0)
    return jnp.sum(jnp.where(lanes == chans + start, col, 0.0), axis=0, keepdims=True)


def at_lane(value, lane):
    lanes = lax.broadcasted_iota(jnp.int32, (1, LANES), 1)
    return jnp.where(lanes == lane, value, 0.0)


def affine(total, square, cells, gains, offset):
    mean = total / cells
    spread = square / cells - mean * mean
    scale = lax.rsqrt(spread + norm_eps) * gains
    return scale, offset - mean * scale


def activated(values, scale, offset):
    normed = values * scale + offset
    return jnp.maximum(normed, leak_slope * normed).astype(bf16)


def peak_of(values):
    values = values.astype(f32)
    return jnp.max(jnp.max(values, axis=1, keepdims=True), axis=0, keepdims=True)


def bounded(values, bound):
    return jnp.minimum(jnp.maximum(values, -bound), bound)


def bound_of(hist_ref, level):
    return jnp.max(hist_ref[level : level + 1, :], axis=1, keepdims=True).astype(bf16)


def matrix_of(weight, taps_ref):
    taps, out_chan, in_chan = weight.shape
    for dx in range(3):
        taps_ref[dx * out_chan : (dx + 1) * out_chan, :] = jnp.concatenate(
            [weight[3 * j + dx] for j in range(taps // 3)], axis=1
        )


def matrix_kernel(
    peak_ref, first_ref, second_ref, third_ref, fourth_ref, m1_ref, m2_ref, m3_ref, m4_ref, wide_ref
):
    matrix_of(first_ref, m1_ref)
    matrix_of(second_ref, m2_ref)
    matrix_of(fourth_ref, m4_ref)
    matrix_of(third_ref, wide_ref)
    rows, span = m3_ref.shape[0] // 2, m3_ref.shape[1]
    rest = wide_ref.shape[1] - span
    m3_ref[:rows, :] = wide_ref[:, :span]
    m3_ref[rows:, :] = jnp.concatenate(
        [wide_ref[:, span:], jnp.zeros((rows, span - rest), bf16)], axis=1
    )


def tap_sum(left, middle, right, period):
    lane = lax.broadcasted_iota(jnp.int32, middle.shape, 1) % period
    up = pltpu.roll(left, 1, 1)
    down = pltpu.roll(right, LANES - 1, 1)
    return middle + jnp.where(lane == 0, 0.0, up) + jnp.where(lane == period - 1, 0.0, down)


def prep_kernel(vol_ref, hist_ref, cells_ref, first_ref, second_ref, peak_ref, wide_ref):
    channels, depth, height, width = vol_ref.shape[1:]
    rows = depth * height
    wide = vol_ref[0].astype(f32).reshape(channels * rows, width)
    wide_ref[...] = wide
    peak_ref[...] = jnp.broadcast_to(peak_of(jnp.abs(wide)), (1, LANES))
    bound = bound_of(hist_ref, 0)
    for r in range(rows):
        cells_ref[r // height, r % height] = bounded(
            wide_ref[pl.ds(r, channels, stride=rows), :].astype(bf16), bound
        )
    even = lax.axis_index("sz") % 2 == 0
    start_first = jnp.where(even, depth - HALO, 0)
    start_second = jnp.where(even, 0, depth - HALO)
    first_ref[...] = cells_ref[pl.ds(start_first, HALO)]
    second_ref[...] = cells_ref[pl.ds(start_second, HALO)]


def sides(axis, first, second):
    at = lax.axis_index(axis)
    count = lax.axis_size(axis)
    even = at % 2 == 0
    blank = jnp.zeros_like(first)
    below = jnp.where(at == 0, blank, jnp.where(even, second, first))
    above = jnp.where(at == count - 1, blank, jnp.where(even, first, second))
    return below, above


def deep_kernel(cells_ref, got_first_ref, got_second_ref, matrix_ref, first_ref, second_ref):
    depth, height = cells_ref.shape[:2]
    even = lax.axis_index("sy") % 2 == 0
    starts = (jnp.where(even, height - HALO, 0), jnp.where(even, 0, height - HALO))
    odd_z = lax.axis_index("sz") % 2
    far = HALO + depth
    for start, out_ref in zip(starts, (first_ref, second_ref)):
        rows = pl.ds(start, HALO)
        out_ref[pl.ds((1 - odd_z) * far, HALO)] = got_first_ref[:, rows]
        out_ref[pl.ds(odd_z * far, HALO)] = got_second_ref[:, rows]
        out_ref[HALO:far] = cells_ref[:, rows]


def conv_rows(cells_ref, weight, z, y, out_chan):
    window = jnp.concatenate(
        [
            jnp.concatenate(
                [cells_ref[z + dz, y + dy], cells_ref[z + dz, y + 1 + dy]], axis=1
            )
            for dz in range(3)
            for dy in range(3)
        ],
        axis=0,
    )
    taps = jnp.dot(weight, window, preferred_element_type=f32)
    outs = []
    for half in range(2):
        part = taps[:, half * LANES : (half + 1) * LANES]
        outs.append(
            tap_sum(
                part[:out_chan], part[out_chan : 2 * out_chan], part[2 * out_chan :], LANES
            )
        )
    return outs


def first_kernel(
    own_ref,
    z_first_ref,
    z_second_ref,
    y_first_ref,
    y_second_ref,
    weight_ref,
    peak_ref,
    raw_ref,
    row_ref,
    cells_ref,
):
    depth, height = raw_ref.shape[:2]
    channels = raw_ref.shape[2]
    own_depth, own_height = own_ref.shape[:2]
    below, above = sides("sz", z_first_ref[...], z_second_ref[...])
    rows = slice(HALO, HALO + own_height)
    cells_ref[0:HALO, rows] = below
    cells_ref[HALO : HALO + own_depth, rows] = own_ref[...]
    cells_ref[HALO + own_depth :, rows] = above
    below, above = sides("sy", y_first_ref[...], y_second_ref[...])
    cells_ref[:, 0:HALO] = below
    cells_ref[:, HALO + own_height :] = above

    @pl.when(lax.axis_index("sz") == 0)
    def _():
        for edge in (slice(0, HALO), slice(HALO + own_height, 2 * HALO + own_height)):
            cells_ref[0:HALO, edge] = jnp.zeros((HALO, HALO) + own_ref.shape[2:], bf16)

    @pl.when(lax.axis_index("sz") == lax.axis_size("sz") - 1)
    def _():
        for edge in (slice(0, HALO), slice(HALO + own_height, 2 * HALO + own_height)):
            cells_ref[HALO + own_depth :, edge] = jnp.zeros(
                (HALO, HALO) + own_ref.shape[2:], bf16
            )

    weight = weight_ref[...]

    def plane(z, sums):
        total, square = sums
        own = jnp.where((z >= 1) & (z < depth - 1), 1.0, 0.0).astype(f32)
        for y in range(0, height, 2):
            outs = conv_rows(cells_ref, weight, z, y, channels)
            for half in range(2):
                raw_ref[z, y + half] = outs[half]
                if 1 <= y + half < height - 1:
                    mine = outs[half] * own
                    total = total + mine
                    square = square + mine * mine
        return total, square

    blank = jnp.zeros((channels, LANES), f32)
    total, square = lax.fori_loop(0, depth, plane, (blank, blank))
    row = as_row(jnp.sum(total, axis=1, keepdims=True), 0)
    row = row + as_row(jnp.sum(square, axis=1, keepdims=True), channels)
    row = row + at_lane(peak_ref[...], PEAK_AT)
    row_ref[...] = jnp.broadcast_to(row[None], row_ref.shape)


def second_kernel(cell_count):
    def kernel(
        raw_ref,
        rows_ref,
        weight_ref,
        hist_ref,
        gain_ref,
        shift_ref,
        gain_coarse_ref,
        shift_coarse_ref,
        out_ref,
        load_ref,
        hidden_ref,
        pool_ref,
    ):
        wide_depth, wide_height, channels, width = raw_ref.shape
        depth, height = out_ref.shape[:2]
        rows = rows_ref[...]
        merged = jnp.sum(rows, axis=0)
        peak_vol = jnp.max(rows, axis=0)
        scale, offset = affine(
            column(merged, channels, 0),
            column(merged, channels, channels),
            cell_count,
            column(gain_ref[0:1, :], channels, 0),
            column(shift_ref[0:1, :], channels, 0),
        )
        bound = bound_of(hist_ref, 1)
        at_z = lax.axis_index("sz")
        at_y = lax.axis_index("sy")
        last_z = lax.axis_size("sz") - 1
        last_y = lax.axis_size("sy") - 1

        def plane(z, peak):
            inside_z = ((z > 0) | (at_z > 0)) & ((z < wide_depth - 1) | (at_z < last_z))
            own = jnp.where((z >= 1) & (z < wide_depth - 1), 1.0, 0.0).astype(bf16)
            for y in range(wide_height):
                inside = inside_z
                if y == 0:
                    inside = inside & (at_y > 0)
                if y == wide_height - 1:
                    inside = inside & (at_y < last_y)
                hidden = activated(raw_ref[z, y], scale, offset)
                if 1 <= y < wide_height - 1:
                    peak = jnp.maximum(peak, jnp.abs(hidden) * own)
                inside = jnp.where(inside, 1.0, 0.0).astype(bf16)
                hidden_ref[z, y] = bounded(hidden, bound) * inside
            return peak

        blank = jnp.zeros((channels, width), f32)
        peak = lax.fori_loop(0, wide_depth, plane, jnp.zeros((channels, width), bf16))
        weight = weight_ref[...]
        sign = jnp.where(column(gain_ref[1:2, :], channels, 0) >= 0, 1.0, -1.0).astype(f32)
        half_height = height // 2

        def pair(zp, sums):
            total, square, least, most = sums
            for yp in range(half_height):
                best = None
                for dz in range(2):
                    outs = conv_rows(hidden_ref, weight, 2 * zp + dz, 2 * yp, channels)
                    for half in range(2):
                        out_ref[2 * zp + dz, 2 * yp + half] = outs[half]
                        total = total + outs[half]
                        square = square + outs[half] * outs[half]
                        signed = outs[half] * sign
                        best = signed if best is None else jnp.maximum(best, signed)
                best = jnp.maximum(best, pltpu.roll(best, LANES - 1, 1)) * sign
                pool_ref[zp, yp] = best
                least = jnp.minimum(least, best)
                most = jnp.maximum(most, best)
            return total, square, least, most

        total, square, least, most = lax.fori_loop(
            0, depth // 2, pair, (blank, blank, blank + 1e30, blank - 1e30)
        )
        most, least = peak_of(most), -peak_of(-least)
        center = 0.5 * (most + least)
        reach = jnp.maximum(0.5 * (most - least), 1e-30)
        rate = CODE_SPAN / reach
        pick = jnp.where(
            lax.broadcasted_iota(jnp.int32, (2 * LANES, LANES), 0)
            == 2 * lax.broadcasted_iota(jnp.int32, (2 * LANES, LANES), 1),
            1.0,
            0.0,
        ).astype(bf16)
        for zp in range(depth // 2):
            for yq in range(half_height // 2):
                both = jnp.concatenate([pool_ref[zp, 2 * yq], pool_ref[zp, 2 * yq + 1]], axis=1)
                both = jnp.exp((both - center) * rate).astype(bf16)
                load_ref[
                    zp * channels : (zp + 1) * channels, yq * LANES : (yq + 1) * LANES
                ] = jnp.dot(both, pick, preferred_element_type=f32).astype(bf16)
        mine = gain_coarse_ref.shape[1]
        row = as_row(jnp.sum(total, axis=1, keepdims=True), 0)
        row = row + as_row(jnp.sum(square, axis=1, keepdims=True), channels)
        row = row + at_lane(peak_vol, PEAK_AT)
        row = row + at_lane(peak_of(peak), PEAK_AT + 1)
        row = row + at_lane(center, CODE_AT)
        row = row + at_lane(reach / CODE_SPAN, CODE_AT + 1)
        row = row + as_row(column(gain_coarse_ref[0:1, :], mine, 0), GAIN_AT)
        row = row + as_row(column(shift_coarse_ref[0:1, :], mine, 0), SHIFT_AT)
        high = row.astype(bf16).astype(f32)
        middle = (row - high).astype(bf16).astype(f32)
        low = row - high - middle
        level = lax.broadcasted_iota(jnp.int32, (16, LANES), 0)
        parts = jnp.where(
            level == 0, high, jnp.where(level == 1, middle, jnp.where(level == 2, low, 0.0))
        )
        body = (depth // 2) * channels
        load_ref[body:, 0:LANES] = parts.astype(bf16)
        load_ref[body:, LANES:] = jnp.zeros((16, load_ref.shape[1] - LANES), bf16)

    return kernel


def spread_rows(cells, store):
    count = cells.shape[1] // LANES
    parts = [cells[:, j * LANES : (j + 1) * LANES] for j in range(count)]
    turned = [pltpu.roll(part, LANES // 2, 1) for part in parts]
    lower = lax.broadcasted_iota(jnp.int32, parts[0].shape, 1) < LANES // 2
    blank = jnp.zeros_like(parts[0])
    for j in range(count):
        before = turned[j - 1] if j > 0 else blank
        after = turned[j + 1] if j + 1 < count else blank
        store(0, j, jnp.where(lower, before, turned[j]))
        store(1, j, parts[j])
        store(2, j, jnp.where(lower, turned[j], after))


def third_kernel(fine_cells, coarse_cells, load_rows, piece):
    def kernel(
        all_ref,
        hist_ref,
        gain_ref,
        shift_ref,
        out_ref,
        peak_ref,
        affine_ref,
        pool_ref,
        cells_ref,
        raw_ref,
    ):
        y_groups = all_ref.shape[0]
        z_groups = lax.axis_size("sz")
        span = all_ref.shape[2]
        planes, chan_all, flat = raw_ref.shape
        channels = gain_ref.shape[1]
        chan_own = piece // 3
        row_len = LANES // 2
        body = load_rows - 16
        z_own = body // channels
        at_z = lax.axis_index("sz")
        totals = jnp.zeros((16, LANES), f32)
        tops = jnp.zeros((1, LANES), f32)
        rows = {}
        for s in range(y_groups):
            for k in range(z_groups):
                parts = all_ref[s, k * load_rows + body : (k + 1) * load_rows, 0:LANES].astype(f32)
                totals = totals + parts
                rows[s, k] = jnp.sum(parts, axis=0, keepdims=True)
                tops = jnp.maximum(tops, rows[s, k])
        merged = jnp.sum(totals, axis=0, keepdims=True)
        scale, offset = affine(
            column(merged, channels, 0),
            column(merged, channels, channels),
            fine_cells,
            column(gain_ref[1:2, :], channels, 0),
            column(shift_ref[1:2, :], channels, 0),
        )
        lanes = lax.broadcasted_iota(jnp.int32, (channels, LANES), 1)
        affine_ref[...] = jnp.where(lanes == 0, scale, jnp.where(lanes == 1, offset, 0.0))
        bound = bound_of(hist_ref, 2)
        peak_pool = jnp.zeros((channels, span), bf16)
        for s in range(y_groups):
            for k in range(z_groups):
                center = rows[s, k][:, CODE_AT : CODE_AT + 1]
                reach = rows[s, k][:, CODE_AT + 1 : CODE_AT + 2]
                rate = scale * reach
                start = scale * center + offset
                for zp in range(z_own):
                    at = k * load_rows + zp * channels
                    code = jnp.log(all_ref[s, at : at + channels, :].astype(f32))
                    value = activated(code, rate, start)
                    peak_pool = jnp.maximum(peak_pool, jnp.abs(value))
                    pool_ref[(at_z ^ k) * z_own + zp, :, s * span : (s + 1) * span] = bounded(
                        value, bound
                    )
        cells_ref[0] = jnp.zeros(cells_ref.shape[1:], bf16)
        cells_ref[planes + 1] = jnp.zeros(cells_ref.shape[1:], bf16)

        def spread_pool(z, carry):
            def store(dy, j, value):
                cells_ref[
                    z + 1, dy * channels : (dy + 1) * channels, j * LANES : (j + 1) * LANES
                ] = value

            spread_rows(pool_ref[z], store)
            return carry

        lax.fori_loop(0, planes, spread_pool, 0)
        weights = z_groups * load_rows
        near_weight = jnp.concatenate(
            [all_ref[s, weights : weights + piece, :] for s in range(y_groups)], axis=0
        )
        far_weight = jnp.concatenate(
            [all_ref[s, weights + piece :, 0 : 9 * channels - span] for s in range(y_groups)],
            axis=0,
        )

        def third(z, sums):
            totals, squares = list(sums[0]), list(sums[1])
            for t in range(flat // span):
                window = jnp.concatenate(
                    [cells_ref[z + dz, :, t * span : (t + 1) * span] for dz in range(3)], axis=0
                )
                taps = jnp.dot(near_weight, window[:span], preferred_element_type=f32)
                taps = taps + jnp.dot(far_weight, window[span:], preferred_element_type=f32)
                for s in range(y_groups):
                    for half in range(span // LANES):
                        at = s * piece
                        part = taps[at : at + piece, half * LANES : (half + 1) * LANES]
                        out = tap_sum(
                            part[:chan_own],
                            part[chan_own : 2 * chan_own],
                            part[2 * chan_own :],
                            row_len,
                        )
                        start = t * span + half * LANES
                        raw_ref[
                            z, s * chan_own : (s + 1) * chan_own, start : start + LANES
                        ] = out
                        totals[s] = totals[s] + out
                        squares[s] = squares[s] + out * out
            return tuple(totals), tuple(squares)

        blank = jnp.zeros((chan_own, LANES), f32)
        zero = tuple(blank for _ in range(y_groups))
        totals, squares = lax.fori_loop(0, planes, third, (zero, zero))
        pairs = [
            affine(
                jnp.sum(totals[s], axis=1, keepdims=True),
                jnp.sum(squares[s], axis=1, keepdims=True),
                coarse_cells,
                column(rows[s, 0], chan_own, GAIN_AT),
                column(rows[s, 0], chan_own, SHIFT_AT),
            )
            for s in range(y_groups)
        ]
        scale = jnp.concatenate([one[0] for one in pairs], axis=0)
        offset = jnp.concatenate([one[1] for one in pairs], axis=0)
        bound = bound_of(hist_ref, 3)

        def normed(z, peak):
            for j in range(flat // LANES):
                lanes = slice(j * LANES, (j + 1) * LANES)
                value = activated(raw_ref[z, :, lanes], scale, offset)
                peak = jnp.maximum(peak, jnp.abs(value))
                out_ref[z, :, lanes] = bounded(value, bound)
            return peak

        peak_coarse = lax.fori_loop(0, planes, normed, jnp.zeros((chan_all, LANES), bf16))
        row = at_lane(tops[:, PEAK_AT : PEAK_AT + 1], 0)
        row = row + at_lane(tops[:, PEAK_AT + 1 : PEAK_AT + 2], 1)
        row = row + at_lane(peak_of(peak_pool), 2)
        row = row + at_lane(peak_of(peak_coarse), 3)
        peak_ref[...] = row

    return kernel


def fourth_kernel(coarse_cells):
    def kernel(
        cells_ref,
        weight_ref,
        gain_ref,
        shift_ref,
        raw_ref,
        affine_ref,
        out_ref,
        skip_ref,
        hidden_ref,
        last_ref,
        wide_ref,
    ):
        planes, chan_all, flat = cells_ref.shape
        chan_own, z_own = out_ref.shape[1:3]
        span = 2 * LANES
        row_len = LANES // 2
        hidden_ref[0] = jnp.zeros(hidden_ref.shape[1:], bf16)
        hidden_ref[planes + 1] = jnp.zeros(hidden_ref.shape[1:], bf16)

        def spread_hidden(z, carry):
            def store(dy, j, part):
                hidden_ref[
                    z + 1, dy * chan_all : (dy + 1) * chan_all, j * LANES : (j + 1) * LANES
                ] = part

            spread_rows(cells_ref[z], store)
            return carry

        lax.fori_loop(0, planes, spread_hidden, 0)
        weight = weight_ref[...]

        def fourth(z, sums):
            total, square = sums
            for t in range(flat // span):
                window = jnp.concatenate(
                    [hidden_ref[z + dz, :, t * span : (t + 1) * span] for dz in range(3)], axis=0
                )
                taps = jnp.dot(weight, window, preferred_element_type=f32)
                for half in range(span // LANES):
                    part = taps[:, half * LANES : (half + 1) * LANES]
                    out = tap_sum(
                        part[:chan_own],
                        part[chan_own : 2 * chan_own],
                        part[2 * chan_own :],
                        row_len,
                    )
                    start = t * span + half * LANES
                    last_ref[z, :, start : start + LANES] = out
                    total = total + out
                    square = square + out * out
            return total, square

        blank = jnp.zeros((chan_own, LANES), f32)
        total, square = lax.fori_loop(0, planes, fourth, (blank, blank))
        scale, offset = affine(
            jnp.sum(total, axis=1, keepdims=True),
            jnp.sum(square, axis=1, keepdims=True),
            coarse_cells,
            column(gain_ref[1:2, :], chan_own, 0),
            column(shift_ref[1:2, :], chan_own, 0),
        )
        at_z = lax.axis_index("sz")
        own = [
            activated(last_ref[at_z * z_own + i], scale, offset).astype(f32) for i in range(z_own)
        ]
        for c in range(chan_own):
            out_ref[0, c] = jnp.concatenate([one[c : c + 1] for one in own], axis=0).astype(bf16)
        depth, height, channels, width = raw_ref.shape
        rows = depth * height
        scale = affine_ref[:, 0:1]
        offset = affine_ref[:, 1:2]
        for r in range(rows):
            wide_ref[pl.ds(r, channels, stride=rows), :] = activated(
                raw_ref[r // height, r % height], scale, offset
            ).astype(f32)
        skip_ref[0] = wide_ref[...].reshape(channels, depth, height, width).astype(bf16)

    return kernel


def shape(dims, dtype):
    return jax.ShapeDtypeStruct(dims, dtype)


def near_shape(dims, dtype):
    return pltpu.VMEM(dims, dtype)


def held(value):
    return pltpu.with_memory_space_constraint(value, pltpu.VMEM)


def per_device(
    volume,
    amax_history,
    conv_first,
    conv_second,
    conv_third,
    conv_fourth,
    gain_fine,
    shift_fine,
    gain_coarse,
    shift_coarse,
):
    channels, depth, height, width = volume.shape[1:]
    z_groups = lax.axis_size("sz")
    y_groups = lax.axis_size("sy")
    samples = lax.axis_size("sample")
    fine_cells = float(depth * z_groups * height * y_groups * width)
    coarse_cells = fine_cells / 8
    chan_own = conv_third.shape[1]
    chan_all = conv_fourth.shape[2]
    span = (height // 2) * (width // 2)
    planes = (depth // 2) * z_groups
    flat = span * y_groups
    group = z_groups * y_groups
    load_rows = (depth // 2) * channels + 16

    cells, first, second, peak = pl.pallas_call(
        prep_kernel,
        out_shape=(
            near_shape((depth, height, channels, width), bf16),
            near_shape((HALO, height, channels, width), bf16),
            near_shape((HALO, height, channels, width), bf16),
            near_shape((1, LANES), f32),
        ),
        scratch_shapes=[pltpu.VMEM((channels * depth * height, width), f32)],
        name="prep",
    )(volume, amax_history)
    third_rows = 3 * chan_own
    m1, m2, m3, m4 = pl.pallas_call(
        matrix_kernel,
        out_shape=(
            near_shape((3 * channels, 9 * channels), bf16),
            near_shape((3 * channels, 9 * channels), bf16),
            near_shape((2 * third_rows, span), bf16),
            near_shape((third_rows, 9 * chan_all), bf16),
        ),
        scratch_shapes=[pltpu.VMEM((third_rows, 9 * channels), bf16)],
        name="matrices",
    )(held(peak), conv_first, conv_second, conv_third, conv_fourth)
    pair_first, pair_second = near("sz")
    z_first = lax.ppermute(first, "sz", pair_first)
    z_second = lax.ppermute(second, "sz", pair_second)
    deep_depth = depth + 2 * HALO
    first, second = pl.pallas_call(
        deep_kernel,
        out_shape=(
            near_shape((deep_depth, HALO, channels, width), bf16),
            near_shape((deep_depth, HALO, channels, width), bf16),
        ),
        name="deep",
    )(held(cells), held(z_first), held(z_second), held(m1))
    pair_first, pair_second = near("sy")
    y_first = lax.ppermute(first, "sy", pair_first)
    y_second = lax.ppermute(second, "sy", pair_second)
    raw_first, row = pl.pallas_call(
        first_kernel,
        out_shape=(
            near_shape((depth + 2, height + 2, channels, width), f32),
            near_shape((group, 1, LANES), f32),
        ),
        scratch_shapes=[pltpu.VMEM((deep_depth, height + 2 * HALO, channels, width), bf16)],
        name="first",
    )(*(held(x) for x in (cells, z_first, z_second, y_first, y_second, m1, peak)))
    rows = lax.all_to_all(row, ("sy", "sz"), 0, 0, tiled=True)
    raw_second, load = pl.pallas_call(
        second_kernel(fine_cells),
        out_shape=(
            near_shape((depth, height, channels, width), f32),
            near_shape((load_rows, span), bf16),
        ),
        scratch_shapes=[
            pltpu.VMEM((depth + 2, height + 2, channels, width), bf16),
            pltpu.VMEM((depth // 2, height // 2, channels, width), f32),
        ],
        name="second",
    )(held(raw_first), held(rows), held(m2), amax_history, gain_fine, shift_fine, gain_coarse, shift_coarse)
    loads = [load]
    for k in range(1, z_groups):
        loads.append(lax.ppermute(load, "sz", [(i, i ^ k) for i in range(z_groups)]))
    loads.append(m3)
    gathered = lax.all_gather(jnp.concatenate(loads, axis=0), "sy", axis=0)
    hidden, peaks, fine_affine = pl.pallas_call(
        third_kernel(fine_cells, coarse_cells, load_rows, third_rows),
        out_shape=(
            near_shape((planes, chan_all, flat), bf16),
            near_shape((1, LANES), f32),
            near_shape((channels, LANES), f32),
        ),
        scratch_shapes=[
            pltpu.VMEM((planes, channels, flat), bf16),
            pltpu.VMEM((planes + 2, 3 * channels, flat), bf16),
            pltpu.VMEM((planes, chan_all, flat), f32),
        ],
        name="third",
    )(held(gathered), amax_history, gain_fine, shift_fine)
    if samples <= 4:
        others = [
            lax.ppermute(peaks, "sample", [(i, (i + k) % samples) for i in range(samples)])
            for k in range(1, samples)
        ]
    else:
        others = [lax.pmax(peaks, "sample")]
    coarse, skip = pl.pallas_call(
        fourth_kernel(coarse_cells),
        out_shape=(
            shape((1, chan_own, depth // 2, flat), bf16),
            shape((1, channels, depth, height, width), bf16),
        ),
        scratch_shapes=[
            pltpu.VMEM((planes + 2, 3 * chan_all, flat), bf16),
            pltpu.VMEM((planes, chan_own, flat), f32),
            pltpu.VMEM((channels * depth * height, width), f32),
        ],
        name="fourth",
    )(held(hidden), held(m4), gain_coarse, shift_coarse, held(raw_second), held(fine_affine))
    for other in others:
        peaks = jnp.maximum(peaks, other)
    levels = amax_history.shape[0]
    return skip, coarse, peaks[0, :levels]


def solution(mesh):
    return jax.shard_map(
        per_device,
        mesh=mesh,
        in_specs=(
            P("sample", None, "sz", "sy", None),
            P(),
            P(),
            P(),
            P(None, "sy", None),
            P(None, "sy", None),
            P(),
            P(),
            P(None, "sy"),
            P(None, "sy"),
        ),
        out_specs=(P("sample", None, "sz", "sy", None), P("sample", "sy", "sz", None), P()),
        check_vma=False,
    )
```

```python
import jax
import jax.numpy as jnp
from jax import lax
from jax.experimental import pallas as pl
from jax.experimental.pallas import tpu as pltpu
from jax.sharding import PartitionSpec as P

norm_eps = 1e-05
leak_slope = 0.01
UNROLL_FIRST = 1
UNROLL_HIDDEN = 1
UNROLL_SECOND = 1
UNROLL_SPREAD = 1
UNROLL_THIRD = 1
UNROLL_NORMED = 1
UNROLL_FOURTH = 1
f32 = jnp.float32
bf16 = jnp.bfloat16
LANES = 128
HALO = 2
PEAK_AT = 64
CODE_AT = 66
GAIN_AT = 80
SHIFT_AT = 96
CODE_SPAN = 83.0


def near(axis):
    count = lax.axis_size(axis)
    first = [(i, i ^ 1) for i in range(count)]
    second = [(i, min(max(((i + 1) ^ 1) - 1, 0), count - 1)) for i in range(count)]
    return first, second


def column(row, channels, start):
    lanes = lax.broadcasted_iota(jnp.int32, (channels, row.shape[1]), 1)
    chans = lax.broadcasted_iota(jnp.int32, (channels, row.shape[1]), 0)
    return jnp.sum(jnp.where(lanes == chans + start, row, 0.0), axis=1, keepdims=True)


def as_row(col, start):
    channels = col.shape[0]
    lanes = lax.broadcasted_iota(jnp.int32, (channels, LANES), 1)
    chans = lax.broadcasted_iota(jnp.int32, (channels, LANES), 0)
    return jnp.sum(jnp.where(lanes == chans + start, col, 0.0), axis=0, keepdims=True)


def at_lane(value, lane):
    lanes = lax.broadcasted_iota(jnp.int32, (1, LANES), 1)
    return jnp.where(lanes == lane, value, 0.0)


def affine(total, square, cells, gains, offset):
    mean = total / cells
    spread = square / cells - mean * mean
    scale = lax.rsqrt(spread + norm_eps) * gains
    return scale, offset - mean * scale


def activated(values, scale, offset):
    normed = values * scale + offset
    return jnp.maximum(normed, leak_slope * normed).astype(bf16)


def peak_of(values):
    values = values.astype(f32)
    return jnp.max(jnp.max(values, axis=1, keepdims=True), axis=0, keepdims=True)


def bounded(values, bound):
    return jnp.minimum(jnp.maximum(values, -bound), bound)


BOUND_AT = 4
LAST_AT = 8


def bound_of(hist_ref, level):
    return jnp.max(hist_ref[level : level + 1, :], axis=1, keepdims=True)


def lane_of(param_ref, lane, channels):
    return param_ref[0:channels, lane : lane + 1]


def clip_bound(param_ref, level):
    return param_ref[0:1, BOUND_AT + level : BOUND_AT + level + 1].astype(bf16)


def matrix_of(weight, taps_ref, groups):
    out_chan = weight.shape[1]
    for dx in range(3):
        taps_ref[dx * out_chan : (dx + 1) * out_chan, :] = jnp.concatenate(
            [weight[3 * j + dx] for j in groups], axis=1
        )


def matrix_kernel(
    peak_ref,
    first_ref,
    second_ref,
    third_ref,
    fourth_ref,
    hist_ref,
    gain_ref,
    shift_ref,
    gain_coarse_ref,
    shift_coarse_ref,
    m1_ref,
    m2_ref,
    m3_ref,
    m4_ref,
    param_ref,
    gain_row_ref,
):
    taps = first_ref.shape[0]
    matrix_of(first_ref, m1_ref, range(taps // 3))
    matrix_of(second_ref, m2_ref, range(taps // 3))
    own = third_ref.shape[1]
    matrix_of(third_ref, m3_ref.at[0 : 3 * own], range(taps // 3 - 1))
    last = [third_ref[taps - 3 + dx] for dx in range(3)]
    rest = m3_ref.shape[1] - 3 * third_ref.shape[2]
    m3_ref[3 * own :, :] = jnp.concatenate(last + [jnp.zeros((own, rest), bf16)], axis=1)
    for dy in range(3):
        for dx in range(3):
            at = (3 * dy + dx) * own
            m4_ref[at : at + own, :] = jnp.concatenate(
                [fourth_ref[9 * dz + 3 * dy + dx] for dz in range(3)], axis=1
            )
    channels = param_ref.shape[0]
    lanes = lax.broadcasted_iota(jnp.int32, (channels, LANES), 1)
    params = jnp.zeros((channels, LANES), f32)
    columns = []
    for layer in range(2):
        columns.append((2 * layer, column(gain_ref[layer : layer + 1, :], channels, 0)))
        columns.append((2 * layer + 1, column(shift_ref[layer : layer + 1, :], channels, 0)))
    for level in range(hist_ref.shape[0]):
        columns.append((BOUND_AT + level, bound_of(hist_ref, level)))
    pad = jnp.zeros((channels - own, 1), f32)
    for place, ref in ((LAST_AT, gain_coarse_ref), (LAST_AT + 1, shift_coarse_ref)):
        columns.append((place, jnp.concatenate([column(ref[1:2, :], own, 0), pad], axis=0)))
    for lane, value in columns:
        params = jnp.where(lanes == lane, value, params)
    param_ref[...] = params
    gain_row_ref[...] = as_row(column(gain_coarse_ref[0:1, :], own, 0), GAIN_AT) + as_row(
        column(shift_coarse_ref[0:1, :], own, 0), SHIFT_AT
    )


def tap_sum(left, middle, right, period):
    lane = lax.broadcasted_iota(jnp.int32, middle.shape, 1) % period
    up = pltpu.roll(left, 1, 1)
    down = pltpu.roll(right, LANES - 1, 1)
    return middle + jnp.where(lane == 0, 0.0, up) + jnp.where(lane == period - 1, 0.0, down)


def prep_kernel(vol_ref, hist_ref, cells_ref, first_ref, second_ref, peak_ref, wide_ref):
    channels, depth, height, width = vol_ref.shape[1:]
    rows = depth * height
    wide = vol_ref[0].astype(f32).reshape(channels * rows, width)
    wide_ref[...] = wide
    peak_ref[...] = jnp.broadcast_to(peak_of(jnp.abs(wide)), (1, LANES))
    bound = bound_of(hist_ref, 0).astype(bf16)
    for r in range(rows):
        cells_ref[r // height, r % height] = bounded(
            wide_ref[pl.ds(r, channels, stride=rows), :].astype(bf16), bound
        )
    even = lax.axis_index("sz") % 2 == 0
    start_first = jnp.where(even, depth - HALO, 0)
    start_second = jnp.where(even, 0, depth - HALO)
    first_ref[...] = cells_ref[pl.ds(start_first, HALO)]
    second_ref[...] = cells_ref[pl.ds(start_second, HALO)]


def sides(axis, first, second):
    at = lax.axis_index(axis)
    count = lax.axis_size(axis)
    even = at % 2 == 0
    blank = jnp.zeros_like(first)
    below = jnp.where(at == 0, blank, jnp.where(even, second, first))
    above = jnp.where(at == count - 1, blank, jnp.where(even, first, second))
    return below, above


def deep_kernel(cells_ref, got_first_ref, got_second_ref, matrix_ref, first_ref, second_ref):
    depth, height = cells_ref.shape[:2]
    even = lax.axis_index("sy") % 2 == 0
    starts = (jnp.where(even, height - HALO, 0), jnp.where(even, 0, height - HALO))
    odd_z = lax.axis_index("sz") % 2
    far = HALO + depth
    for start, out_ref in zip(starts, (first_ref, second_ref)):
        rows = pl.ds(start, HALO)
        out_ref[pl.ds((1 - odd_z) * far, HALO)] = got_first_ref[:, rows]
        out_ref[pl.ds(odd_z * far, HALO)] = got_second_ref[:, rows]
        out_ref[HALO:far] = cells_ref[:, rows]


def conv_rows(cells_ref, weight, z, y, out_chan):
    window = jnp.concatenate(
        [
            jnp.concatenate(
                [cells_ref[z + dz, y + dy], cells_ref[z + dz, y + 1 + dy]], axis=1
            )
            for dz in range(3)
            for dy in range(3)
        ],
        axis=0,
    )
    taps = jnp.dot(weight, window, preferred_element_type=f32)
    outs = []
    for half in range(2):
        part = taps[:, half * LANES : (half + 1) * LANES]
        outs.append(
            tap_sum(
                part[:out_chan], part[out_chan : 2 * out_chan], part[2 * out_chan :], LANES
            )
        )
    return outs


def first_kernel(
    own_ref,
    z_first_ref,
    z_second_ref,
    y_first_ref,
    y_second_ref,
    weight_ref,
    peak_ref,
    raw_ref,
    row_ref,
    cells_ref,
):
    depth, height = raw_ref.shape[:2]
    channels = raw_ref.shape[2]
    own_depth, own_height = own_ref.shape[:2]
    below, above = sides("sz", z_first_ref[...], z_second_ref[...])
    rows = slice(HALO, HALO + own_height)
    cells_ref[0:HALO, rows] = below
    cells_ref[HALO : HALO + own_depth, rows] = own_ref[...]
    cells_ref[HALO + own_depth :, rows] = above
    below, above = sides("sy", y_first_ref[...], y_second_ref[...])
    cells_ref[:, 0:HALO] = below
    cells_ref[:, HALO + own_height :] = above

    @pl.when(lax.axis_index("sz") == 0)
    def _():
        for edge in (slice(0, HALO), slice(HALO + own_height, 2 * HALO + own_height)):
            cells_ref[0:HALO, edge] = jnp.zeros((HALO, HALO) + own_ref.shape[2:], bf16)

    @pl.when(lax.axis_index("sz") == lax.axis_size("sz") - 1)
    def _():
        for edge in (slice(0, HALO), slice(HALO + own_height, 2 * HALO + own_height)):
            cells_ref[HALO + own_depth :, edge] = jnp.zeros(
                (HALO, HALO) + own_ref.shape[2:], bf16
            )

    weight = weight_ref[...]

    def plane(z, sums):
        total, square = sums
        own = jnp.where((z >= 1) & (z < depth - 1), 1.0, 0.0).astype(f32)
        for y in range(0, height, 2):
            outs = conv_rows(cells_ref, weight, z, y, channels)
            for half in range(2):
                raw_ref[z, y + half] = outs[half]
                if 1 <= y + half < height - 1:
                    mine = outs[half] * own
                    total = total + mine
                    square = square + mine * mine
        return total, square

    blank = jnp.zeros((channels, LANES), f32)
    total, square = lax.fori_loop(0, depth, plane, (blank, blank), unroll=UNROLL_FIRST)
    row = as_row(jnp.sum(total, axis=1, keepdims=True), 0)
    row = row + as_row(jnp.sum(square, axis=1, keepdims=True), channels)
    row = row + at_lane(peak_ref[...], PEAK_AT)
    row_ref[...] = jnp.broadcast_to(row[None], row_ref.shape)


def second_kernel(cell_count):
    def kernel(
        raw_ref,
        rows_ref,
        weight_ref,
        param_ref,
        gain_row_ref,
        out_ref,
        load_ref,
        hidden_ref,
        pool_ref,
    ):
        wide_depth, wide_height, channels, width = raw_ref.shape
        depth, height = out_ref.shape[:2]
        rows = rows_ref[...]
        merged = jnp.sum(rows, axis=0)
        peak_vol = jnp.max(rows, axis=0)
        scale, offset = affine(
            column(merged, channels, 0),
            column(merged, channels, channels),
            cell_count,
            lane_of(param_ref, 0, channels),
            lane_of(param_ref, 1, channels),
        )
        bound = clip_bound(param_ref, 1)
        at_z = lax.axis_index("sz")
        at_y = lax.axis_index("sy")
        last_z = lax.axis_size("sz") - 1
        last_y = lax.axis_size("sy") - 1

        def plane(z, peak):
            inside_z = ((z > 0) | (at_z > 0)) & ((z < wide_depth - 1) | (at_z < last_z))
            own = jnp.where((z >= 1) & (z < wide_depth - 1), 1.0, 0.0).astype(bf16)
            for y in range(wide_height):
                inside = inside_z
                if y == 0:
                    inside = inside & (at_y > 0)
                if y == wide_height - 1:
                    inside = inside & (at_y < last_y)
                hidden = activated(raw_ref[z, y], scale, offset)
                if 1 <= y < wide_height - 1:
                    peak = jnp.maximum(peak, jnp.abs(hidden) * own)
                inside = jnp.where(inside, 1.0, 0.0).astype(bf16)
                hidden_ref[z, y] = bounded(hidden, bound) * inside
            return peak

        blank = jnp.zeros((channels, width), f32)
        peak = lax.fori_loop(
            0, wide_depth, plane, jnp.zeros((channels, width), bf16), unroll=UNROLL_HIDDEN
        )
        weight = weight_ref[...]
        sign = jnp.where(lane_of(param_ref, 2, channels) >= 0, 1.0, -1.0).astype(f32)
        half_height = height // 2

        def pair(zp, sums):
            total, square, least, most = sums
            for yp in range(half_height):
                best = None
                for dz in range(2):
                    outs = conv_rows(hidden_ref, weight, 2 * zp + dz, 2 * yp, channels)
                    for half in range(2):
                        out_ref[2 * zp + dz, 2 * yp + half] = outs[half]
                        total = total + outs[half]
                        square = square + outs[half] * outs[half]
                        signed = outs[half] * sign
                        best = signed if best is None else jnp.maximum(best, signed)
                best = jnp.maximum(best, pltpu.roll(best, LANES - 1, 1)) * sign
                pool_ref[zp, yp] = best
                least = jnp.minimum(least, best)
                most = jnp.maximum(most, best)
            return total, square, least, most

        total, square, least, most = lax.fori_loop(
            0,
            depth // 2,
            pair,
            (blank, blank, blank + 1e30, blank - 1e30),
            unroll=UNROLL_SECOND,
        )
        most, least = peak_of(most), -peak_of(-least)
        center = 0.5 * (most + least)
        reach = jnp.maximum(0.5 * (most - least), 1e-30)
        rate = CODE_SPAN / reach
        pick = jnp.where(
            lax.broadcasted_iota(jnp.int32, (2 * LANES, LANES), 0)
            == 2 * lax.broadcasted_iota(jnp.int32, (2 * LANES, LANES), 1),
            1.0,
            0.0,
        ).astype(bf16)
        for zp in range(depth // 2):
            for yq in range(half_height // 2):
                both = jnp.concatenate([pool_ref[zp, 2 * yq], pool_ref[zp, 2 * yq + 1]], axis=1)
                both = jnp.exp((both - center) * rate).astype(bf16)
                load_ref[
                    zp * channels : (zp + 1) * channels, yq * LANES : (yq + 1) * LANES
                ] = jnp.dot(both, pick, preferred_element_type=f32).astype(bf16)
        row = as_row(jnp.sum(total, axis=1, keepdims=True), 0)
        row = row + as_row(jnp.sum(square, axis=1, keepdims=True), channels)
        row = row + at_lane(peak_vol, PEAK_AT)
        row = row + at_lane(peak_of(peak), PEAK_AT + 1)
        row = row + at_lane(center, CODE_AT)
        row = row + at_lane(reach / CODE_SPAN, CODE_AT + 1)
        row = row + gain_row_ref[...]
        high = row.astype(bf16).astype(f32)
        middle = (row - high).astype(bf16).astype(f32)
        low = row - high - middle
        level = lax.broadcasted_iota(jnp.int32, (16, LANES), 0)
        parts = jnp.where(
            level == 0, high, jnp.where(level == 1, middle, jnp.where(level == 2, low, 0.0))
        )
        body = (depth // 2) * channels
        load_ref[body:, 0:LANES] = parts.astype(bf16)
        load_ref[body:, LANES:] = jnp.zeros((16, load_ref.shape[1] - LANES), bf16)

    return kernel


def spread_rows(cells, store):
    count = cells.shape[1] // LANES
    parts = [cells[:, j * LANES : (j + 1) * LANES] for j in range(count)]
    turned = [pltpu.roll(part, LANES // 2, 1) for part in parts]
    lower = lax.broadcasted_iota(jnp.int32, parts[0].shape, 1) < LANES // 2
    blank = jnp.zeros_like(parts[0])
    for j in range(count):
        before = turned[j - 1] if j > 0 else blank
        after = turned[j + 1] if j + 1 < count else blank
        store(0, j, jnp.where(lower, before, turned[j]))
        store(1, j, parts[j])
        store(2, j, jnp.where(lower, turned[j], after))


def third_kernel(fine_cells, coarse_cells, load_rows, piece):
    def kernel(
        all_ref,
        param_ref,
        fine_ref,
        out_ref,
        peak_ref,
        skip_ref,
        pool_ref,
        cells_ref,
        raw_ref,
        wide_ref,
        narrow_ref,
        done,
    ):
        y_groups = all_ref.shape[0]
        z_groups = lax.axis_size("sz")
        span = all_ref.shape[2]
        planes, chan_all, flat = raw_ref.shape
        channels = fine_ref.shape[2]
        chan_own = piece // 4
        row_len = LANES // 2
        body = load_rows - 16
        z_own = body // channels
        at_z = lax.axis_index("sz")
        totals = jnp.zeros((16, LANES), f32)
        tops = jnp.zeros((1, LANES), f32)
        rows = {}
        for s in range(y_groups):
            for k in range(z_groups):
                parts = all_ref[s, k * load_rows + body : (k + 1) * load_rows, 0:LANES].astype(f32)
                totals = totals + parts
                rows[s, k] = jnp.sum(parts, axis=0, keepdims=True)
                tops = jnp.maximum(tops, rows[s, k])
        merged = jnp.sum(totals, axis=0, keepdims=True)
        scale, offset = affine(
            column(merged, channels, 0),
            column(merged, channels, channels),
            fine_cells,
            lane_of(param_ref, 2, channels),
            lane_of(param_ref, 3, channels),
        )
        depth, height = fine_ref.shape[:2]
        fine_rows = depth * height
        for r in range(fine_rows):
            wide_ref[pl.ds(r, channels, stride=fine_rows), :] = activated(
                fine_ref[r // height, r % height], scale, offset
            ).astype(f32)
        narrow_ref[...] = wide_ref[...].reshape(narrow_ref.shape).astype(bf16)
        skip_copy = pltpu.make_async_copy(narrow_ref, skip_ref.at[0], done)
        skip_copy.start()
        bound = clip_bound(param_ref, 2)
        peak_pool = jnp.zeros((channels, span), bf16)
        for s in range(y_groups):
            for k in range(z_groups):
                center = rows[s, k][:, CODE_AT : CODE_AT + 1]
                reach = rows[s, k][:, CODE_AT + 1 : CODE_AT + 2]
                rate = scale * reach
                start = scale * center + offset
                for zp in range(z_own):
                    at = k * load_rows + zp * channels
                    code = jnp.log(all_ref[s, at : at + channels, :].astype(f32))
                    value = activated(code, rate, start)
                    peak_pool = jnp.maximum(peak_pool, jnp.abs(value))
                    pool_ref[(at_z ^ k) * z_own + zp, :, s * span : (s + 1) * span] = bounded(
                        value, bound
                    )
        cells_ref[0] = jnp.zeros(cells_ref.shape[1:], bf16)
        cells_ref[planes + 1] = jnp.zeros(cells_ref.shape[1:], bf16)
        places = (0, channels, 3 * channels)
        edge = lax.broadcasted_iota(jnp.int32, (channels, LANES), 1) % row_len

        def spread_pool(z, carry):
            def store(dy, j, value):
                lanes = slice(j * LANES, (j + 1) * LANES)
                cells_ref[z + 1, places[dy] : places[dy] + channels, lanes] = value
                if dy == 2:
                    blank = jnp.zeros_like(value)
                    up = jnp.where(edge == 0, blank, pltpu.roll(value, 1, 1))
                    down = jnp.where(edge == row_len - 1, blank, pltpu.roll(value, LANES - 1, 1))
                    cells_ref[z + 1, 2 * channels : 3 * channels, lanes] = up
                    cells_ref[z + 1, 4 * channels :, lanes] = down

            spread_rows(pool_ref[z], store)
            return carry

        lax.fori_loop(0, planes, spread_pool, 0, unroll=UNROLL_SPREAD)
        weights = z_groups * load_rows
        main = 3 * chan_own
        near_weight = jnp.concatenate(
            [all_ref[s, weights : weights + main, :] for s in range(y_groups)], axis=0
        )
        far_weight = jnp.concatenate(
            [all_ref[s, weights + main :, 0 : 3 * channels] for s in range(y_groups)], axis=0
        )

        def third(z, sums):
            totals, squares = list(sums[0]), list(sums[1])
            for t in range(flat // span):
                lanes = slice(t * span, (t + 1) * span)
                window = []
                for dz in range(3):
                    window.append(cells_ref[z + dz, 0 : 2 * channels, lanes])
                    if dz < 2:
                        window.append(cells_ref[z + dz, 3 * channels : 4 * channels, lanes])
                window = jnp.concatenate(window, axis=0)
                taps = jnp.dot(near_weight, window, preferred_element_type=f32)
                rest = jnp.dot(
                    far_weight,
                    cells_ref[z + 2, 2 * channels :, lanes],
                    preferred_element_type=f32,
                )
                for s in range(y_groups):
                    for half in range(span // LANES):
                        at = s * main
                        lanes = slice(half * LANES, (half + 1) * LANES)
                        part = taps[at : at + main, lanes]
                        out = tap_sum(
                            part[:chan_own],
                            part[chan_own : 2 * chan_own]
                            + rest[s * chan_own : (s + 1) * chan_own, lanes],
                            part[2 * chan_own :],
                            row_len,
                        )
                        start = t * span + half * LANES
                        raw_ref[
                            z, s * chan_own : (s + 1) * chan_own, start : start + LANES
                        ] = out
                        totals[s] = totals[s] + out
                        squares[s] = squares[s] + out * out
            return tuple(totals), tuple(squares)

        blank = jnp.zeros((chan_own, LANES), f32)
        zero = tuple(blank for _ in range(y_groups))
        totals, squares = lax.fori_loop(0, planes, third, (zero, zero), unroll=UNROLL_THIRD)
        pairs = [
            affine(
                jnp.sum(totals[s], axis=1, keepdims=True),
                jnp.sum(squares[s], axis=1, keepdims=True),
                coarse_cells,
                column(rows[s, 0], chan_own, GAIN_AT),
                column(rows[s, 0], chan_own, SHIFT_AT),
            )
            for s in range(y_groups)
        ]
        scale = jnp.concatenate([one[0] for one in pairs], axis=0)
        offset = jnp.concatenate([one[1] for one in pairs], axis=0)
        bound = clip_bound(param_ref, 3)

        def normed(z, peak):
            for j in range(flat // LANES):
                lanes = slice(j * LANES, (j + 1) * LANES)
                value = activated(raw_ref[z, :, lanes], scale, offset)
                peak = jnp.maximum(peak, jnp.abs(value))
                out_ref[z, :, lanes] = bounded(value, bound)
            return peak

        peak_coarse = lax.fori_loop(
            0, planes, normed, jnp.zeros((chan_all, LANES), bf16), unroll=UNROLL_NORMED
        )
        row = at_lane(tops[:, PEAK_AT : PEAK_AT + 1], 0)
        row = row + at_lane(tops[:, PEAK_AT + 1 : PEAK_AT + 2], 1)
        row = row + at_lane(peak_of(peak_pool), 2)
        row = row + at_lane(peak_of(peak_coarse), 3)
        peak_ref[...] = row
        skip_copy.wait()

    return kernel


def fourth_kernel(coarse_cells):
    def kernel(cells_ref, weight_ref, param_ref, out_ref, last_ref):
        planes, chan_all, flat = cells_ref.shape
        chan_own, z_own = out_ref.shape[1:3]
        span = 2 * LANES
        row_len = LANES // 2
        count = flat // LANES
        weight = weight_ref[...]
        lower = lax.broadcasted_iota(jnp.int32, (chan_own, LANES), 1) < row_len
        blank = jnp.zeros((chan_own, LANES), f32)

        def plane(z, taps_of, sums):
            total, square = sums
            by_row = [[], [], []]
            for t in range(flat // span):
                taps = taps_of(z, slice(t * span, (t + 1) * span))
                for half in range(span // LANES):
                    part = taps[:, half * LANES : (half + 1) * LANES]
                    for dy in range(3):
                        three = [
                            part[(3 * dy + dx) * chan_own : (3 * dy + dx + 1) * chan_own]
                            for dx in range(3)
                        ]
                        by_row[dy].append(tap_sum(*three, row_len))
            turned = [[pltpu.roll(one, row_len, 1) for one in by_row[dy]] for dy in (0, 2)]
            for j in range(count):
                before = turned[0][j - 1] if j > 0 else blank
                after = turned[1][j + 1] if j + 1 < count else blank
                out = by_row[1][j] + jnp.where(lower, before, turned[0][j])
                out = out + jnp.where(lower, turned[1][j], after)
                last_ref[z, :, j * LANES : (j + 1) * LANES] = out
                total = total + out
                square = square + out * out
            return total, square

        def inner(z, lanes):
            window = jnp.concatenate([cells_ref[z + dz, :, lanes] for dz in (-1, 0, 1)], axis=0)
            return jnp.dot(weight, window, preferred_element_type=f32)

        def lowest(z, lanes):
            window = jnp.concatenate([cells_ref[z + dz, :, lanes] for dz in (0, 1)], axis=0)
            return jnp.dot(weight[:, chan_all:], window, preferred_element_type=f32)

        def highest(z, lanes):
            window = jnp.concatenate([cells_ref[z + dz, :, lanes] for dz in (-1, 0)], axis=0)
            return jnp.dot(weight[:, : 2 * chan_all], window, preferred_element_type=f32)

        sums = plane(0, lowest, (blank, blank))
        sums = lax.fori_loop(
            1, planes - 1, lambda z, sums: plane(z, inner, sums), sums, unroll=UNROLL_FOURTH
        )
        total, square = plane(planes - 1, highest, sums)
        scale, offset = affine(
            jnp.sum(total, axis=1, keepdims=True),
            jnp.sum(square, axis=1, keepdims=True),
            coarse_cells,
            lane_of(param_ref, LAST_AT, chan_own),
            lane_of(param_ref, LAST_AT + 1, chan_own),
        )
        at_z = lax.axis_index("sz")
        own = [
            activated(last_ref[at_z * z_own + i], scale, offset).astype(f32) for i in range(z_own)
        ]
        for c in range(chan_own):
            out_ref[0, c] = jnp.concatenate([one[c : c + 1] for one in own], axis=0).astype(bf16)

    return kernel


def shape(dims, dtype):
    return jax.ShapeDtypeStruct(dims, dtype)


def near_shape(dims, dtype):
    return pltpu.VMEM(dims, dtype)


def held(value):
    return pltpu.with_memory_space_constraint(value, pltpu.VMEM)


def per_device(
    volume,
    amax_history,
    conv_first,
    conv_second,
    conv_third,
    conv_fourth,
    gain_fine,
    shift_fine,
    gain_coarse,
    shift_coarse,
):
    channels, depth, height, width = volume.shape[1:]
    z_groups = lax.axis_size("sz")
    y_groups = lax.axis_size("sy")
    samples = lax.axis_size("sample")
    fine_cells = float(depth * z_groups * height * y_groups * width)
    coarse_cells = fine_cells / 8
    chan_own = conv_third.shape[1]
    chan_all = conv_fourth.shape[2]
    span = (height // 2) * (width // 2)
    planes = (depth // 2) * z_groups
    flat = span * y_groups
    group = z_groups * y_groups
    load_rows = (depth // 2) * channels + 16

    cells, first, second, peak = pl.pallas_call(
        prep_kernel,
        out_shape=(
            near_shape((depth, height, channels, width), bf16),
            near_shape((HALO, height, channels, width), bf16),
            near_shape((HALO, height, channels, width), bf16),
            near_shape((1, LANES), f32),
        ),
        scratch_shapes=[pltpu.VMEM((channels * depth * height, width), f32)],
        name="prep",
    )(volume, amax_history)
    third_rows = 4 * chan_own
    m1, m2, m3, m4, params, gain_row = pl.pallas_call(
        matrix_kernel,
        out_shape=(
            near_shape((3 * channels, 9 * channels), bf16),
            near_shape((3 * channels, 9 * channels), bf16),
            near_shape((third_rows, 8 * channels), bf16),
            near_shape((9 * chan_own, 3 * chan_all), bf16),
            near_shape((channels, LANES), f32),
            near_shape((1, LANES), f32),
        ),
        name="matrices",
    )(
        held(peak),
        conv_first,
        conv_second,
        conv_third,
        conv_fourth,
        amax_history,
        gain_fine,
        shift_fine,
        gain_coarse,
        shift_coarse,
    )
    pair_first, pair_second = near("sz")
    z_first = lax.ppermute(first, "sz", pair_first)
    z_second = lax.ppermute(second, "sz", pair_second)
    deep_depth = depth + 2 * HALO
    first, second = pl.pallas_call(
        deep_kernel,
        out_shape=(
            near_shape((deep_depth, HALO, channels, width), bf16),
            near_shape((deep_depth, HALO, channels, width), bf16),
        ),
        name="deep",
    )(held(cells), held(z_first), held(z_second), held(m1))
    pair_first, pair_second = near("sy")
    y_first = lax.ppermute(first, "sy", pair_first)
    y_second = lax.ppermute(second, "sy", pair_second)
    raw_first, row = pl.pallas_call(
        first_kernel,
        out_shape=(
            near_shape((depth + 2, height + 2, channels, width), f32),
            near_shape((group, 1, LANES), f32),
        ),
        scratch_shapes=[pltpu.VMEM((deep_depth, height + 2 * HALO, channels, width), bf16)],
        name="first",
    )(*(held(x) for x in (cells, z_first, z_second, y_first, y_second, m1, peak)))
    rows = lax.all_to_all(row, ("sy", "sz"), 0, 0, tiled=True)
    raw_second, load = pl.pallas_call(
        second_kernel(fine_cells),
        out_shape=(
            near_shape((depth, height, channels, width), f32),
            near_shape((load_rows, span), bf16),
        ),
        scratch_shapes=[
            pltpu.VMEM((depth + 2, height + 2, channels, width), bf16),
            pltpu.VMEM((depth // 2, height // 2, channels, width), f32),
        ],
        name="second",
    )(*(held(x) for x in (raw_first, rows, m2, params, gain_row)))
    loads = [load]
    for k in range(1, z_groups):
        loads.append(lax.ppermute(load, "sz", [(i, i ^ k) for i in range(z_groups)]))
    loads.append(m3)
    gathered = lax.all_gather(jnp.concatenate(loads, axis=0), "sy", axis=0)
    hidden, peaks, skip = pl.pallas_call(
        third_kernel(fine_cells, coarse_cells, load_rows, third_rows),
        out_shape=(
            near_shape((planes, chan_all, flat), bf16),
            near_shape((1, LANES), f32),
            shape((1, channels, depth, height, width), bf16),
        ),
        out_specs=(
            pl.BlockSpec(memory_space=pltpu.VMEM),
            pl.BlockSpec(memory_space=pltpu.VMEM),
            pl.BlockSpec(memory_space=pl.ANY),
        ),
        scratch_shapes=[
            pltpu.VMEM((planes, channels, flat), bf16),
            pltpu.VMEM((planes + 2, 5 * channels, flat), bf16),
            pltpu.VMEM((planes, chan_all, flat), f32),
            pltpu.VMEM((channels * depth * height, width), f32),
            pltpu.VMEM((channels, depth, height, width), bf16),
            pltpu.SemaphoreType.DMA,
        ],
        name="third",
    )(*(held(x) for x in (gathered, params, raw_second)))
    if samples <= 4:
        others = [
            lax.ppermute(peaks, "sample", [(i, (i + k) % samples) for i in range(samples)])
            for k in range(1, samples)
        ]
    else:
        others = [lax.pmax(peaks, "sample")]
    coarse = pl.pallas_call(
        fourth_kernel(coarse_cells),
        out_shape=shape((1, chan_own, depth // 2, flat), bf16),
        scratch_shapes=[pltpu.VMEM((planes, chan_own, flat), f32)],
        name="fourth",
    )(*(held(x) for x in (hidden, m4, params)))
    for other in others:
        peaks = jnp.maximum(peaks, other)
    levels = amax_history.shape[0]
    return skip, coarse, peaks[0, :levels]


def solution(mesh):
    return jax.shard_map(
        per_device,
        mesh=mesh,
        in_specs=(
            P("sample", None, "sz", "sy", None),
            P(),
            P(),
            P(),
            P(None, "sy", None),
            P(None, "sy", None),
            P(),
            P(),
            P(None, "sy"),
            P(None, "sy"),
        ),
        out_specs=(P("sample", None, "sz", "sy", None), P("sample", "sy", "sz", None), P()),
        check_vma=False,
    )
```

```python
import jax
import jax.numpy as jnp
from jax import lax
from jax.experimental import pallas as pl
from jax.experimental.pallas import tpu as pltpu
from jax.sharding import PartitionSpec as P

norm_eps = 1e-05
leak_slope = 0.01
f32 = jnp.float32
bf16 = jnp.bfloat16
LANES = 128
HALO = 2
PEAK_AT = 64
CODE_AT = 66
GAIN_AT = 80
SHIFT_AT = 96
CODE_SPAN = 83.0


def pairings(axis):
    count = lax.axis_size(axis)
    first = [(i, i ^ 1) for i in range(count)]
    second = [(i, min(max(((i + 1) ^ 1) - 1, 0), count - 1)) for i in range(count)]
    return first, second


def column(row, channels, start):
    lanes = lax.broadcasted_iota(jnp.int32, (channels, row.shape[1]), 1)
    chans = lax.broadcasted_iota(jnp.int32, (channels, row.shape[1]), 0)
    return jnp.sum(jnp.where(lanes == chans + start, row, 0.0), axis=1, keepdims=True)


def as_row(col, start):
    channels = col.shape[0]
    lanes = lax.broadcasted_iota(jnp.int32, (channels, LANES), 1)
    chans = lax.broadcasted_iota(jnp.int32, (channels, LANES), 0)
    return jnp.sum(jnp.where(lanes == chans + start, col, 0.0), axis=0, keepdims=True)


def at_lane(value, lane):
    lanes = lax.broadcasted_iota(jnp.int32, (1, LANES), 1)
    return jnp.where(lanes == lane, value, 0.0)


def affine(total, square, cells, gains, offset):
    mean = total / cells
    spread = square / cells - mean * mean
    scale = lax.rsqrt(spread + norm_eps) * gains
    return scale, offset - mean * scale


def activated(values, scale, offset):
    normed = values * scale + offset
    return jnp.maximum(normed, leak_slope * normed).astype(bf16)


def peak_of(values):
    values = values.astype(f32)
    return jnp.max(jnp.max(values, axis=0, keepdims=True), axis=1, keepdims=True)


def bounded(values, bound):
    return jnp.minimum(jnp.maximum(values, -bound), bound)


BOUND_AT = 4
LAST_AT = 8


def bound_of(hist_ref, level):
    return jnp.max(hist_ref[level : level + 1, :], axis=1, keepdims=True)


def lane_of(param_ref, lane, channels):
    return param_ref[0:channels, lane : lane + 1]


def clip_bound(param_ref, level):
    return param_ref[0:1, BOUND_AT + level : BOUND_AT + level + 1].astype(bf16)


def matrix_of(weight, taps_ref, groups):
    out_chan = weight.shape[1]
    for dx in range(3):
        taps_ref[dx * out_chan : (dx + 1) * out_chan, :] = jnp.concatenate(
            [weight[3 * j + dx] for j in groups], axis=1
        )


def matrix_kernel(
    peak_ref,
    first_ref,
    second_ref,
    third_ref,
    fourth_ref,
    hist_ref,
    gain_ref,
    shift_ref,
    gain_coarse_ref,
    shift_coarse_ref,
    m1_ref,
    m2_ref,
    m3_ref,
    m4_ref,
    param_ref,
    gain_row_ref,
):
    taps = first_ref.shape[0]
    matrix_of(first_ref, m1_ref, range(taps // 3))
    matrix_of(second_ref, m2_ref, range(taps // 3))
    own = third_ref.shape[1]
    matrix_of(third_ref, m3_ref.at[0 : 3 * own], range(taps // 3 - 1))
    last = [third_ref[taps - 3 + dx] for dx in range(3)]
    rest = m3_ref.shape[1] - 3 * third_ref.shape[2]
    m3_ref[3 * own :, :] = jnp.concatenate(last + [jnp.zeros((own, rest), bf16)], axis=1)
    for dy in range(3):
        for dx in range(3):
            at = (3 * dy + dx) * own
            m4_ref[at : at + own, :] = jnp.concatenate(
                [fourth_ref[9 * dz + 3 * dy + dx] for dz in range(3)], axis=1
            )
    channels = param_ref.shape[0]
    lanes = lax.broadcasted_iota(jnp.int32, (channels, LANES), 1)
    params = jnp.zeros((channels, LANES), f32)
    columns = []
    for layer in range(2):
        columns.append((2 * layer, column(gain_ref[layer : layer + 1, :], channels, 0)))
        columns.append((2 * layer + 1, column(shift_ref[layer : layer + 1, :], channels, 0)))
    for level in range(hist_ref.shape[0]):
        columns.append((BOUND_AT + level, bound_of(hist_ref, level)))
    pad = jnp.zeros((channels - own, 1), f32)
    for place, ref in ((LAST_AT, gain_coarse_ref), (LAST_AT + 1, shift_coarse_ref)):
        columns.append((place, jnp.concatenate([column(ref[1:2, :], own, 0), pad], axis=0)))
    for lane, value in columns:
        params = jnp.where(lanes == lane, value, params)
    param_ref[...] = params
    gain_row_ref[...] = as_row(column(gain_coarse_ref[0:1, :], own, 0), GAIN_AT) + as_row(
        column(shift_coarse_ref[0:1, :], own, 0), SHIFT_AT
    )


def tap_sum(left, middle, right, period):
    lane = lax.broadcasted_iota(jnp.int32, middle.shape, 1) % period
    up = pltpu.roll(left, 1, 1)
    down = pltpu.roll(right, LANES - 1, 1)
    return middle + jnp.where(lane == 0, 0.0, up) + jnp.where(lane == period - 1, 0.0, down)


def prep_kernel(vol_ref, hist_ref, cells_ref, first_ref, second_ref, peak_ref):
    depth = vol_ref.shape[2]
    bound = bound_of(hist_ref, 0).astype(bf16)
    top = jnp.zeros(cells_ref.shape[2:], bf16)
    for z in range(depth):
        rows = jnp.transpose(vol_ref[0, :, z], (1, 0, 2))
        for y in range(rows.shape[0]):
            top = jnp.maximum(top, jnp.abs(rows[y]))
            cells_ref[z, y] = bounded(rows[y], bound)
    peak_ref[...] = jnp.broadcast_to(peak_of(top), (1, LANES))
    even = lax.axis_index("sz") % 2 == 0
    start_first = jnp.where(even, depth - HALO, 0)
    start_second = jnp.where(even, 0, depth - HALO)
    first_ref[...] = cells_ref[pl.ds(start_first, HALO)]
    second_ref[...] = cells_ref[pl.ds(start_second, HALO)]


def sides(axis, first, second):
    at = lax.axis_index(axis)
    count = lax.axis_size(axis)
    even = at % 2 == 0
    blank = jnp.zeros_like(first)
    below = jnp.where(at == 0, blank, jnp.where(even, second, first))
    above = jnp.where(at == count - 1, blank, jnp.where(even, first, second))
    return below, above


def deep_kernel(cells_ref, got_first_ref, got_second_ref, matrix_ref, first_ref, second_ref):
    depth, height = cells_ref.shape[:2]
    even = lax.axis_index("sy") % 2 == 0
    starts = (jnp.where(even, height - HALO, 0), jnp.where(even, 0, height - HALO))
    odd_z = lax.axis_index("sz") % 2
    far = HALO + depth
    for start, out_ref in zip(starts, (first_ref, second_ref)):
        rows = pl.ds(start, HALO)
        out_ref[pl.ds((1 - odd_z) * far, HALO)] = got_first_ref[:, rows]
        out_ref[pl.ds(odd_z * far, HALO)] = got_second_ref[:, rows]
        out_ref[HALO:far] = cells_ref[:, rows]


def conv_rows(cell, weight, z, rows, out_chan):
    window = jnp.concatenate(
        [
            jnp.concatenate([cell(z + dz, y + dy) for y in rows], axis=1)
            for dz in range(3)
            for dy in range(3)
        ],
        axis=0,
    )
    taps = jnp.dot(weight, window, preferred_element_type=f32)
    outs = []
    for half in range(2):
        part = taps[:, half * LANES : (half + 1) * LANES]
        outs.append(
            tap_sum(
                part[:out_chan], part[out_chan : 2 * out_chan], part[2 * out_chan :], LANES
            )
        )
    return outs


def first_inner_kernel(own_ref, got_first_ref, got_second_ref, weight_ref, deep_ref, raw_ref, sum_ref):
    depth, count, channels = raw_ref.shape[:3]
    own_depth = own_ref.shape[0]
    below, above = sides("sz", got_first_ref[...], got_second_ref[...])
    deep_ref[0:HALO] = below
    deep_ref[HALO : HALO + own_depth] = own_ref[...]
    deep_ref[HALO + own_depth :] = above
    weight = weight_ref[...]
    total = jnp.zeros((channels, LANES), f32)
    square = total
    for z in range(depth):
        for y in range(0, count, 2):
            outs = conv_rows(lambda z, y: deep_ref[z, y], weight, z, (y, y + 1), channels)
            for half in range(2):
                raw_ref[z, y + half] = outs[half]
                if 1 <= z < depth - 1:
                    total = total + outs[half]
                    square = square + outs[half] * outs[half]
    sum_ref[0] = total
    sum_ref[1] = square


def first_outer_kernel(
    deep_ref, got_first_ref, got_second_ref, weight_ref, peak_ref, sum_ref, raw_ref, row_ref, edge_ref
):
    depth, count, channels = raw_ref.shape[:3]
    planes, own_height = deep_ref.shape[:2]
    below, above = sides("sy", got_first_ref[...], got_second_ref[...])
    edge_ref[0] = below
    edge_ref[1] = above

    for at_end, end in (
        (lax.axis_index("sz") == 0, slice(0, HALO)),
        (lax.axis_index("sz") == lax.axis_size("sz") - 1, slice(planes - HALO, planes)),
    ):

        @pl.when(at_end)
        def _():
            edge_ref[:, end] = jnp.zeros((2, HALO) + edge_ref.shape[2:], bf16)

    def cell(z, y):
        if y < HALO:
            return edge_ref[0, z, y]
        if y < HALO + own_height:
            return deep_ref[z, y - HALO]
        return edge_ref[1, z, y - HALO - own_height]

    weight = weight_ref[...]
    total = sum_ref[0]
    square = sum_ref[1]
    last = own_height + 2 - 1
    for z in range(depth):
        for place, rows in ((0, (0, 1)), (2, (last - 1, last))):
            outs = conv_rows(cell, weight, z, rows, channels)
            for half in range(2):
                raw_ref[z, place + half] = outs[half]
                if 1 <= z < depth - 1 and 1 <= rows[half] < last:
                    total = total + outs[half]
                    square = square + outs[half] * outs[half]
    row = as_row(jnp.sum(total, axis=1, keepdims=True), 0)
    row = row + as_row(jnp.sum(square, axis=1, keepdims=True), channels)
    row = row + at_lane(peak_ref[...], PEAK_AT)
    row_ref[...] = jnp.broadcast_to(row[None], row_ref.shape)


def second_kernel(cell_count):
    def kernel(
        inner_ref,
        outer_ref,
        rows_ref,
        weight_ref,
        param_ref,
        gain_row_ref,
        out_ref,
        load_ref,
        hidden_ref,
        pool_ref,
        raw_ref,
        done,
    ):
        depth, height, channels, width = raw_ref.shape
        wide_depth, wide_height = hidden_ref.shape[:2]
        rows = rows_ref[...]
        merged = jnp.sum(rows, axis=0)
        peak_vol = jnp.max(rows, axis=0)
        scale, offset = affine(
            column(merged, channels, 0),
            column(merged, channels, channels),
            cell_count,
            lane_of(param_ref, 0, channels),
            lane_of(param_ref, 1, channels),
        )
        bound = clip_bound(param_ref, 1)
        at_z = lax.axis_index("sz")
        at_y = lax.axis_index("sy")
        last_z = lax.axis_size("sz") - 1
        last_y = lax.axis_size("sy") - 1
        peak = jnp.zeros((channels, width), bf16)
        for z in range(wide_depth):
            for y in range(wide_height):
                if y < HALO:
                    raw = outer_ref[z, y]
                elif y < height:
                    raw = inner_ref[z, y - HALO]
                else:
                    raw = outer_ref[z, y - height + HALO]
                hidden = activated(raw, scale, offset)
                if 1 <= y < wide_height - 1 and 1 <= z < wide_depth - 1:
                    peak = jnp.maximum(peak, jnp.abs(hidden))
                hidden_ref[z, y] = bounded(hidden, bound)
        outside = (
            (at_z == 0, (slice(0, 1), slice(0, wide_height))),
            (at_z == last_z, (slice(wide_depth - 1, wide_depth), slice(0, wide_height))),
            (at_y == 0, (slice(0, wide_depth), slice(0, 1))),
            (at_y == last_y, (slice(0, wide_depth), slice(wide_height - 1, wide_height))),
        )
        for at_end, (zs, ys) in outside:

            @pl.when(at_end)
            def _():
                count = (zs.stop - zs.start, ys.stop - ys.start)
                hidden_ref[zs, ys] = jnp.zeros(count + (channels, width), bf16)

        blank = jnp.zeros((channels, width), f32)
        weight = weight_ref[...]
        sign = jnp.where(lane_of(param_ref, 2, channels) >= 0, 1.0, -1.0).astype(f32)
        half_height = height // 2
        total, square, least, most = blank, blank, blank + 1e30, blank - 1e30
        copies = []
        for zp in range(depth // 2):
            for yp in range(half_height):
                best = None
                for dz in range(2):
                    z = 2 * zp + dz
                    outs = conv_rows(
                        lambda z, y: hidden_ref[z, y], weight, z, (2 * yp, 2 * yp + 1), channels
                    )
                    for half in range(2):
                        raw_ref[z, 2 * yp + half] = outs[half]
                        total = total + outs[half]
                        square = square + outs[half] * outs[half]
                        signed = outs[half] * sign
                        best = signed if best is None else jnp.maximum(best, signed)
                best = jnp.maximum(best, pltpu.roll(best, LANES - 1, 1)) * sign
                pool_ref[zp, yp] = best
                least = jnp.minimum(least, best)
                most = jnp.maximum(most, best)
            pair = slice(2 * zp, 2 * zp + 2)
            copies.append(pltpu.make_async_copy(raw_ref.at[pair], out_ref.at[pair], done.at[zp]))
            copies[-1].start()
        most, least = peak_of(most), -peak_of(-least)
        center = 0.5 * (most + least)
        reach = jnp.maximum(0.5 * (most - least), 1e-30)
        rate = CODE_SPAN / reach
        pick = jnp.where(
            lax.broadcasted_iota(jnp.int32, (2 * LANES, LANES), 0)
            == 2 * lax.broadcasted_iota(jnp.int32, (2 * LANES, LANES), 1),
            1.0,
            0.0,
        ).astype(bf16)
        for zp in range(depth // 2):
            for yq in range(half_height // 2):
                both = jnp.concatenate([pool_ref[zp, 2 * yq], pool_ref[zp, 2 * yq + 1]], axis=1)
                both = jnp.exp((both - center) * rate).astype(bf16)
                load_ref[
                    zp * channels : (zp + 1) * channels, yq * LANES : (yq + 1) * LANES
                ] = jnp.dot(both, pick, preferred_element_type=f32).astype(bf16)
        row = as_row(jnp.sum(total, axis=1, keepdims=True), 0)
        row = row + as_row(jnp.sum(square, axis=1, keepdims=True), channels)
        row = row + at_lane(peak_vol, PEAK_AT)
        row = row + at_lane(peak_of(peak), PEAK_AT + 1)
        row = row + at_lane(center, CODE_AT)
        row = row + at_lane(reach / CODE_SPAN, CODE_AT + 1)
        row = row + gain_row_ref[...]
        high = row.astype(bf16).astype(f32)
        middle = (row - high).astype(bf16).astype(f32)
        low = row - high - middle
        level = lax.broadcasted_iota(jnp.int32, (16, LANES), 0)
        parts = jnp.where(
            level == 0, high, jnp.where(level == 1, middle, jnp.where(level == 2, low, 0.0))
        )
        body = (depth // 2) * channels
        load_ref[body:, 0:LANES] = parts.astype(bf16)
        load_ref[body:, LANES:] = jnp.zeros((16, load_ref.shape[1] - LANES), bf16)
        for copy in copies:
            copy.wait()

    return kernel


def spread_rows(cells, store):
    count = cells.shape[1] // LANES
    parts = [cells[:, j * LANES : (j + 1) * LANES] for j in range(count)]
    turned = [pltpu.roll(part, LANES // 2, 1) for part in parts]
    lower = lax.broadcasted_iota(jnp.int32, parts[0].shape, 1) < LANES // 2
    blank = jnp.zeros_like(parts[0])
    for j in range(count):
        before = turned[j - 1] if j > 0 else blank
        after = turned[j + 1] if j + 1 < count else blank
        store(0, j, jnp.where(lower, before, turned[j]))
        store(1, j, parts[j])
        store(2, j, jnp.where(lower, turned[j], after))


def third_kernel(fine_cells, coarse_cells, load_rows, piece):
    def kernel(
        all_ref,
        param_ref,
        out_ref,
        peak_ref,
        affine_ref,
        pool_ref,
        cells_ref,
        raw_ref,
    ):
        y_groups = all_ref.shape[0]
        z_groups = lax.axis_size("sz")
        span = all_ref.shape[2]
        planes, chan_all, flat = raw_ref.shape
        channels = pool_ref.shape[1]
        chan_own = piece // 4
        row_len = LANES // 2
        body = load_rows - 16
        z_own = body // channels
        at_z = lax.axis_index("sz")
        totals = jnp.zeros((16, LANES), f32)
        tops = jnp.zeros((1, LANES), f32)
        rows = {}
        for s in range(y_groups):
            for k in range(z_groups):
                parts = all_ref[s, k * load_rows + body : (k + 1) * load_rows, 0:LANES].astype(f32)
                totals = totals + parts
                rows[s, k] = jnp.sum(parts, axis=0, keepdims=True)
                tops = jnp.maximum(tops, rows[s, k])
        merged = jnp.sum(totals, axis=0, keepdims=True)
        scale, offset = affine(
            column(merged, channels, 0),
            column(merged, channels, channels),
            fine_cells,
            lane_of(param_ref, 2, channels),
            lane_of(param_ref, 3, channels),
        )
        lanes = lax.broadcasted_iota(jnp.int32, (channels, LANES), 1)
        affine_ref[...] = jnp.where(lanes == 0, scale, jnp.where(lanes == 1, offset, 0.0))
        bound = clip_bound(param_ref, 2)
        peak_pool = jnp.zeros((channels, span), bf16)
        for s in range(y_groups):
            for k in range(z_groups):
                center = rows[s, k][:, CODE_AT : CODE_AT + 1]
                reach = rows[s, k][:, CODE_AT + 1 : CODE_AT + 2]
                rate = scale * reach
                start = scale * center + offset
                for zp in range(z_own):
                    at = k * load_rows + zp * channels
                    code = jnp.log(all_ref[s, at : at + channels, :].astype(f32))
                    value = activated(code, rate, start)
                    peak_pool = jnp.maximum(peak_pool, jnp.abs(value))
                    pool_ref[(at_z ^ k) * z_own + zp, :, s * span : (s + 1) * span] = bounded(
                        value, bound
                    )
        cells_ref[0] = jnp.zeros(cells_ref.shape[1:], bf16)
        cells_ref[planes + 1] = jnp.zeros(cells_ref.shape[1:], bf16)
        places = (0, channels, 3 * channels)
        edge = lax.broadcasted_iota(jnp.int32, (channels, LANES), 1) % row_len

        for z in range(planes):

            def store(dy, j, value):
                lanes = slice(j * LANES, (j + 1) * LANES)
                cells_ref[z + 1, places[dy] : places[dy] + channels, lanes] = value
                if dy == 2:
                    blank = jnp.zeros_like(value)
                    up = jnp.where(edge == 0, blank, pltpu.roll(value, 1, 1))
                    down = jnp.where(edge == row_len - 1, blank, pltpu.roll(value, LANES - 1, 1))
                    cells_ref[z + 1, 2 * channels : 3 * channels, lanes] = up
                    cells_ref[z + 1, 4 * channels :, lanes] = down

            spread_rows(pool_ref[z], store)

        weights = z_groups * load_rows
        main = 3 * chan_own
        near_weight = jnp.concatenate(
            [all_ref[s, weights : weights + main, :] for s in range(y_groups)], axis=0
        )
        far_weight = jnp.concatenate(
            [all_ref[s, weights + main :, 0 : 3 * channels] for s in range(y_groups)], axis=0
        )

        blank = jnp.zeros((chan_own, LANES), f32)
        totals = [blank for _ in range(y_groups)]
        squares = [blank for _ in range(y_groups)]
        for z in range(planes):
            for t in range(flat // span):
                lanes = slice(t * span, (t + 1) * span)
                window = []
                for dz in range(3):
                    window.append(cells_ref[z + dz, 0 : 2 * channels, lanes])
                    if dz < 2:
                        window.append(cells_ref[z + dz, 3 * channels : 4 * channels, lanes])
                window = jnp.concatenate(window, axis=0)
                taps = jnp.dot(near_weight, window, preferred_element_type=f32)
                rest = jnp.dot(
                    far_weight,
                    cells_ref[z + 2, 2 * channels :, lanes],
                    preferred_element_type=f32,
                )
                for s in range(y_groups):
                    for half in range(span // LANES):
                        at = s * main
                        lanes = slice(half * LANES, (half + 1) * LANES)
                        part = taps[at : at + main, lanes]
                        out = tap_sum(
                            part[:chan_own],
                            part[chan_own : 2 * chan_own]
                            + rest[s * chan_own : (s + 1) * chan_own, lanes],
                            part[2 * chan_own :],
                            row_len,
                        )
                        start = t * span + half * LANES
                        raw_ref[
                            z, s * chan_own : (s + 1) * chan_own, start : start + LANES
                        ] = out
                        totals[s] = totals[s] + out
                        squares[s] = squares[s] + out * out
        pairs = [
            affine(
                jnp.sum(totals[s], axis=1, keepdims=True),
                jnp.sum(squares[s], axis=1, keepdims=True),
                coarse_cells,
                column(rows[s, 0], chan_own, GAIN_AT),
                column(rows[s, 0], chan_own, SHIFT_AT),
            )
            for s in range(y_groups)
        ]
        scale = jnp.concatenate([one[0] for one in pairs], axis=0)
        offset = jnp.concatenate([one[1] for one in pairs], axis=0)
        bound = clip_bound(param_ref, 3)

        peak = jnp.zeros((chan_all, LANES), bf16)
        for z in range(planes):
            for j in range(flat // LANES):
                lanes = slice(j * LANES, (j + 1) * LANES)
                value = activated(raw_ref[z, :, lanes], scale, offset)
                peak = jnp.maximum(peak, jnp.abs(value))
                out_ref[z, :, lanes] = bounded(value, bound)
        row = at_lane(tops[:, PEAK_AT : PEAK_AT + 1], 0)
        row = row + at_lane(tops[:, PEAK_AT + 1 : PEAK_AT + 2], 1)
        row = row + at_lane(peak_of(peak_pool), 2)
        row = row + at_lane(peak_of(peak), 3)
        peak_ref[...] = row[:, : peak_ref.shape[1]]

    return kernel


def fourth_kernel(coarse_cells):
    def kernel(
        cells_ref,
        weight_ref,
        param_ref,
        affine_ref,
        raw_ref,
        out_ref,
        skip_ref,
        last_ref,
        fine_ref,
        narrow_ref,
        done,
    ):
        fetch = pltpu.make_async_copy(raw_ref, fine_ref, done.at[0])
        fetch.start()
        planes, chan_all, flat = cells_ref.shape
        chan_own, z_own = out_ref.shape[1:3]
        span = 2 * LANES
        row_len = LANES // 2
        count = flat // LANES
        weight = weight_ref[...]
        lower = lax.broadcasted_iota(jnp.int32, (chan_own, LANES), 1) < row_len
        blank = jnp.zeros((chan_own, LANES), f32)

        def plane(z, taps_of, sums):
            total, square = sums
            by_row = [[], [], []]
            for t in range(flat // span):
                taps = taps_of(z, slice(t * span, (t + 1) * span))
                for half in range(span // LANES):
                    part = taps[:, half * LANES : (half + 1) * LANES]
                    for dy in range(3):
                        three = [
                            part[(3 * dy + dx) * chan_own : (3 * dy + dx + 1) * chan_own]
                            for dx in range(3)
                        ]
                        by_row[dy].append(tap_sum(*three, row_len))
            turned = [[pltpu.roll(one, row_len, 1) for one in by_row[dy]] for dy in (0, 2)]
            for j in range(count):
                before = turned[0][j - 1] if j > 0 else blank
                after = turned[1][j + 1] if j + 1 < count else blank
                out = by_row[1][j] + jnp.where(lower, before, turned[0][j])
                out = out + jnp.where(lower, turned[1][j], after)
                last_ref[z, :, j * LANES : (j + 1) * LANES] = out
                total = total + out
                square = square + out * out
            return total, square

        def inner(z, lanes):
            window = jnp.concatenate([cells_ref[z + dz, :, lanes] for dz in (-1, 0, 1)], axis=0)
            return jnp.dot(weight, window, preferred_element_type=f32)

        def lowest(z, lanes):
            window = jnp.concatenate([cells_ref[z + dz, :, lanes] for dz in (0, 1)], axis=0)
            return jnp.dot(weight[:, chan_all:], window, preferred_element_type=f32)

        def highest(z, lanes):
            window = jnp.concatenate([cells_ref[z + dz, :, lanes] for dz in (-1, 0)], axis=0)
            return jnp.dot(weight[:, : 2 * chan_all], window, preferred_element_type=f32)

        sums = plane(0, lowest, (blank, blank))
        for z in range(1, planes // 2):
            sums = plane(z, inner, sums)
        fetch.wait()
        scale = affine_ref[:, 0:1]
        offset = affine_ref[:, 1:2]
        for z in range(fine_ref.shape[0]):
            act = jnp.stack(
                [activated(fine_ref[z, y], scale, offset) for y in range(fine_ref.shape[1])]
            )
            narrow_ref[:, z] = jnp.transpose(act, (1, 0, 2))
        send = pltpu.make_async_copy(narrow_ref, skip_ref.at[0], done.at[1])
        send.start()
        for z in range(planes // 2, planes - 1):
            sums = plane(z, inner, sums)
        total, square = plane(planes - 1, highest, sums)
        scale, offset = affine(
            jnp.sum(total, axis=1, keepdims=True),
            jnp.sum(square, axis=1, keepdims=True),
            coarse_cells,
            lane_of(param_ref, LAST_AT, chan_own),
            lane_of(param_ref, LAST_AT + 1, chan_own),
        )
        at_z = lax.axis_index("sz")
        own = [
            activated(last_ref[at_z * z_own + i], scale, offset).astype(f32) for i in range(z_own)
        ]
        for c in range(chan_own):
            out_ref[0, c] = jnp.concatenate([one[c : c + 1] for one in own], axis=0).astype(bf16)
        send.wait()

    return kernel


def shape(dims, dtype):
    return jax.ShapeDtypeStruct(dims, dtype)


def near_shape(dims, dtype):
    return pltpu.VMEM(dims, dtype)


def held(value):
    return pltpu.with_memory_space_constraint(value, pltpu.VMEM)


def per_device(
    volume,
    amax_history,
    conv_first,
    conv_second,
    conv_third,
    conv_fourth,
    gain_fine,
    shift_fine,
    gain_coarse,
    shift_coarse,
):
    channels, depth, height, width = volume.shape[1:]
    z_groups = lax.axis_size("sz")
    y_groups = lax.axis_size("sy")
    samples = lax.axis_size("sample")
    fine_cells = float(depth * z_groups * height * y_groups * width)
    coarse_cells = fine_cells / 8
    chan_own = conv_third.shape[1]
    chan_all = conv_fourth.shape[2]
    span = (height // 2) * (width // 2)
    planes = (depth // 2) * z_groups
    flat = span * y_groups
    group = z_groups * y_groups
    load_rows = (depth // 2) * channels + 16

    cells, first, second, peak = pl.pallas_call(
        prep_kernel,
        out_shape=(
            near_shape((depth, height, channels, width), bf16),
            near_shape((HALO, height, channels, width), bf16),
            near_shape((HALO, height, channels, width), bf16),
            near_shape((1, LANES), f32),
        ),
        name="prep",
    )(volume, amax_history)
    third_rows = 4 * chan_own
    m1, m2, m3, m4, params, gain_row = pl.pallas_call(
        matrix_kernel,
        out_shape=(
            near_shape((3 * channels, 9 * channels), bf16),
            near_shape((3 * channels, 9 * channels), bf16),
            near_shape((third_rows, 8 * channels), bf16),
            near_shape((9 * chan_own, 3 * chan_all), bf16),
            near_shape((channels, LANES), f32),
            near_shape((1, LANES), f32),
        ),
        name="matrices",
    )(
        held(peak),
        conv_first,
        conv_second,
        conv_third,
        conv_fourth,
        amax_history,
        gain_fine,
        shift_fine,
        gain_coarse,
        shift_coarse,
    )
    pair_first, pair_second = pairings("sz")
    z_first = lax.ppermute(first, "sz", pair_first)
    z_second = lax.ppermute(second, "sz", pair_second)
    deep_depth = depth + 2 * HALO
    anywhere = pl.BlockSpec(memory_space=pl.ANY)
    levels = amax_history.shape[0]
    first, second = pl.pallas_call(
        deep_kernel,
        out_shape=(
            near_shape((deep_depth, HALO, channels, width), bf16),
            near_shape((deep_depth, HALO, channels, width), bf16),
        ),
        name="deep",
    )(held(cells), held(z_first), held(z_second), held(m1))
    pair_first, pair_second = pairings("sy")
    y_first = lax.ppermute(first, "sy", pair_first)
    y_second = lax.ppermute(second, "sy", pair_second)
    deep, raw_inner, sums = pl.pallas_call(
        first_inner_kernel,
        out_shape=(
            near_shape((deep_depth, height, channels, width), bf16),
            near_shape((depth + 2, height - 2, channels, width), f32),
            near_shape((2, channels, LANES), f32),
        ),
        name="first_inner",
    )(*(held(x) for x in (cells, z_first, z_second, m1)))
    raw_outer, row = pl.pallas_call(
        first_outer_kernel,
        out_shape=(
            near_shape((depth + 2, 2 * HALO, channels, width), f32),
            near_shape((group, 1, LANES), f32),
        ),
        scratch_shapes=[pltpu.VMEM((2, deep_depth, HALO, channels, width), bf16)],
        name="first_outer",
    )(*(held(x) for x in (deep, y_first, y_second, m1, peak, sums)))
    rows = lax.all_to_all(row, ("sy", "sz"), 0, 0, tiled=True)
    raw_second, load = pl.pallas_call(
        second_kernel(fine_cells),
        out_shape=(
            shape((depth, height, channels, width), f32),
            near_shape((load_rows, span), bf16),
        ),
        out_specs=(anywhere, pl.BlockSpec(memory_space=pltpu.VMEM)),
        scratch_shapes=[
            pltpu.VMEM((depth + 2, height + 2, channels, width), bf16),
            pltpu.VMEM((depth // 2, height // 2, channels, width), f32),
            pltpu.VMEM((depth, height, channels, width), f32),
            pltpu.SemaphoreType.DMA((depth // 2,)),
        ],
        name="second",
    )(*(held(x) for x in (raw_inner, raw_outer, rows, m2, params, gain_row)))
    loads = [load]
    for k in range(1, z_groups):
        loads.append(lax.ppermute(load, "sz", [(i, i ^ k) for i in range(z_groups)]))
    loads.append(m3)
    gathered = lax.all_gather(jnp.concatenate(loads, axis=0), "sy", axis=0)
    hidden, peaks, fine_affine = pl.pallas_call(
        third_kernel(fine_cells, coarse_cells, load_rows, third_rows),
        out_shape=(
            near_shape((planes, chan_all, flat), bf16),
            near_shape((1, levels), f32),
            near_shape((channels, LANES), f32),
        ),
        scratch_shapes=[
            pltpu.VMEM((planes, channels, flat), bf16),
            pltpu.VMEM((planes + 2, 5 * channels, flat), bf16),
            pltpu.VMEM((planes, chan_all, flat), f32),
        ],
        name="third",
    )(held(gathered), held(params))
    if samples <= 4:
        others = [
            lax.ppermute(peaks, "sample", [(i, (i + k) % samples) for i in range(samples)])
            for k in range(1, samples)
        ]
    else:
        others = [lax.pmax(peaks, "sample")]
    near = pl.BlockSpec(memory_space=pltpu.VMEM)
    coarse, skip = pl.pallas_call(
        fourth_kernel(coarse_cells),
        out_shape=(
            shape((1, chan_own, depth // 2, flat), bf16),
            shape((1, channels, depth, height, width), bf16),
        ),
        in_specs=[near, near, near, near, anywhere],
        out_specs=(near, anywhere),
        scratch_shapes=[
            pltpu.VMEM((planes, chan_own, flat), f32),
            pltpu.VMEM((depth, height, channels, width), f32),
            pltpu.VMEM((channels, depth, height, width), bf16),
            pltpu.SemaphoreType.DMA((2,)),
        ],
        name="fourth",
    )(*(held(x) for x in (hidden, m4, params, fine_affine)), raw_second)
    for other in others:
        peaks = jnp.maximum(peaks, other)
    return skip, coarse, peaks.reshape(levels)


def solution(mesh):
    return jax.shard_map(
        per_device,
        mesh=mesh,
        in_specs=(
            P("sample", None, "sz", "sy", None),
            P(),
            P(),
            P(),
            P(None, "sy", None),
            P(None, "sy", None),
            P(),
            P(),
            P(None, "sy"),
            P(None, "sy"),
        ),
        out_specs=(P("sample", None, "sz", "sy", None), P("sample", "sy", "sz", None), P()),
        check_vma=False,
    )
```

```python
import jax
import jax.numpy as jnp
from jax import lax
from jax.experimental import pallas as pl
from jax.experimental.pallas import tpu as pltpu
from jax.sharding import PartitionSpec as P

norm_eps = 1e-05
leak_slope = 0.01
f32 = jnp.float32
bf16 = jnp.bfloat16
LANES = 128
HALO = 2
PEAK_AT = 64
CODE_AT = 66
GAIN_AT = 80
SHIFT_AT = 96
CODE_SPAN = 83.0
ROWS = 8


def pairings(axis):
    count = lax.axis_size(axis)
    first = [(i, i ^ 1) for i in range(count)]
    second = [(i, min(max(((i + 1) ^ 1) - 1, 0), count - 1)) for i in range(count)]
    return first, second


def column(row, channels, start):
    lanes = lax.broadcasted_iota(jnp.int32, (channels, row.shape[1]), 1)
    chans = lax.broadcasted_iota(jnp.int32, (channels, row.shape[1]), 0)
    return jnp.sum(jnp.where(lanes == chans + start, row, 0.0), axis=1, keepdims=True)


def as_row(col, start):
    channels = col.shape[0]
    lanes = lax.broadcasted_iota(jnp.int32, (channels, LANES), 1)
    chans = lax.broadcasted_iota(jnp.int32, (channels, LANES), 0)
    return jnp.sum(jnp.where(lanes == chans + start, col, 0.0), axis=0, keepdims=True)


def at_lane(value, lane):
    lanes = lax.broadcasted_iota(jnp.int32, (1, LANES), 1)
    return jnp.where(lanes == lane, value, 0.0)


def affine(total, square, cells, gains, offset):
    mean = total / cells
    spread = square / cells - mean * mean
    scale = lax.rsqrt(spread + norm_eps) * gains
    return scale, offset - mean * scale


def activated(values, scale, offset):
    normed = values * scale + offset
    return jnp.maximum(normed, leak_slope * normed).astype(bf16)


def peak_of(values):
    values = values.astype(f32)
    return jnp.max(jnp.max(values, axis=0, keepdims=True), axis=1, keepdims=True)


def bounded(values, bound):
    return jnp.minimum(jnp.maximum(values, -bound), bound)


BOUND_AT = 4
LAST_AT = 8


def bound_of(hist_ref, level):
    return jnp.max(hist_ref[level : level + 1, :], axis=1, keepdims=True)


def lane_of(param_ref, lane, channels):
    return param_ref[0:channels, lane : lane + 1]


def clip_bound(param_ref, level):
    return param_ref[0:1, BOUND_AT + level : BOUND_AT + level + 1].astype(bf16)


def matrix_of(weight, taps_ref, groups):
    out_chan = weight.shape[1]
    for dx in range(3):
        taps_ref[dx * out_chan : (dx + 1) * out_chan, :] = jnp.concatenate(
            [weight[3 * j + dx] for j in groups], axis=1
        )


def matrix_kernel(
    peak_ref,
    first_ref,
    second_ref,
    third_ref,
    fourth_ref,
    hist_ref,
    gain_ref,
    shift_ref,
    gain_coarse_ref,
    shift_coarse_ref,
    m1_ref,
    m2_ref,
    m3_ref,
    m4_ref,
    param_ref,
    gain_row_ref,
):
    taps = first_ref.shape[0]
    matrix_of(first_ref, m1_ref, range(taps // 3))
    matrix_of(second_ref, m2_ref, range(taps // 3))
    own = third_ref.shape[1]
    matrix_of(third_ref, m3_ref.at[0 : 3 * own], range(taps // 3 - 1))
    last = [third_ref[taps - 3 + dx] for dx in range(3)]
    rest = m3_ref.shape[1] - 3 * third_ref.shape[2]
    m3_ref[3 * own :, :] = jnp.concatenate(last + [jnp.zeros((own, rest), bf16)], axis=1)
    for dy in range(3):
        for dx in range(3):
            at = (3 * dy + dx) * own
            m4_ref[at : at + own, :] = jnp.concatenate(
                [fourth_ref[9 * dz + 3 * dy + dx] for dz in range(3)], axis=1
            )
    channels = param_ref.shape[0]
    lanes = lax.broadcasted_iota(jnp.int32, (channels, LANES), 1)
    params = jnp.zeros((channels, LANES), f32)
    columns = []
    for layer in range(2):
        columns.append((2 * layer, column(gain_ref[layer : layer + 1, :], channels, 0)))
        columns.append((2 * layer + 1, column(shift_ref[layer : layer + 1, :], channels, 0)))
    for level in range(hist_ref.shape[0]):
        columns.append((BOUND_AT + level, bound_of(hist_ref, level)))
    pad = jnp.zeros((channels - own, 1), f32)
    for place, ref in ((LAST_AT, gain_coarse_ref), (LAST_AT + 1, shift_coarse_ref)):
        columns.append((place, jnp.concatenate([column(ref[1:2, :], own, 0), pad], axis=0)))
    for lane, value in columns:
        params = jnp.where(lanes == lane, value, params)
    param_ref[...] = params
    gain_row_ref[...] = as_row(column(gain_coarse_ref[0:1, :], own, 0), GAIN_AT) + as_row(
        column(shift_coarse_ref[0:1, :], own, 0), SHIFT_AT
    )


def tap_sum(left, middle, right, period):
    lane = lax.broadcasted_iota(jnp.int32, middle.shape, 1) % period
    up = pltpu.roll(left, 1, 1)
    down = pltpu.roll(right, LANES - 1, 1)
    return middle + jnp.where(lane == 0, 0.0, up) + jnp.where(lane == period - 1, 0.0, down)


def prep_kernel(vol_ref, hist_ref, cells_ref, first_ref, second_ref, peak_ref):
    depth = vol_ref.shape[2]
    bound = bound_of(hist_ref, 0).astype(bf16)
    top = jnp.zeros(cells_ref.shape[2:], bf16)
    for z in range(depth):
        rows = jnp.transpose(vol_ref[0, :, z], (1, 0, 2))
        for y in range(rows.shape[0]):
            top = jnp.maximum(top, jnp.abs(rows[y]))
            cells_ref[z, y] = bounded(rows[y], bound)
    peak_ref[...] = jnp.broadcast_to(peak_of(top), (1, LANES))
    even = lax.axis_index("sz") % 2 == 0
    start_first = jnp.where(even, depth - HALO, 0)
    start_second = jnp.where(even, 0, depth - HALO)
    first_ref[...] = cells_ref[pl.ds(start_first, HALO)]
    second_ref[...] = cells_ref[pl.ds(start_second, HALO)]


def sides(axis, first, second):
    at = lax.axis_index(axis)
    count = lax.axis_size(axis)
    even = at % 2 == 0
    blank = jnp.zeros_like(first)
    below = jnp.where(at == 0, blank, jnp.where(even, second, first))
    above = jnp.where(at == count - 1, blank, jnp.where(even, first, second))
    return below, above


def deep_kernel(cells_ref, got_first_ref, got_second_ref, matrix_ref, first_ref, second_ref):
    depth, height = cells_ref.shape[:2]
    even = lax.axis_index("sy") % 2 == 0
    starts = (jnp.where(even, height - HALO, 0), jnp.where(even, 0, height - HALO))
    odd_z = lax.axis_index("sz") % 2
    far = HALO + depth
    for start, out_ref in zip(starts, (first_ref, second_ref)):
        rows = pl.ds(start, HALO)
        out_ref[pl.ds((1 - odd_z) * far, HALO)] = got_first_ref[:, rows]
        out_ref[pl.ds(odd_z * far, HALO)] = got_second_ref[:, rows]
        out_ref[HALO:far] = cells_ref[:, rows]


def conv_rows(cell, weight, z, rows, out_chan):
    window = jnp.concatenate(
        [
            jnp.concatenate([cell(z + dz, y + dy) for y in rows], axis=1)
            for dz in range(3)
            for dy in range(3)
        ],
        axis=0,
    )
    taps = jnp.dot(weight, window, preferred_element_type=f32)
    outs = []
    for half in range(2):
        part = taps[:, half * LANES : (half + 1) * LANES]
        outs.append(
            tap_sum(
                part[:out_chan], part[out_chan : 2 * out_chan], part[2 * out_chan :], LANES
            )
        )
    return outs


def first_inner_kernel(own_ref, got_first_ref, got_second_ref, weight_ref, deep_ref, raw_ref, sum_ref):
    depth, count, channels = raw_ref.shape[:3]
    own_depth = own_ref.shape[0]
    below, above = sides("sz", got_first_ref[...], got_second_ref[...])
    deep_ref[0:HALO] = below
    deep_ref[HALO : HALO + own_depth] = own_ref[...]
    deep_ref[HALO + own_depth :] = above
    weight = weight_ref[...]
    total = jnp.zeros((channels, LANES), f32)
    square = total
    for z in range(depth):
        for y in range(0, count, 2):
            outs = conv_rows(lambda z, y: deep_ref[z, y], weight, z, (y, y + 1), channels)
            for half in range(2):
                raw_ref[z, y + half] = outs[half]
                if 1 <= z < depth - 1:
                    total = total + outs[half]
                    square = square + outs[half] * outs[half]
    sum_ref[0] = total
    sum_ref[1] = square


def first_outer_kernel(
    deep_ref, got_first_ref, got_second_ref, weight_ref, peak_ref, sum_ref, raw_ref, row_ref, edge_ref
):
    depth, count, channels = raw_ref.shape[:3]
    planes, own_height = deep_ref.shape[:2]
    below, above = sides("sy", got_first_ref[...], got_second_ref[...])
    edge_ref[0] = below
    edge_ref[1] = above

    for at_end, end in (
        (lax.axis_index("sz") == 0, slice(0, HALO)),
        (lax.axis_index("sz") == lax.axis_size("sz") - 1, slice(planes - HALO, planes)),
    ):

        @pl.when(at_end)
        def _():
            edge_ref[:, end] = jnp.zeros((2, HALO) + edge_ref.shape[2:], bf16)

    def cell(z, y):
        if y < HALO:
            return edge_ref[0, z, y]
        if y < HALO + own_height:
            return deep_ref[z, y - HALO]
        return edge_ref[1, z, y - HALO - own_height]

    weight = weight_ref[...]
    total = sum_ref[0]
    square = sum_ref[1]
    last = own_height + 2 - 1
    for z in range(depth):
        for place, rows in ((0, (0, 1)), (2, (last - 1, last))):
            outs = conv_rows(cell, weight, z, rows, channels)
            for half in range(2):
                raw_ref[z, place + half] = outs[half]
                if 1 <= z < depth - 1 and 1 <= rows[half] < last:
                    total = total + outs[half]
                    square = square + outs[half] * outs[half]
    row = as_row(jnp.sum(total, axis=1, keepdims=True), 0)
    row = row + as_row(jnp.sum(square, axis=1, keepdims=True), channels)
    row = row + at_lane(peak_ref[...], PEAK_AT)
    row_ref[...] = jnp.broadcast_to(row[None], row_ref.shape)


def second_kernel(cell_count):
    def kernel(
        inner_ref,
        outer_ref,
        rows_ref,
        weight_ref,
        param_ref,
        gain_row_ref,
        out_ref,
        load_ref,
        hidden_ref,
        pool_ref,
        raw_ref,
        done,
    ):
        depth, height, channels, width = raw_ref.shape
        wide_depth, wide_height = hidden_ref.shape[:2]
        rows = rows_ref[...]
        merged = jnp.sum(rows, axis=0)
        peak_vol = jnp.max(rows, axis=0)
        scale, offset = affine(
            column(merged, channels, 0),
            column(merged, channels, channels),
            cell_count,
            lane_of(param_ref, 0, channels),
            lane_of(param_ref, 1, channels),
        )
        bound = clip_bound(param_ref, 1)
        at_z = lax.axis_index("sz")
        at_y = lax.axis_index("sy")
        last_z = lax.axis_size("sz") - 1
        last_y = lax.axis_size("sy") - 1
        peak = jnp.zeros((channels, width), bf16)
        for z in range(wide_depth):
            for y in range(wide_height):
                if y < HALO:
                    raw = outer_ref[z, y]
                elif y < height:
                    raw = inner_ref[z, y - HALO]
                else:
                    raw = outer_ref[z, y - height + HALO]
                hidden = activated(raw, scale, offset)
                if 1 <= y < wide_height - 1 and 1 <= z < wide_depth - 1:
                    peak = jnp.maximum(peak, jnp.abs(hidden))
                hidden_ref[z, y] = bounded(hidden, bound)
        outside = (
            (at_z == 0, (slice(0, 1), slice(0, wide_height))),
            (at_z == last_z, (slice(wide_depth - 1, wide_depth), slice(0, wide_height))),
            (at_y == 0, (slice(0, wide_depth), slice(0, 1))),
            (at_y == last_y, (slice(0, wide_depth), slice(wide_height - 1, wide_height))),
        )
        for at_end, (zs, ys) in outside:

            @pl.when(at_end)
            def _():
                count = (zs.stop - zs.start, ys.stop - ys.start)
                hidden_ref[zs, ys] = jnp.zeros(count + (channels, width), bf16)

        blank = jnp.zeros((channels, width), f32)
        weight = weight_ref[...]
        sign = jnp.where(lane_of(param_ref, 2, channels) >= 0, 1.0, -1.0).astype(f32)
        half_height = height // 2
        total, square, least, most = blank, blank, blank + 1e30, blank - 1e30
        copies = []
        for zp in range(depth // 2):
            for yp in range(half_height):
                best = None
                for dz in range(2):
                    z = 2 * zp + dz
                    outs = conv_rows(
                        lambda z, y: hidden_ref[z, y], weight, z, (2 * yp, 2 * yp + 1), channels
                    )
                    for half in range(2):
                        raw_ref[z, 2 * yp + half] = outs[half]
                        total = total + outs[half]
                        square = square + outs[half] * outs[half]
                        signed = outs[half] * sign
                        best = signed if best is None else jnp.maximum(best, signed)
                best = jnp.maximum(best, pltpu.roll(best, LANES - 1, 1)) * sign
                pool_ref[zp, yp] = best
                least = jnp.minimum(least, best)
                most = jnp.maximum(most, best)
                part = (slice(2 * zp, 2 * zp + 2), slice(2 * yp, 2 * yp + 2))
                copies.append(
                    pltpu.make_async_copy(
                        raw_ref.at[part], out_ref.at[part], done.at[zp * half_height + yp]
                    )
                )
                copies[-1].start()
        most, least = peak_of(most), -peak_of(-least)
        center = 0.5 * (most + least)
        reach = jnp.maximum(0.5 * (most - least), 1e-30)
        rate = CODE_SPAN / reach
        pick = jnp.where(
            lax.broadcasted_iota(jnp.int32, (2 * LANES, LANES), 0)
            == 2 * lax.broadcasted_iota(jnp.int32, (2 * LANES, LANES), 1),
            1.0,
            0.0,
        ).astype(bf16)
        for zp in range(depth // 2):
            for yq in range(half_height // 2):
                both = jnp.concatenate([pool_ref[zp, 2 * yq], pool_ref[zp, 2 * yq + 1]], axis=1)
                both = jnp.exp((both - center) * rate).astype(bf16)
                load_ref[
                    zp * channels : (zp + 1) * channels, yq * LANES : (yq + 1) * LANES
                ] = jnp.dot(both, pick, preferred_element_type=f32).astype(bf16)
        row = as_row(jnp.sum(total, axis=1, keepdims=True), 0)
        row = row + as_row(jnp.sum(square, axis=1, keepdims=True), channels)
        row = row + at_lane(peak_vol, PEAK_AT)
        row = row + at_lane(peak_of(peak), PEAK_AT + 1)
        row = row + at_lane(center, CODE_AT)
        row = row + at_lane(reach / CODE_SPAN, CODE_AT + 1)
        row = row + gain_row_ref[...]
        high = row.astype(bf16).astype(f32)
        middle = (row - high).astype(bf16).astype(f32)
        low = row - high - middle
        level = lax.broadcasted_iota(jnp.int32, (ROWS, LANES), 0)
        parts = jnp.where(
            level == 0, high, jnp.where(level == 1, middle, jnp.where(level == 2, low, 0.0))
        )
        body = (depth // 2) * channels
        load_ref[body:, 0:LANES] = parts.astype(bf16)
        load_ref[body:, LANES:] = jnp.zeros((ROWS, load_ref.shape[1] - LANES), bf16)
        for copy in copies:
            copy.wait()

    return kernel


def turned(cells):
    return pltpu.roll(cells, LANES // 2, 1)


def third_kernel(fine_cells, coarse_cells, load_rows, piece):
    def kernel(all_ref, param_ref, out_ref, peak_ref, affine_ref, cells_ref, raw_ref):
        y_groups = all_ref.shape[0]
        z_groups = lax.axis_size("sz")
        span = all_ref.shape[2]
        planes, chan_all, flat = raw_ref.shape
        channels = cells_ref.shape[1] // 3
        chan_own = piece // 4
        row_len = LANES // 2
        blocks = flat // LANES
        body = load_rows - ROWS
        z_own = body // channels
        at_z = lax.axis_index("sz")
        totals = jnp.zeros((ROWS, LANES), f32)
        tops = jnp.zeros((1, LANES), f32)
        rows = {}
        for s in range(y_groups):
            for k in range(z_groups):
                parts = all_ref[s, k * load_rows + body : (k + 1) * load_rows, 0:LANES].astype(f32)
                totals = totals + parts
                rows[s, k] = jnp.sum(parts, axis=0, keepdims=True)
                tops = jnp.maximum(tops, rows[s, k])
        merged = jnp.sum(totals, axis=0, keepdims=True)
        scale, offset = affine(
            column(merged, channels, 0),
            column(merged, channels, channels),
            fine_cells,
            lane_of(param_ref, 2, channels),
            lane_of(param_ref, 3, channels),
        )
        lanes = lax.broadcasted_iota(jnp.int32, (channels, LANES), 1)
        affine_ref[...] = jnp.where(lanes == 0, scale, jnp.where(lanes == 1, offset, 0.0))
        bound = clip_bound(param_ref, 2)
        lower = lanes < row_len
        edge = lanes % row_len
        blank = jnp.zeros((channels, LANES), bf16)
        middle = slice(channels, 2 * channels)

        def at_block(block):
            return slice(block * LANES, (block + 1) * LANES)

        def keep(place, block, value):
            cells_ref[place, middle, at_block(block)] = value
            if block >= 2:
                cells_ref[place, :channels, at_block(block)] = jnp.where(
                    edge == 0, blank, pltpu.roll(value, 1, 1)
                )
                cells_ref[place, 2 * channels :, at_block(block)] = jnp.where(
                    edge == row_len - 1, blank, pltpu.roll(value, LANES - 1, 1)
                )

        cells_ref[0] = jnp.zeros(cells_ref.shape[1:], bf16)
        cells_ref[planes + 1] = jnp.zeros(cells_ref.shape[1:], bf16)
        peak_pool = jnp.zeros((channels, span), bf16)
        half_groups = y_groups // 2
        for k in range(z_groups):
            for zp in range(z_own):
                place = (at_z ^ k) * z_own + zp + 1
                at = k * load_rows + zp * channels
                ends = []
                for s in range(half_groups):
                    both = []
                    for own in (s, s + half_groups):
                        center = rows[own, k][:, CODE_AT : CODE_AT + 1]
                        reach = rows[own, k][:, CODE_AT + 1 : CODE_AT + 2]
                        code = jnp.log(all_ref[own, at : at + channels, :].astype(f32))
                        value = activated(code, scale * reach, scale * center + offset)
                        peak_pool = jnp.maximum(peak_pool, jnp.abs(value))
                        both.append(bounded(value, bound))
                    for q in range(span // LANES):
                        low, high = (one[:, at_block(q)] for one in both)
                        block = s * (span // row_len) + 2 * q
                        one = jnp.where(lower, low, turned(high))
                        two = jnp.where(lower, turned(low), high)
                        keep(place, block + 1, one)
                        keep(place, block + 2, two)
                        if block == 0:
                            ends.append((blocks + 1, jnp.where(lower, turned(one), blank)))
                        if block + 2 == blocks:
                            ends.append((0, jnp.where(lower, blank, turned(two))))
                for block, value in ends:
                    keep(place, block, value)
        weights = z_groups * load_rows
        main = 3 * chan_own
        near_weight = jnp.concatenate(
            [all_ref[s, weights : weights + main, :] for s in range(y_groups)], axis=0
        )
        far_weight = jnp.concatenate(
            [all_ref[s, weights + main :, 0 : 3 * channels] for s in range(y_groups)], axis=0
        )
        blank = jnp.zeros((chan_own, LANES), f32)
        totals = [blank for _ in range(y_groups)]
        squares = [blank for _ in range(y_groups)]
        width = 2 * LANES
        for z in range(planes):
            for t in range(blocks // 2):
                window = [
                    cells_ref[z + dz, middle, (2 * t + dy) * LANES : (2 * t + dy) * LANES + width]
                    for dz in range(3)
                    for dy in range(3)
                    if dz + dy < 4
                ]
                taps = jnp.dot(
                    near_weight, jnp.concatenate(window, axis=0), preferred_element_type=f32
                )
                rest = jnp.dot(
                    far_weight,
                    cells_ref[z + 2, :, (2 * t + 2) * LANES : (2 * t + 2) * LANES + width],
                    preferred_element_type=f32,
                )
                for s in range(y_groups):
                    for half in range(2):
                        at = s * main
                        part = taps[at : at + main, at_block(half)]
                        out = tap_sum(
                            part[:chan_own],
                            part[chan_own : 2 * chan_own]
                            + rest[s * chan_own : (s + 1) * chan_own, at_block(half)],
                            part[2 * chan_own :],
                            row_len,
                        )
                        raw_ref[
                            z, s * chan_own : (s + 1) * chan_own, at_block(2 * t + half)
                        ] = out
                        totals[s] = totals[s] + out
                        squares[s] = squares[s] + out * out
        pairs = [
            affine(
                jnp.sum(totals[s], axis=1, keepdims=True),
                jnp.sum(squares[s], axis=1, keepdims=True),
                coarse_cells,
                column(rows[s, 0], chan_own, GAIN_AT),
                column(rows[s, 0], chan_own, SHIFT_AT),
            )
            for s in range(y_groups)
        ]
        scale = jnp.concatenate([one[0] for one in pairs], axis=0)
        offset = jnp.concatenate([one[1] for one in pairs], axis=0)
        bound = clip_bound(param_ref, 3)
        peak = jnp.zeros((chan_all, LANES), bf16)
        for z in range(planes):
            for j in range(blocks):
                value = activated(raw_ref[z, :, at_block(j)], scale, offset)
                peak = jnp.maximum(peak, jnp.abs(value))
                out_ref[z, :, at_block(j)] = bounded(value, bound)
        row = at_lane(tops[:, PEAK_AT : PEAK_AT + 1], 0)
        row = row + at_lane(tops[:, PEAK_AT + 1 : PEAK_AT + 2], 1)
        row = row + at_lane(peak_of(peak_pool), 2)
        row = row + at_lane(peak_of(peak), 3)
        peak_ref[...] = row[:, : peak_ref.shape[1]]

    return kernel


def fourth_kernel(coarse_cells):
    def kernel(
        cells_ref,
        weight_ref,
        param_ref,
        affine_ref,
        raw_ref,
        out_ref,
        skip_ref,
        last_ref,
        fine_ref,
        narrow_ref,
        done,
    ):
        fetch = pltpu.make_async_copy(raw_ref, fine_ref, done.at[0])
        fetch.start()
        planes, chan_all, flat = cells_ref.shape
        chan_own, z_own = out_ref.shape[1:3]
        row_len = LANES // 2
        blocks = flat // LANES
        weight = weight_ref[...]
        lower = lax.broadcasted_iota(jnp.int32, (chan_own, LANES), 1) < row_len
        blank = jnp.zeros((chan_own, LANES), f32)

        def at_block(block):
            return slice(block * LANES, (block + 1) * LANES)

        def plane(z, sums):
            total, square = sums
            depths = [dz for dz in range(3) if 0 <= z + dz - 1 < planes]
            columns = slice(depths[0] * chan_all, (depths[-1] + 1) * chan_all)
            parts = []
            for t in range(blocks // 2):
                window = jnp.concatenate(
                    [
                        cells_ref[z + dz - 1, :, 2 * t * LANES : 2 * (t + 1) * LANES]
                        for dz in depths
                    ],
                    axis=0,
                )
                taps = jnp.dot(weight[:, columns], window, preferred_element_type=f32)
                parts.extend(taps[:, at_block(half)] for half in range(2))

            def tap(dy, dx, j):
                at = (3 * dy + dx) * chan_own
                return parts[j][at : at + chan_own]

            for j in range(blocks):
                three = []
                for dx in range(3):
                    if j > 0:
                        before = tap(0, dx, j - 1)
                    else:
                        before = jnp.where(lower, blank, turned(tap(0, dx, blocks - 1)))
                    if j + 1 < blocks:
                        after = tap(2, dx, j + 1)
                    else:
                        after = jnp.where(lower, turned(tap(2, dx, 0)), blank)
                    three.append(tap(1, dx, j) + before + after)
                out = tap_sum(*three, row_len)
                last_ref[z, :, at_block(j)] = out
                total = total + out
                square = square + out * out
            return total, square

        sums = (blank, blank)
        for z in range(planes // 2):
            sums = plane(z, sums)
        fetch.wait()
        scale = affine_ref[:, 0:1]
        offset = affine_ref[:, 1:2]
        for z in range(fine_ref.shape[0]):
            act = jnp.stack(
                [activated(fine_ref[z, y], scale, offset) for y in range(fine_ref.shape[1])]
            )
            narrow_ref[:, z] = jnp.transpose(act, (1, 0, 2))
        send = pltpu.make_async_copy(narrow_ref, skip_ref.at[0], done.at[1])
        send.start()
        for z in range(planes // 2, planes):
            sums = plane(z, sums)
        total, square = sums
        scale, offset = affine(
            jnp.sum(total, axis=1, keepdims=True),
            jnp.sum(square, axis=1, keepdims=True),
            coarse_cells,
            lane_of(param_ref, LAST_AT, chan_own),
            lane_of(param_ref, LAST_AT + 1, chan_own),
        )
        at_z = lax.axis_index("sz")
        own = []
        for i in range(z_own):
            cells = activated(last_ref[at_z * z_own + i], scale, offset).astype(f32)
            natural = []
            for p in range(blocks):
                row = (2 * p) % blocks
                first, second = cells[:, at_block(row)], cells[:, at_block(row + 1)]
                if 2 * p < blocks:
                    natural.append(jnp.where(lower, first, turned(second)))
                else:
                    natural.append(jnp.where(lower, turned(first), second))
            own.append(jnp.concatenate(natural, axis=1))
        for c in range(chan_own):
            out_ref[0, c] = jnp.concatenate([one[c : c + 1] for one in own], axis=0).astype(bf16)
        send.wait()

    return kernel


def shape(dims, dtype):
    return jax.ShapeDtypeStruct(dims, dtype)


def near_shape(dims, dtype):
    return pltpu.VMEM(dims, dtype)


def held(value):
    return pltpu.with_memory_space_constraint(value, pltpu.VMEM)


def per_device(
    volume,
    amax_history,
    conv_first,
    conv_second,
    conv_third,
    conv_fourth,
    gain_fine,
    shift_fine,
    gain_coarse,
    shift_coarse,
):
    channels, depth, height, width = volume.shape[1:]
    z_groups = lax.axis_size("sz")
    y_groups = lax.axis_size("sy")
    samples = lax.axis_size("sample")
    fine_cells = float(depth * z_groups * height * y_groups * width)
    coarse_cells = fine_cells / 8
    chan_own = conv_third.shape[1]
    chan_all = conv_fourth.shape[2]
    span = (height // 2) * (width // 2)
    planes = (depth // 2) * z_groups
    flat = span * y_groups
    group = z_groups * y_groups
    load_rows = (depth // 2) * channels + ROWS

    cells, first, second, peak = pl.pallas_call(
        prep_kernel,
        out_shape=(
            near_shape((depth, height, channels, width), bf16),
            near_shape((HALO, height, channels, width), bf16),
            near_shape((HALO, height, channels, width), bf16),
            near_shape((1, LANES), f32),
        ),
        name="prep",
    )(volume, amax_history)
    third_rows = 4 * chan_own
    m1, m2, m3, m4, params, gain_row = pl.pallas_call(
        matrix_kernel,
        out_shape=(
            near_shape((3 * channels, 9 * channels), bf16),
            near_shape((3 * channels, 9 * channels), bf16),
            near_shape((third_rows, 8 * channels), bf16),
            near_shape((9 * chan_own, 3 * chan_all), bf16),
            near_shape((channels, LANES), f32),
            near_shape((1, LANES), f32),
        ),
        name="matrices",
    )(
        held(peak),
        conv_first,
        conv_second,
        conv_third,
        conv_fourth,
        amax_history,
        gain_fine,
        shift_fine,
        gain_coarse,
        shift_coarse,
    )
    pair_first, pair_second = pairings("sz")
    z_first = lax.ppermute(first, "sz", pair_first)
    z_second = lax.ppermute(second, "sz", pair_second)
    deep_depth = depth + 2 * HALO
    anywhere = pl.BlockSpec(memory_space=pl.ANY)
    levels = amax_history.shape[0]
    first, second = pl.pallas_call(
        deep_kernel,
        out_shape=(
            near_shape((deep_depth, HALO, channels, width), bf16),
            near_shape((deep_depth, HALO, channels, width), bf16),
        ),
        name="deep",
    )(held(cells), held(z_first), held(z_second), held(m1))
    pair_first, pair_second = pairings("sy")
    y_first = lax.ppermute(first, "sy", pair_first)
    y_second = lax.ppermute(second, "sy", pair_second)
    deep, raw_inner, sums = pl.pallas_call(
        first_inner_kernel,
        out_shape=(
            near_shape((deep_depth, height, channels, width), bf16),
            near_shape((depth + 2, height - 2, channels, width), f32),
            near_shape((2, channels, LANES), f32),
        ),
        name="first_inner",
    )(*(held(x) for x in (cells, z_first, z_second, m1)))
    raw_outer, row = pl.pallas_call(
        first_outer_kernel,
        out_shape=(
            near_shape((depth + 2, 2 * HALO, channels, width), f32),
            near_shape((group, 1, LANES), f32),
        ),
        scratch_shapes=[pltpu.VMEM((2, deep_depth, HALO, channels, width), bf16)],
        name="first_outer",
    )(*(held(x) for x in (deep, y_first, y_second, m1, peak, sums)))
    rows = lax.all_to_all(row, ("sy", "sz"), 0, 0, tiled=True)
    raw_second, load = pl.pallas_call(
        second_kernel(fine_cells),
        out_shape=(
            shape((depth, height, channels, width), f32),
            near_shape((load_rows, span), bf16),
        ),
        out_specs=(anywhere, pl.BlockSpec(memory_space=pltpu.VMEM)),
        scratch_shapes=[
            pltpu.VMEM((depth + 2, height + 2, channels, width), bf16),
            pltpu.VMEM((depth // 2, height // 2, channels, width), f32),
            pltpu.VMEM((depth, height, channels, width), f32),
            pltpu.SemaphoreType.DMA(((depth // 2) * (height // 2),)),
        ],
        name="second",
    )(*(held(x) for x in (raw_inner, raw_outer, rows, m2, params, gain_row)))
    loads = [load]
    for k in range(1, z_groups):
        loads.append(lax.ppermute(load, "sz", [(i, i ^ k) for i in range(z_groups)]))
    loads.append(m3)
    gathered = lax.all_gather(jnp.concatenate(loads, axis=0), "sy", axis=0)
    hidden, peaks, fine_affine = pl.pallas_call(
        third_kernel(fine_cells, coarse_cells, load_rows, third_rows),
        out_shape=(
            near_shape((planes, chan_all, flat), bf16),
            near_shape((1, levels), f32),
            near_shape((channels, LANES), f32),
        ),
        scratch_shapes=[
            pltpu.VMEM((planes + 2, 3 * channels, flat + 2 * LANES), bf16),
            pltpu.VMEM((planes, chan_all, flat), f32),
        ],
        name="third",
    )(held(gathered), held(params))
    if samples <= 4:
        others = [
            lax.ppermute(peaks, "sample", [(i, (i + k) % samples) for i in range(samples)])
            for k in range(1, samples)
        ]
    else:
        others = [lax.pmax(peaks, "sample")]
    near = pl.BlockSpec(memory_space=pltpu.VMEM)
    coarse, skip = pl.pallas_call(
        fourth_kernel(coarse_cells),
        out_shape=(
            shape((1, chan_own, depth // 2, flat), bf16),
            shape((1, channels, depth, height, width), bf16),
        ),
        in_specs=[near, near, near, near, anywhere],
        out_specs=(near, anywhere),
        scratch_shapes=[
            pltpu.VMEM((planes, chan_own, flat), f32),
            pltpu.VMEM((depth, height, channels, width), f32),
            pltpu.VMEM((channels, depth, height, width), bf16),
            pltpu.SemaphoreType.DMA((2,)),
        ],
        name="fourth",
    )(*(held(x) for x in (hidden, m4, params, fine_affine)), raw_second)
    for other in others:
        peaks = jnp.maximum(peaks, other)
    return skip, coarse, peaks.reshape(levels)


def solution(mesh):
    return jax.shard_map(
        per_device,
        mesh=mesh,
        in_specs=(
            P("sample", None, "sz", "sy", None),
            P(),
            P(),
            P(),
            P(None, "sy", None),
            P(None, "sy", None),
            P(),
            P(),
            P(None, "sy"),
            P(None, "sy"),
        ),
        out_specs=(P("sample", None, "sz", "sy", None), P("sample", "sy", "sz", None), P()),
        check_vma=False,
    )
```

```python
import jax
import jax.numpy as jnp
from jax import lax
from jax.experimental import pallas as pl
from jax.experimental.pallas import tpu as pltpu
from jax.sharding import PartitionSpec as P

norm_eps = 1e-05
leak_slope = 0.01
f32 = jnp.float32
bf16 = jnp.bfloat16
LANES = 128
HALO = 2
KERNEL_BYTES = 24 * 1024 * 1024
PEAK_AT = 64
CODE_AT = 66
GAIN_AT = 80
SHIFT_AT = 96
CODE_SPAN = 83.0
ROWS = 8


def pairings(axis):
    count = lax.axis_size(axis)
    first = [(i, i ^ 1) for i in range(count)]
    second = [(i, min(max(((i + 1) ^ 1) - 1, 0), count - 1)) for i in range(count)]
    return first, second


def column(row, channels, start):
    lanes = lax.broadcasted_iota(jnp.int32, (channels, row.shape[1]), 1)
    chans = lax.broadcasted_iota(jnp.int32, (channels, row.shape[1]), 0)
    return jnp.sum(jnp.where(lanes == chans + start, row, 0.0), axis=1, keepdims=True)


def as_row(col, start):
    channels = col.shape[0]
    lanes = lax.broadcasted_iota(jnp.int32, (channels, LANES), 1)
    chans = lax.broadcasted_iota(jnp.int32, (channels, LANES), 0)
    return jnp.sum(jnp.where(lanes == chans + start, col, 0.0), axis=0, keepdims=True)


def at_lane(value, lane):
    lanes = lax.broadcasted_iota(jnp.int32, (1, LANES), 1)
    return jnp.where(lanes == lane, value, 0.0)


def affine(total, square, cells, gains, offset):
    mean = total / cells
    spread = square / cells - mean * mean
    scale = lax.rsqrt(spread + norm_eps) * gains
    return scale, offset - mean * scale


def activated(values, scale, offset):
    normed = values * scale + offset
    return jnp.maximum(normed, leak_slope * normed).astype(bf16)


def peak_of(values):
    values = values.astype(f32)
    return jnp.max(jnp.max(values, axis=0, keepdims=True), axis=1, keepdims=True)


def bounded(values, bound):
    return jnp.minimum(jnp.maximum(values, -bound), bound)


BOUND_AT = 4
LAST_AT = 8


def bound_of(hist_ref, level):
    return jnp.max(hist_ref[level : level + 1, :], axis=1, keepdims=True)


def lane_of(param_ref, lane, channels):
    return param_ref[0:channels, lane : lane + 1]


def clip_bound(param_ref, level):
    return param_ref[0:1, BOUND_AT + level : BOUND_AT + level + 1].astype(bf16)


def matrix_of(weight, taps_ref, groups):
    out_chan = weight.shape[1]
    for dx in range(3):
        taps_ref[dx * out_chan : (dx + 1) * out_chan, :] = jnp.concatenate(
            [weight[3 * j + dx] for j in groups], axis=1
        )


def matrix_kernel(
    peak_ref,
    first_ref,
    second_ref,
    third_ref,
    fourth_ref,
    hist_ref,
    gain_ref,
    shift_ref,
    gain_coarse_ref,
    shift_coarse_ref,
    m1_ref,
    m2_ref,
    m3_ref,
    m4_ref,
    param_ref,
    gain_row_ref,
):
    taps = first_ref.shape[0]
    matrix_of(first_ref, m1_ref, range(taps // 3))
    matrix_of(second_ref, m2_ref, range(taps // 3))
    own = third_ref.shape[1]
    matrix_of(third_ref, m3_ref.at[0 : 3 * own], range(taps // 3 - 1))
    last = [third_ref[taps - 3 + dx] for dx in range(3)]
    rest = m3_ref.shape[1] - 3 * third_ref.shape[2]
    m3_ref[3 * own :, :] = jnp.concatenate(last + [jnp.zeros((own, rest), bf16)], axis=1)
    for dy in range(3):
        for dx in range(3):
            at = (3 * dy + dx) * own
            m4_ref[at : at + own, :] = jnp.concatenate(
                [fourth_ref[9 * dz + 3 * dy + dx] for dz in range(3)], axis=1
            )
    channels = param_ref.shape[0]
    lanes = lax.broadcasted_iota(jnp.int32, (channels, LANES), 1)
    params = jnp.zeros((channels, LANES), f32)
    columns = []
    for layer in range(2):
        columns.append((2 * layer, column(gain_ref[layer : layer + 1, :], channels, 0)))
        columns.append((2 * layer + 1, column(shift_ref[layer : layer + 1, :], channels, 0)))
    for level in range(hist_ref.shape[0]):
        columns.append((BOUND_AT + level, bound_of(hist_ref, level)))
    pad = jnp.zeros((channels - own, 1), f32)
    for place, ref in ((LAST_AT, gain_coarse_ref), (LAST_AT + 1, shift_coarse_ref)):
        columns.append((place, jnp.concatenate([column(ref[1:2, :], own, 0), pad], axis=0)))
    for lane, value in columns:
        params = jnp.where(lanes == lane, value, params)
    param_ref[...] = params
    gain_row_ref[...] = as_row(column(gain_coarse_ref[0:1, :], own, 0), GAIN_AT) + as_row(
        column(shift_coarse_ref[0:1, :], own, 0), SHIFT_AT
    )


def tap_sum(left, middle, right, period):
    lane = lax.broadcasted_iota(jnp.int32, middle.shape, 1) % period
    up = pltpu.roll(left, 1, 1)
    down = pltpu.roll(right, LANES - 1, 1)
    return middle + jnp.where(lane == 0, 0.0, up) + jnp.where(lane == period - 1, 0.0, down)


def prep_kernel(vol_ref, hist_ref, cells_ref, first_ref, second_ref, peak_ref):
    depth = vol_ref.shape[2]
    bound = bound_of(hist_ref, 0).astype(bf16)
    top = jnp.zeros(cells_ref.shape[2:], bf16)
    for z in range(depth):
        rows = jnp.transpose(vol_ref[0, :, z], (1, 0, 2))
        for y in range(rows.shape[0]):
            top = jnp.maximum(top, jnp.abs(rows[y]))
            cells_ref[z, y] = bounded(rows[y], bound)
    peak_ref[...] = jnp.broadcast_to(peak_of(top), (1, LANES))
    even = lax.axis_index("sz") % 2 == 0
    start_first = jnp.where(even, depth - HALO, 0)
    start_second = jnp.where(even, 0, depth - HALO)
    first_ref[...] = cells_ref[pl.ds(start_first, HALO)]
    second_ref[...] = cells_ref[pl.ds(start_second, HALO)]


def sides(axis, first, second):
    at = lax.axis_index(axis)
    count = lax.axis_size(axis)
    even = at % 2 == 0
    blank = jnp.zeros_like(first)
    below = jnp.where(at == 0, blank, jnp.where(even, second, first))
    above = jnp.where(at == count - 1, blank, jnp.where(even, first, second))
    return below, above


def deep_kernel(cells_ref, got_first_ref, got_second_ref, matrix_ref, first_ref, second_ref):
    depth, height = cells_ref.shape[:2]
    even = lax.axis_index("sy") % 2 == 0
    starts = (jnp.where(even, height - HALO, 0), jnp.where(even, 0, height - HALO))
    odd_z = lax.axis_index("sz") % 2
    far = HALO + depth
    for start, out_ref in zip(starts, (first_ref, second_ref)):
        rows = pl.ds(start, HALO)
        out_ref[pl.ds((1 - odd_z) * far, HALO)] = got_first_ref[:, rows]
        out_ref[pl.ds(odd_z * far, HALO)] = got_second_ref[:, rows]
        out_ref[HALO:far] = cells_ref[:, rows]


def conv_rows(cell, weight, z, rows, out_chan):
    window = jnp.concatenate(
        [
            jnp.concatenate([cell(z + dz, y + dy) for y in rows], axis=1)
            for dz in range(3)
            for dy in range(3)
        ],
        axis=0,
    )
    taps = jnp.dot(weight, window, preferred_element_type=f32)
    outs = []
    for half in range(2):
        part = taps[:, half * LANES : (half + 1) * LANES]
        outs.append(
            tap_sum(
                part[:out_chan], part[out_chan : 2 * out_chan], part[2 * out_chan :], LANES
            )
        )
    return outs


def first_inner_kernel(own_ref, got_first_ref, got_second_ref, weight_ref, deep_ref, raw_ref, sum_ref):
    depth, count, channels = raw_ref.shape[:3]
    own_depth = own_ref.shape[0]
    below, above = sides("sz", got_first_ref[...], got_second_ref[...])
    deep_ref[0:HALO] = below
    deep_ref[HALO : HALO + own_depth] = own_ref[...]
    deep_ref[HALO + own_depth :] = above
    weight = weight_ref[...]
    total = jnp.zeros((channels, LANES), f32)
    square = total
    for z in range(depth):
        for y in range(0, count, 2):
            outs = conv_rows(lambda z, y: deep_ref[z, y], weight, z, (y, y + 1), channels)
            for half in range(2):
                raw_ref[z, y + half] = outs[half]
                if 1 <= z < depth - 1:
                    total = total + outs[half]
                    square = square + outs[half] * outs[half]
    sum_ref[0] = total
    sum_ref[1] = square


def first_outer_kernel(
    deep_ref, got_first_ref, got_second_ref, weight_ref, peak_ref, sum_ref, raw_ref, row_ref, edge_ref
):
    depth, count, channels = raw_ref.shape[:3]
    planes, own_height = deep_ref.shape[:2]
    below, above = sides("sy", got_first_ref[...], got_second_ref[...])
    edge_ref[0] = below
    edge_ref[1] = above

    for at_end, end in (
        (lax.axis_index("sz") == 0, slice(0, HALO)),
        (lax.axis_index("sz") == lax.axis_size("sz") - 1, slice(planes - HALO, planes)),
    ):

        @pl.when(at_end)
        def _():
            edge_ref[:, end] = jnp.zeros((2, HALO) + edge_ref.shape[2:], bf16)

    def cell(z, y):
        if y < HALO:
            return edge_ref[0, z, y]
        if y < HALO + own_height:
            return deep_ref[z, y - HALO]
        return edge_ref[1, z, y - HALO - own_height]

    weight = weight_ref[...]
    total = sum_ref[0]
    square = sum_ref[1]
    last = own_height + 2 - 1
    for z in range(depth):
        for place, rows in ((0, (0, 1)), (2, (last - 1, last))):
            outs = conv_rows(cell, weight, z, rows, channels)
            for half in range(2):
                raw_ref[z, place + half] = outs[half]
                if 1 <= z < depth - 1 and 1 <= rows[half] < last:
                    total = total + outs[half]
                    square = square + outs[half] * outs[half]
    row = as_row(jnp.sum(total, axis=1, keepdims=True), 0)
    row = row + as_row(jnp.sum(square, axis=1, keepdims=True), channels)
    row = row + at_lane(peak_ref[...], PEAK_AT)
    row_ref[...] = jnp.broadcast_to(row[None], row_ref.shape)


def second_kernel(cell_count):
    def kernel(
        inner_ref,
        outer_ref,
        rows_ref,
        weight_ref,
        param_ref,
        gain_row_ref,
        raw_ref,
        load_ref,
        hidden_ref,
        pool_ref,
    ):
        depth, height, channels, width = raw_ref.shape
        wide_depth, wide_height = hidden_ref.shape[:2]
        rows = rows_ref[...]
        merged = jnp.sum(rows, axis=0)
        peak_vol = jnp.max(rows, axis=0)
        scale, offset = affine(
            column(merged, channels, 0),
            column(merged, channels, channels),
            cell_count,
            lane_of(param_ref, 0, channels),
            lane_of(param_ref, 1, channels),
        )
        bound = clip_bound(param_ref, 1)
        at_z = lax.axis_index("sz")
        at_y = lax.axis_index("sy")
        last_z = lax.axis_size("sz") - 1
        last_y = lax.axis_size("sy") - 1
        peak = jnp.zeros((channels, width), bf16)
        for z in range(wide_depth):
            for y in range(wide_height):
                if y < HALO:
                    raw = outer_ref[z, y]
                elif y < height:
                    raw = inner_ref[z, y - HALO]
                else:
                    raw = outer_ref[z, y - height + HALO]
                hidden = activated(raw, scale, offset)
                if 1 <= y < wide_height - 1 and 1 <= z < wide_depth - 1:
                    peak = jnp.maximum(peak, jnp.abs(hidden))
                hidden_ref[z, y] = bounded(hidden, bound)
        outside = (
            (at_z == 0, (slice(0, 1), slice(0, wide_height))),
            (at_z == last_z, (slice(wide_depth - 1, wide_depth), slice(0, wide_height))),
            (at_y == 0, (slice(0, wide_depth), slice(0, 1))),
            (at_y == last_y, (slice(0, wide_depth), slice(wide_height - 1, wide_height))),
        )
        for at_end, (zs, ys) in outside:

            @pl.when(at_end)
            def _():
                count = (zs.stop - zs.start, ys.stop - ys.start)
                hidden_ref[zs, ys] = jnp.zeros(count + (channels, width), bf16)

        blank = jnp.zeros((channels, width), f32)
        weight = weight_ref[...]
        sign = jnp.where(lane_of(param_ref, 2, channels) >= 0, 1.0, -1.0).astype(f32)
        half_height = height // 2
        total, square, least, most = blank, blank, blank + 1e30, blank - 1e30
        for zp in range(depth // 2):
            for yp in range(half_height):
                best = None
                for dz in range(2):
                    z = 2 * zp + dz
                    outs = conv_rows(
                        lambda z, y: hidden_ref[z, y], weight, z, (2 * yp, 2 * yp + 1), channels
                    )
                    for half in range(2):
                        raw_ref[z, 2 * yp + half] = outs[half]
                        total = total + outs[half]
                        square = square + outs[half] * outs[half]
                        signed = outs[half] * sign
                        best = signed if best is None else jnp.maximum(best, signed)
                best = jnp.maximum(best, pltpu.roll(best, LANES - 1, 1)) * sign
                pool_ref[zp, yp] = best
                least = jnp.minimum(least, best)
                most = jnp.maximum(most, best)
        most, least = peak_of(most), -peak_of(-least)
        center = 0.5 * (most + least)
        reach = jnp.maximum(0.5 * (most - least), 1e-30)
        rate = CODE_SPAN / reach
        pick = jnp.where(
            lax.broadcasted_iota(jnp.int32, (2 * LANES, LANES), 0)
            == 2 * lax.broadcasted_iota(jnp.int32, (2 * LANES, LANES), 1),
            1.0,
            0.0,
        ).astype(bf16)
        for zp in range(depth // 2):
            for yq in range(half_height // 2):
                both = jnp.concatenate([pool_ref[zp, 2 * yq], pool_ref[zp, 2 * yq + 1]], axis=1)
                both = jnp.exp((both - center) * rate).astype(bf16)
                load_ref[
                    zp * channels : (zp + 1) * channels, yq * LANES : (yq + 1) * LANES
                ] = jnp.dot(both, pick, preferred_element_type=f32).astype(bf16)
        row = as_row(jnp.sum(total, axis=1, keepdims=True), 0)
        row = row + as_row(jnp.sum(square, axis=1, keepdims=True), channels)
        row = row + at_lane(peak_vol, PEAK_AT)
        row = row + at_lane(peak_of(peak), PEAK_AT + 1)
        row = row + at_lane(center, CODE_AT)
        row = row + at_lane(reach / CODE_SPAN, CODE_AT + 1)
        row = row + gain_row_ref[...]
        high = row.astype(bf16).astype(f32)
        middle = (row - high).astype(bf16).astype(f32)
        low = row - high - middle
        level = lax.broadcasted_iota(jnp.int32, (ROWS, LANES), 0)
        parts = jnp.where(
            level == 0, high, jnp.where(level == 1, middle, jnp.where(level == 2, low, 0.0))
        )
        body = (depth // 2) * channels
        load_ref[body:, 0:LANES] = parts.astype(bf16)
        load_ref[body:, LANES:] = jnp.zeros((ROWS, load_ref.shape[1] - LANES), bf16)

    return kernel


def turned(cells):
    return pltpu.roll(cells, LANES // 2, 1)


def third_kernel(fine_cells, coarse_cells, load_rows, piece):
    def kernel(all_ref, param_ref, raw_ref, peak_ref, affine_ref, next_ref, cells_ref):
        y_groups = all_ref.shape[0]
        z_groups = lax.axis_size("sz")
        span = all_ref.shape[2]
        planes, chan_all, flat = raw_ref.shape
        channels = cells_ref.shape[1] // 3
        chan_own = piece // 4
        row_len = LANES // 2
        blocks = flat // LANES
        body = load_rows - ROWS
        z_own = body // channels
        at_z = lax.axis_index("sz")
        totals = jnp.zeros((ROWS, LANES), f32)
        tops = jnp.zeros((1, LANES), f32)
        rows = {}
        for s in range(y_groups):
            for k in range(z_groups):
                parts = all_ref[s, k * load_rows + body : (k + 1) * load_rows, 0:LANES].astype(f32)
                totals = totals + parts
                rows[s, k] = jnp.sum(parts, axis=0, keepdims=True)
                tops = jnp.maximum(tops, rows[s, k])
        merged = jnp.sum(totals, axis=0, keepdims=True)
        scale, offset = affine(
            column(merged, channels, 0),
            column(merged, channels, channels),
            fine_cells,
            lane_of(param_ref, 2, channels),
            lane_of(param_ref, 3, channels),
        )
        lanes = lax.broadcasted_iota(jnp.int32, (channels, LANES), 1)
        affine_ref[...] = jnp.where(lanes == 0, scale, jnp.where(lanes == 1, offset, 0.0))
        bound = clip_bound(param_ref, 2)
        lower = lanes < row_len
        edge = lanes % row_len
        blank = jnp.zeros((channels, LANES), bf16)
        middle = slice(channels, 2 * channels)

        def at_block(block):
            return slice(block * LANES, (block + 1) * LANES)

        def keep(place, block, value):
            cells_ref[place, middle, at_block(block)] = value
            if block >= 2:
                cells_ref[place, :channels, at_block(block)] = jnp.where(
                    edge == 0, blank, pltpu.roll(value, 1, 1)
                )
                cells_ref[place, 2 * channels :, at_block(block)] = jnp.where(
                    edge == row_len - 1, blank, pltpu.roll(value, LANES - 1, 1)
                )

        cells_ref[0] = jnp.zeros(cells_ref.shape[1:], bf16)
        cells_ref[planes + 1] = jnp.zeros(cells_ref.shape[1:], bf16)
        peak_pool = jnp.zeros((channels, span), bf16)
        half_groups = y_groups // 2
        for k in range(z_groups):
            for zp in range(z_own):
                place = (at_z ^ k) * z_own + zp + 1
                at = k * load_rows + zp * channels
                ends = []
                for s in range(half_groups):
                    both = []
                    for own in (s, s + half_groups):
                        center = rows[own, k][:, CODE_AT : CODE_AT + 1]
                        reach = rows[own, k][:, CODE_AT + 1 : CODE_AT + 2]
                        code = jnp.log(all_ref[own, at : at + channels, :].astype(f32))
                        value = activated(code, scale * reach, scale * center + offset)
                        peak_pool = jnp.maximum(peak_pool, jnp.abs(value))
                        both.append(bounded(value, bound))
                    for q in range(span // LANES):
                        low, high = (one[:, at_block(q)] for one in both)
                        block = s * (span // row_len) + 2 * q
                        one = jnp.where(lower, low, turned(high))
                        two = jnp.where(lower, turned(low), high)
                        keep(place, block + 1, one)
                        keep(place, block + 2, two)
                        if block == 0:
                            ends.append((blocks + 1, jnp.where(lower, turned(one), blank)))
                        if block + 2 == blocks:
                            ends.append((0, jnp.where(lower, blank, turned(two))))
                for block, value in ends:
                    keep(place, block, value)
        weights = z_groups * load_rows
        main = 3 * chan_own
        near_weight = jnp.concatenate(
            [all_ref[s, weights : weights + main, :] for s in range(y_groups)], axis=0
        )
        far_weight = jnp.concatenate(
            [all_ref[s, weights + main :, 0 : 3 * channels] for s in range(y_groups)], axis=0
        )
        blank = jnp.zeros((chan_own, LANES), f32)
        totals = [blank for _ in range(y_groups)]
        squares = [blank for _ in range(y_groups)]
        leasts = [blank + 1e30 for _ in range(y_groups)]
        mosts = [blank - 1e30 for _ in range(y_groups)]
        width = 2 * LANES
        for z in range(planes):
            for t in range(blocks // 2):
                window = [
                    cells_ref[z + dz, middle, (2 * t + dy) * LANES : (2 * t + dy) * LANES + width]
                    for dz in range(3)
                    for dy in range(3)
                    if dz + dy < 4
                ]
                taps = jnp.dot(
                    near_weight, jnp.concatenate(window, axis=0), preferred_element_type=f32
                )
                rest = jnp.dot(
                    far_weight,
                    cells_ref[z + 2, :, (2 * t + 2) * LANES : (2 * t + 2) * LANES + width],
                    preferred_element_type=f32,
                )
                for s in range(y_groups):
                    for half in range(2):
                        at = s * main
                        part = taps[at : at + main, at_block(half)]
                        out = tap_sum(
                            part[:chan_own],
                            part[chan_own : 2 * chan_own]
                            + rest[s * chan_own : (s + 1) * chan_own, at_block(half)],
                            part[2 * chan_own :],
                            row_len,
                        )
                        raw_ref[
                            z, s * chan_own : (s + 1) * chan_own, at_block(2 * t + half)
                        ] = out
                        totals[s] = totals[s] + out
                        squares[s] = squares[s] + out * out
                        leasts[s] = jnp.minimum(leasts[s], out)
                        mosts[s] = jnp.maximum(mosts[s], out)
        pairs = [
            affine(
                jnp.sum(totals[s], axis=1, keepdims=True),
                jnp.sum(squares[s], axis=1, keepdims=True),
                coarse_cells,
                column(rows[s, 0], chan_own, GAIN_AT),
                column(rows[s, 0], chan_own, SHIFT_AT),
            )
            for s in range(y_groups)
        ]
        scale = jnp.concatenate([one[0] for one in pairs], axis=0)
        offset = jnp.concatenate([one[1] for one in pairs], axis=0)
        lanes = lax.broadcasted_iota(jnp.int32, (chan_all, LANES), 1)
        next_ref[...] = jnp.where(lanes == 0, scale, jnp.where(lanes == 1, offset, 0.0))
        peak = jnp.zeros((chan_all, LANES), bf16)
        for extreme in (leasts, mosts):
            value = activated(jnp.concatenate(extreme, axis=0), scale, offset)
            peak = jnp.maximum(peak, jnp.abs(value))
        row = at_lane(tops[:, PEAK_AT : PEAK_AT + 1], 0)
        row = row + at_lane(tops[:, PEAK_AT + 1 : PEAK_AT + 2], 1)
        row = row + at_lane(peak_of(peak_pool), 2)
        row = row + at_lane(peak_of(peak), 3)
        peak_ref[...] = row[:, : peak_ref.shape[1]]

    return kernel


def fourth_kernel(coarse_cells):
    def kernel(
        raw_ref,
        weight_ref,
        param_ref,
        affine_ref,
        next_ref,
        fine_ref,
        out_ref,
        skip_ref,
        cells_ref,
        last_ref,
        narrow_ref,
        done,
    ):
        scale = affine_ref[:, 0:1]
        offset = affine_ref[:, 1:2]
        sends = []
        for z in range(fine_ref.shape[0]):
            act = jnp.stack(
                [activated(fine_ref[z, y], scale, offset) for y in range(fine_ref.shape[1])]
            )
            narrow_ref[:, z] = jnp.transpose(act, (1, 0, 2))
            sends.append(
                pltpu.make_async_copy(narrow_ref.at[:, z], skip_ref.at[0, :, z], done.at[z])
            )
            sends[-1].start()
        planes, chan_all, flat = cells_ref.shape
        chan_own, z_own = out_ref.shape[1:3]
        row_len = LANES // 2
        blocks = flat // LANES
        weight = weight_ref[...]
        lower = lax.broadcasted_iota(jnp.int32, (chan_own, LANES), 1) < row_len
        blank = jnp.zeros((chan_own, LANES), f32)
        bound = clip_bound(param_ref, 3)
        scale = next_ref[:, 0:1]
        offset = next_ref[:, 1:2]

        def at_block(block):
            return slice(block * LANES, (block + 1) * LANES)

        def normed(z):
            for j in range(blocks):
                value = activated(raw_ref[z, :, at_block(j)], scale, offset)
                cells_ref[z, :, at_block(j)] = bounded(value, bound)

        def plane(z, sums):
            total, square = sums
            depths = [dz for dz in range(3) if 0 <= z + dz - 1 < planes]
            columns = slice(depths[0] * chan_all, (depths[-1] + 1) * chan_all)
            parts = []
            for t in range(blocks // 2):
                window = jnp.concatenate(
                    [
                        cells_ref[z + dz - 1, :, 2 * t * LANES : 2 * (t + 1) * LANES]
                        for dz in depths
                    ],
                    axis=0,
                )
                taps = jnp.dot(weight[:, columns], window, preferred_element_type=f32)
                parts.extend(taps[:, at_block(half)] for half in range(2))

            def tap(dy, dx, j):
                at = (3 * dy + dx) * chan_own
                return parts[j][at : at + chan_own]

            for j in range(blocks):
                three = []
                for dx in range(3):
                    if j > 0:
                        before = tap(0, dx, j - 1)
                    else:
                        before = jnp.where(lower, blank, turned(tap(0, dx, blocks - 1)))
                    if j + 1 < blocks:
                        after = tap(2, dx, j + 1)
                    else:
                        after = jnp.where(lower, turned(tap(2, dx, 0)), blank)
                    three.append(tap(1, dx, j) + before + after)
                out = tap_sum(*three, row_len)
                last_ref[z, :, at_block(j)] = out
                total = total + out
                square = square + out * out
            return total, square

        sums = (blank, blank)
        normed(0)
        for z in range(planes):
            if z + 1 < planes:
                normed(z + 1)
            sums = plane(z, sums)
        total, square = sums
        scale, offset = affine(
            jnp.sum(total, axis=1, keepdims=True),
            jnp.sum(square, axis=1, keepdims=True),
            coarse_cells,
            lane_of(param_ref, LAST_AT, chan_own),
            lane_of(param_ref, LAST_AT + 1, chan_own),
        )
        at_z = lax.axis_index("sz")
        own = []
        for i in range(z_own):
            cells = activated(last_ref[at_z * z_own + i], scale, offset).astype(f32)
            natural = []
            for p in range(blocks):
                row = (2 * p) % blocks
                first, second = cells[:, at_block(row)], cells[:, at_block(row + 1)]
                if 2 * p < blocks:
                    natural.append(jnp.where(lower, first, turned(second)))
                else:
                    natural.append(jnp.where(lower, turned(first), second))
            own.append(jnp.concatenate(natural, axis=1))
        for c in range(chan_own):
            out_ref[0, c] = jnp.concatenate([one[c : c + 1] for one in own], axis=0).astype(bf16)
        for send in sends:
            send.wait()

    return kernel


def shape(dims, dtype):
    return jax.ShapeDtypeStruct(dims, dtype)


def near_shape(dims, dtype):
    return pltpu.VMEM(dims, dtype)


def held(value):
    return pltpu.with_memory_space_constraint(value, pltpu.VMEM)


def per_device(
    volume,
    amax_history,
    conv_first,
    conv_second,
    conv_third,
    conv_fourth,
    gain_fine,
    shift_fine,
    gain_coarse,
    shift_coarse,
):
    channels, depth, height, width = volume.shape[1:]
    z_groups = lax.axis_size("sz")
    y_groups = lax.axis_size("sy")
    samples = lax.axis_size("sample")
    fine_cells = float(depth * z_groups * height * y_groups * width)
    coarse_cells = fine_cells / 8
    chan_own = conv_third.shape[1]
    chan_all = conv_fourth.shape[2]
    span = (height // 2) * (width // 2)
    planes = (depth // 2) * z_groups
    flat = span * y_groups
    group = z_groups * y_groups
    load_rows = (depth // 2) * channels + ROWS

    cells, first, second, peak = pl.pallas_call(
        prep_kernel,
        out_shape=(
            near_shape((depth, height, channels, width), bf16),
            near_shape((HALO, height, channels, width), bf16),
            near_shape((HALO, height, channels, width), bf16),
            near_shape((1, LANES), f32),
        ),
        name="prep",
    )(volume, amax_history)
    third_rows = 4 * chan_own
    m1, m2, m3, m4, params, gain_row = pl.pallas_call(
        matrix_kernel,
        out_shape=(
            near_shape((3 * channels, 9 * channels), bf16),
            near_shape((3 * channels, 9 * channels), bf16),
            near_shape((third_rows, 8 * channels), bf16),
            near_shape((9 * chan_own, 3 * chan_all), bf16),
            near_shape((channels, LANES), f32),
            near_shape((1, LANES), f32),
        ),
        name="matrices",
    )(
        held(peak),
        conv_first,
        conv_second,
        conv_third,
        conv_fourth,
        amax_history,
        gain_fine,
        shift_fine,
        gain_coarse,
        shift_coarse,
    )
    pair_first, pair_second = pairings("sz")
    z_first = lax.ppermute(first, "sz", pair_first)
    z_second = lax.ppermute(second, "sz", pair_second)
    deep_depth = depth + 2 * HALO
    anywhere = pl.BlockSpec(memory_space=pl.ANY)
    levels = amax_history.shape[0]
    first, second = pl.pallas_call(
        deep_kernel,
        out_shape=(
            near_shape((deep_depth, HALO, channels, width), bf16),
            near_shape((deep_depth, HALO, channels, width), bf16),
        ),
        name="deep",
    )(held(cells), held(z_first), held(z_second), held(m1))
    pair_first, pair_second = pairings("sy")
    y_first = lax.ppermute(first, "sy", pair_first)
    y_second = lax.ppermute(second, "sy", pair_second)
    deep, raw_inner, sums = pl.pallas_call(
        first_inner_kernel,
        out_shape=(
            near_shape((deep_depth, height, channels, width), bf16),
            near_shape((depth + 2, height - 2, channels, width), f32),
            near_shape((2, channels, LANES), f32),
        ),
        name="first_inner",
    )(*(held(x) for x in (cells, z_first, z_second, m1)))
    raw_outer, row = pl.pallas_call(
        first_outer_kernel,
        out_shape=(
            near_shape((depth + 2, 2 * HALO, channels, width), f32),
            near_shape((group, 1, LANES), f32),
        ),
        scratch_shapes=[pltpu.VMEM((2, deep_depth, HALO, channels, width), bf16)],
        name="first_outer",
    )(*(held(x) for x in (deep, y_first, y_second, m1, peak, sums)))
    rows = lax.all_to_all(row, ("sy", "sz"), 0, 0, tiled=True)
    raw_second, load = pl.pallas_call(
        second_kernel(fine_cells),
        out_shape=(
            near_shape((depth, height, channels, width), f32),
            near_shape((load_rows, span), bf16),
        ),
        scratch_shapes=[
            pltpu.VMEM((depth + 2, height + 2, channels, width), bf16),
            pltpu.VMEM((depth // 2, height // 2, channels, width), f32),
        ],
        compiler_params=pltpu.CompilerParams(vmem_limit_bytes=KERNEL_BYTES),
        name="second",
    )(*(held(x) for x in (raw_inner, raw_outer, rows, m2, params, gain_row)))
    loads = [load]
    for k in range(1, z_groups):
        loads.append(lax.ppermute(load, "sz", [(i, i ^ k) for i in range(z_groups)]))
    loads.append(m3)
    gathered = lax.all_gather(jnp.concatenate(loads, axis=0), "sy", axis=0)
    raw_third, peaks, fine_affine, next_affine = pl.pallas_call(
        third_kernel(fine_cells, coarse_cells, load_rows, third_rows),
        out_shape=(
            near_shape((planes, chan_all, flat), f32),
            near_shape((1, levels), f32),
            near_shape((channels, LANES), f32),
            near_shape((chan_all, LANES), f32),
        ),
        scratch_shapes=[pltpu.VMEM((planes + 2, 3 * channels, flat + 2 * LANES), bf16)],
        compiler_params=pltpu.CompilerParams(vmem_limit_bytes=KERNEL_BYTES),
        name="third",
    )(held(gathered), held(params))
    if samples <= 4:
        others = [
            lax.ppermute(peaks, "sample", [(i, (i + k) % samples) for i in range(samples)])
            for k in range(1, samples)
        ]
    else:
        others = [lax.pmax(peaks, "sample")]
    near = pl.BlockSpec(memory_space=pltpu.VMEM)
    coarse, skip = pl.pallas_call(
        fourth_kernel(coarse_cells),
        out_shape=(
            shape((1, chan_own, depth // 2, flat), bf16),
            shape((1, channels, depth, height, width), bf16),
        ),
        out_specs=(near, anywhere),
        scratch_shapes=[
            pltpu.VMEM((planes, chan_all, flat), bf16),
            pltpu.VMEM((planes, chan_own, flat), f32),
            pltpu.VMEM((channels, depth, height, width), bf16),
            pltpu.SemaphoreType.DMA((depth,)),
        ],
        compiler_params=pltpu.CompilerParams(vmem_limit_bytes=KERNEL_BYTES),
        name="fourth",
    )(*(held(x) for x in (raw_third, m4, params, fine_affine, next_affine, raw_second)))
    for other in others:
        peaks = jnp.maximum(peaks, other)
    return skip, coarse, peaks.reshape(levels)


def solution(mesh):
    return jax.shard_map(
        per_device,
        mesh=mesh,
        in_specs=(
            P("sample", None, "sz", "sy", None),
            P(),
            P(),
            P(),
            P(None, "sy", None),
            P(None, "sy", None),
            P(),
            P(),
            P(None, "sy"),
            P(None, "sy"),
        ),
        out_specs=(P("sample", None, "sz", "sy", None), P("sample", "sy", "sz", None), P()),
        check_vma=False,
    )
```

```python
import jax
import jax.numpy as jnp
from jax import lax
from jax.experimental import pallas as pl
from jax.experimental.pallas import tpu as pltpu
from jax.sharding import PartitionSpec as P

norm_eps = 1e-05
leak_slope = 0.01
f32 = jnp.float32
bf16 = jnp.bfloat16
LANES = 128
HALO = 2
KERNEL_BYTES = 24 * 1024 * 1024
PEAK_AT = 64
CODE_AT = 66
GAIN_AT = 80
SHIFT_AT = 96
CODE_SPAN = 83.0
ROWS = 8


def pairings(axis):
    count = lax.axis_size(axis)
    first = [(i, i ^ 1) for i in range(count)]
    second = [(i, min(max(((i + 1) ^ 1) - 1, 0), count - 1)) for i in range(count)]
    return first, second


def column(row, channels, start):
    lanes = lax.broadcasted_iota(jnp.int32, (channels, row.shape[1]), 1)
    chans = lax.broadcasted_iota(jnp.int32, (channels, row.shape[1]), 0)
    return jnp.sum(jnp.where(lanes == chans + start, row, 0.0), axis=1, keepdims=True)


def as_row(col, start):
    channels = col.shape[0]
    lanes = lax.broadcasted_iota(jnp.int32, (channels, LANES), 1)
    chans = lax.broadcasted_iota(jnp.int32, (channels, LANES), 0)
    return jnp.sum(jnp.where(lanes == chans + start, col, 0.0), axis=0, keepdims=True)


def at_lane(value, lane):
    lanes = lax.broadcasted_iota(jnp.int32, (1, LANES), 1)
    return jnp.where(lanes == lane, value, 0.0)


def affine(total, square, cells, gains, offset):
    mean = total / cells
    spread = square / cells - mean * mean
    scale = lax.rsqrt(spread + norm_eps) * gains
    return scale, offset - mean * scale


def activated(values, scale, offset):
    normed = values * scale + offset
    return jnp.maximum(normed, leak_slope * normed).astype(bf16)


def peak_of(values):
    values = values.astype(f32)
    return jnp.max(jnp.max(values, axis=0, keepdims=True), axis=1, keepdims=True)


def bounded(values, bound):
    return jnp.minimum(jnp.maximum(values, -bound), bound)


BOUND_AT = 4
LAST_AT = 8


def bound_of(hist_ref, level):
    return jnp.max(hist_ref[level : level + 1, :], axis=1, keepdims=True)


def lane_of(param_ref, lane, channels):
    return param_ref[0:channels, lane : lane + 1]


def clip_bound(param_ref, level):
    return param_ref[0:1, BOUND_AT + level : BOUND_AT + level + 1].astype(bf16)


def matrix_of(weight, taps_ref, groups):
    out_chan = weight.shape[1]
    for dx in range(3):
        taps_ref[dx * out_chan : (dx + 1) * out_chan, :] = jnp.concatenate(
            [weight[3 * j + dx] for j in groups], axis=1
        )


def matrix_kernel(
    peak_ref,
    first_ref,
    second_ref,
    third_ref,
    fourth_ref,
    hist_ref,
    gain_ref,
    shift_ref,
    gain_coarse_ref,
    shift_coarse_ref,
    m1_ref,
    m2_ref,
    m3_ref,
    m4_ref,
    param_ref,
    gain_row_ref,
):
    taps = first_ref.shape[0]
    matrix_of(first_ref, m1_ref, range(taps // 3))
    matrix_of(second_ref, m2_ref, range(taps // 3))
    own = third_ref.shape[1]
    matrix_of(third_ref, m3_ref.at[0 : 3 * own], range(taps // 3 - 1))
    last = [third_ref[taps - 3 + dx] for dx in range(3)]
    rest = m3_ref.shape[1] - 3 * third_ref.shape[2]
    m3_ref[3 * own :, :] = jnp.concatenate(last + [jnp.zeros((own, rest), bf16)], axis=1)
    for dy in range(3):
        for dx in range(3):
            at = (3 * dy + dx) * own
            m4_ref[at : at + own, :] = jnp.concatenate(
                [fourth_ref[9 * dz + 3 * dy + dx] for dz in range(3)], axis=1
            )
    channels = param_ref.shape[0]
    lanes = lax.broadcasted_iota(jnp.int32, (channels, LANES), 1)
    params = jnp.zeros((channels, LANES), f32)
    columns = []
    for layer in range(2):
        columns.append((2 * layer, column(gain_ref[layer : layer + 1, :], channels, 0)))
        columns.append((2 * layer + 1, column(shift_ref[layer : layer + 1, :], channels, 0)))
    for level in range(hist_ref.shape[0]):
        columns.append((BOUND_AT + level, bound_of(hist_ref, level)))
    pad = jnp.zeros((channels - own, 1), f32)
    for place, ref in ((LAST_AT, gain_coarse_ref), (LAST_AT + 1, shift_coarse_ref)):
        columns.append((place, jnp.concatenate([column(ref[1:2, :], own, 0), pad], axis=0)))
    for lane, value in columns:
        params = jnp.where(lanes == lane, value, params)
    param_ref[...] = params
    gain_row_ref[...] = as_row(column(gain_coarse_ref[0:1, :], own, 0), GAIN_AT) + as_row(
        column(shift_coarse_ref[0:1, :], own, 0), SHIFT_AT
    )


def tap_sum(left, middle, right, period):
    lane = lax.broadcasted_iota(jnp.int32, middle.shape, 1) % period
    up = pltpu.roll(left, 1, 1)
    down = pltpu.roll(right, LANES - 1, 1)
    return middle + jnp.where(lane == 0, 0.0, up) + jnp.where(lane == period - 1, 0.0, down)


def prep_kernel(vol_ref, hist_ref, cells_ref, first_ref, second_ref, peak_ref):
    depth = vol_ref.shape[2]
    bound = bound_of(hist_ref, 0).astype(bf16)
    top = jnp.zeros(cells_ref.shape[2:], bf16)
    for z in range(depth):
        rows = jnp.transpose(vol_ref[0, :, z], (1, 0, 2))
        for y in range(rows.shape[0]):
            top = jnp.maximum(top, jnp.abs(rows[y]))
            cells_ref[z, y] = bounded(rows[y], bound)
    peak_ref[...] = jnp.broadcast_to(peak_of(top), (1, LANES))
    even = lax.axis_index("sz") % 2 == 0
    start_first = jnp.where(even, depth - HALO, 0)
    start_second = jnp.where(even, 0, depth - HALO)
    first_ref[...] = cells_ref[pl.ds(start_first, HALO)]
    second_ref[...] = cells_ref[pl.ds(start_second, HALO)]


def sides(axis, first, second):
    at = lax.axis_index(axis)
    count = lax.axis_size(axis)
    even = at % 2 == 0
    blank = jnp.zeros_like(first)
    below = jnp.where(at == 0, blank, jnp.where(even, second, first))
    above = jnp.where(at == count - 1, blank, jnp.where(even, first, second))
    return below, above


def deep_kernel(cells_ref, got_first_ref, got_second_ref, matrix_ref, first_ref, second_ref):
    depth, height = cells_ref.shape[:2]
    even = lax.axis_index("sy") % 2 == 0
    starts = (jnp.where(even, height - HALO, 0), jnp.where(even, 0, height - HALO))
    odd_z = lax.axis_index("sz") % 2
    far = HALO + depth
    for start, out_ref in zip(starts, (first_ref, second_ref)):
        rows = pl.ds(start, HALO)
        out_ref[pl.ds((1 - odd_z) * far, HALO)] = got_first_ref[:, rows]
        out_ref[pl.ds(odd_z * far, HALO)] = got_second_ref[:, rows]
        out_ref[HALO:far] = cells_ref[:, rows]


def conv_rows(cell, weight, z, rows, out_chan):
    window = jnp.concatenate(
        [
            jnp.concatenate([cell(z + dz, y + dy) for y in rows], axis=1)
            for dz in range(3)
            for dy in range(3)
        ],
        axis=0,
    )
    taps = jnp.dot(weight, window, preferred_element_type=f32)
    outs = []
    for half in range(2):
        part = taps[:, half * LANES : (half + 1) * LANES]
        outs.append(
            tap_sum(
                part[:out_chan], part[out_chan : 2 * out_chan], part[2 * out_chan :], LANES
            )
        )
    return outs


def first_inner_kernel(own_ref, got_first_ref, got_second_ref, weight_ref, deep_ref, raw_ref, sum_ref):
    depth, count, channels = raw_ref.shape[:3]
    own_depth = own_ref.shape[0]
    below, above = sides("sz", got_first_ref[...], got_second_ref[...])
    deep_ref[0:HALO] = below
    deep_ref[HALO : HALO + own_depth] = own_ref[...]
    deep_ref[HALO + own_depth :] = above
    weight = weight_ref[...]
    total = jnp.zeros((channels, LANES), f32)
    square = total
    for z in range(depth):
        for y in range(0, count, 2):
            outs = conv_rows(lambda z, y: deep_ref[z, y], weight, z, (y, y + 1), channels)
            for half in range(2):
                raw_ref[z, y + half] = outs[half]
                if 1 <= z < depth - 1:
                    total = total + outs[half]
                    square = square + outs[half] * outs[half]
    sum_ref[0] = total
    sum_ref[1] = square


def first_outer_kernel(
    deep_ref, got_first_ref, got_second_ref, weight_ref, peak_ref, sum_ref, raw_ref, row_ref, edge_ref
):
    depth, count, channels = raw_ref.shape[:3]
    planes, own_height = deep_ref.shape[:2]
    below, above = sides("sy", got_first_ref[...], got_second_ref[...])
    edge_ref[0] = below
    edge_ref[1] = above

    for at_end, end in (
        (lax.axis_index("sz") == 0, slice(0, HALO)),
        (lax.axis_index("sz") == lax.axis_size("sz") - 1, slice(planes - HALO, planes)),
    ):

        @pl.when(at_end)
        def _():
            edge_ref[:, end] = jnp.zeros((2, HALO) + edge_ref.shape[2:], bf16)

    def cell(z, y):
        if y < HALO:
            return edge_ref[0, z, y]
        if y < HALO + own_height:
            return deep_ref[z, y - HALO]
        return edge_ref[1, z, y - HALO - own_height]

    weight = weight_ref[...]
    total = sum_ref[0]
    square = sum_ref[1]
    last = own_height + 2 - 1
    for z in range(depth):
        for place, rows in ((0, (0, 1)), (2, (last - 1, last))):
            outs = conv_rows(cell, weight, z, rows, channels)
            for half in range(2):
                raw_ref[z, place + half] = outs[half]
                if 1 <= z < depth - 1 and 1 <= rows[half] < last:
                    total = total + outs[half]
                    square = square + outs[half] * outs[half]
    row = as_row(jnp.sum(total, axis=1, keepdims=True), 0)
    row = row + as_row(jnp.sum(square, axis=1, keepdims=True), channels)
    row = row + at_lane(peak_ref[...], PEAK_AT)
    row_ref[...] = jnp.broadcast_to(row[None], row_ref.shape)


def second_kernel(cell_count):
    def kernel(
        inner_ref,
        outer_ref,
        rows_ref,
        weight_ref,
        param_ref,
        gain_row_ref,
        raw_ref,
        load_ref,
        hidden_ref,
        pool_ref,
    ):
        depth, height, channels, width = raw_ref.shape
        wide_depth, wide_height = hidden_ref.shape[:2]
        rows = rows_ref[...]
        merged = jnp.sum(rows, axis=0)
        peak_vol = jnp.max(rows, axis=0)
        scale, offset = affine(
            column(merged, channels, 0),
            column(merged, channels, channels),
            cell_count,
            lane_of(param_ref, 0, channels),
            lane_of(param_ref, 1, channels),
        )
        bound = clip_bound(param_ref, 1)
        at_z = lax.axis_index("sz")
        at_y = lax.axis_index("sy")
        last_z = lax.axis_size("sz") - 1
        last_y = lax.axis_size("sy") - 1
        peak = jnp.zeros((channels, width), bf16)
        for z in range(wide_depth):
            for y in range(wide_height):
                if y < HALO:
                    raw = outer_ref[z, y]
                elif y < height:
                    raw = inner_ref[z, y - HALO]
                else:
                    raw = outer_ref[z, y - height + HALO]
                hidden = activated(raw, scale, offset)
                if 1 <= y < wide_height - 1 and 1 <= z < wide_depth - 1:
                    peak = jnp.maximum(peak, jnp.abs(hidden))
                hidden_ref[z, y] = bounded(hidden, bound)
        outside = (
            (at_z == 0, (slice(0, 1), slice(0, wide_height))),
            (at_z == last_z, (slice(wide_depth - 1, wide_depth), slice(0, wide_height))),
            (at_y == 0, (slice(0, wide_depth), slice(0, 1))),
            (at_y == last_y, (slice(0, wide_depth), slice(wide_height - 1, wide_height))),
        )
        for at_end, (zs, ys) in outside:

            @pl.when(at_end)
            def _():
                count = (zs.stop - zs.start, ys.stop - ys.start)
                hidden_ref[zs, ys] = jnp.zeros(count + (channels, width), bf16)

        blank = jnp.zeros((channels, width), f32)
        weight = weight_ref[...]
        sign = jnp.where(lane_of(param_ref, 2, channels) >= 0, 1.0, -1.0).astype(f32)
        half_height = height // 2
        total, square, least, most = blank, blank, blank + 1e30, blank - 1e30
        for zp in range(depth // 2):
            for yp in range(half_height):
                best = None
                for dz in range(2):
                    z = 2 * zp + dz
                    outs = conv_rows(
                        lambda z, y: hidden_ref[z, y], weight, z, (2 * yp, 2 * yp + 1), channels
                    )
                    for half in range(2):
                        raw_ref[z, 2 * yp + half] = outs[half]
                        total = total + outs[half]
                        square = square + outs[half] * outs[half]
                        signed = outs[half] * sign
                        best = signed if best is None else jnp.maximum(best, signed)
                best = jnp.maximum(best, pltpu.roll(best, LANES - 1, 1)) * sign
                pool_ref[zp, yp] = best
                least = jnp.minimum(least, best)
                most = jnp.maximum(most, best)
        most, least = peak_of(most), -peak_of(-least)
        center = 0.5 * (most + least)
        reach = jnp.maximum(0.5 * (most - least), 1e-30)
        rate = CODE_SPAN / reach
        pick = jnp.where(
            lax.broadcasted_iota(jnp.int32, (2 * LANES, LANES), 0)
            == 2 * lax.broadcasted_iota(jnp.int32, (2 * LANES, LANES), 1),
            1.0,
            0.0,
        ).astype(bf16)
        for zp in range(depth // 2):
            for yq in range(half_height // 2):
                both = jnp.concatenate([pool_ref[zp, 2 * yq], pool_ref[zp, 2 * yq + 1]], axis=1)
                both = jnp.exp((both - center) * rate).astype(bf16)
                load_ref[
                    zp * channels : (zp + 1) * channels, yq * LANES : (yq + 1) * LANES
                ] = jnp.dot(both, pick, preferred_element_type=f32).astype(bf16)
        row = as_row(jnp.sum(total, axis=1, keepdims=True), 0)
        row = row + as_row(jnp.sum(square, axis=1, keepdims=True), channels)
        row = row + at_lane(peak_vol, PEAK_AT)
        row = row + at_lane(peak_of(peak), PEAK_AT + 1)
        row = row + at_lane(center, CODE_AT)
        row = row + at_lane(reach / CODE_SPAN, CODE_AT + 1)
        row = row + gain_row_ref[...]
        high = row.astype(bf16).astype(f32)
        middle = (row - high).astype(bf16).astype(f32)
        low = row - high - middle
        level = lax.broadcasted_iota(jnp.int32, (ROWS, LANES), 0)
        parts = jnp.where(
            level == 0, high, jnp.where(level == 1, middle, jnp.where(level == 2, low, 0.0))
        )
        body = (depth // 2) * channels
        load_ref[body:, 0:LANES] = parts.astype(bf16)
        load_ref[body:, LANES:] = jnp.zeros((ROWS, load_ref.shape[1] - LANES), bf16)

    return kernel


def turned(cells):
    return pltpu.roll(cells, LANES // 2, 1)


def third_kernel(fine_cells, coarse_cells, load_rows, piece):
    def kernel(*refs):
        all_ref, param_ref = refs[:2]
        piece_refs = refs[2:-7]
        raw_ref, peak_ref, affine_ref, next_ref, cells_ref, near_ref, far_ref = refs[-7:]
        y_groups = all_ref.shape[0]
        z_groups = lax.axis_size("sz")
        span = all_ref.shape[2]
        planes, chan_all, flat = raw_ref.shape
        channels = cells_ref.shape[1] // 3
        chan_own = piece // 4
        row_len = LANES // 2
        blocks = flat // LANES
        body = load_rows - ROWS
        z_own = body // channels
        at_z = lax.axis_index("sz")
        totals = jnp.zeros((ROWS, LANES), f32)
        tops = jnp.zeros((1, LANES), f32)
        rows = {}
        for s in range(y_groups):
            for k in range(z_groups):
                parts = all_ref[s, k * load_rows + body : (k + 1) * load_rows, 0:LANES].astype(f32)
                totals = totals + parts
                rows[s, k] = jnp.sum(parts, axis=0, keepdims=True)
                tops = jnp.maximum(tops, rows[s, k])
        merged = jnp.sum(totals, axis=0, keepdims=True)
        scale, offset = affine(
            column(merged, channels, 0),
            column(merged, channels, channels),
            fine_cells,
            lane_of(param_ref, 2, channels),
            lane_of(param_ref, 3, channels),
        )
        lanes = lax.broadcasted_iota(jnp.int32, (channels, LANES), 1)
        affine_ref[...] = jnp.where(lanes == 0, scale, jnp.where(lanes == 1, offset, 0.0))
        bound = clip_bound(param_ref, 2)
        lower = lanes < row_len
        edge = lanes % row_len
        blank = jnp.zeros((channels, LANES), bf16)
        middle = slice(channels, 2 * channels)

        def at_block(block):
            return slice(block * LANES, (block + 1) * LANES)

        def keep(place, block, value):
            cells_ref[place, middle, at_block(block)] = value
            if block >= 2:
                cells_ref[place, :channels, at_block(block)] = jnp.where(
                    edge == 0, blank, pltpu.roll(value, 1, 1)
                )
                cells_ref[place, 2 * channels :, at_block(block)] = jnp.where(
                    edge == row_len - 1, blank, pltpu.roll(value, LANES - 1, 1)
                )

        cells_ref[0] = jnp.zeros(cells_ref.shape[1:], bf16)
        cells_ref[planes + 1] = jnp.zeros(cells_ref.shape[1:], bf16)
        peak_pool = jnp.zeros((channels, span), bf16)
        half_groups = y_groups // 2
        for k in range(z_groups):
            for zp in range(z_own):
                place = (at_z ^ k) * z_own + zp + 1
                at = k * load_rows + zp * channels
                ends = []
                for s in range(half_groups):
                    both = []
                    for own in (s, s + half_groups):
                        center = rows[own, k][:, CODE_AT : CODE_AT + 1]
                        reach = rows[own, k][:, CODE_AT + 1 : CODE_AT + 2]
                        code = jnp.log(all_ref[own, at : at + channels, :].astype(f32))
                        value = activated(code, scale * reach, scale * center + offset)
                        peak_pool = jnp.maximum(peak_pool, jnp.abs(value))
                        both.append(bounded(value, bound))
                    for q in range(span // LANES):
                        low, high = (one[:, at_block(q)] for one in both)
                        block = s * (span // row_len) + 2 * q
                        one = jnp.where(lower, low, turned(high))
                        two = jnp.where(lower, turned(low), high)
                        keep(place, block + 1, one)
                        keep(place, block + 2, two)
                        if block == 0:
                            ends.append((blocks + 1, jnp.where(lower, turned(one), blank)))
                        if block + 2 == blocks:
                            ends.append((0, jnp.where(lower, blank, turned(two))))
                for block, value in ends:
                    keep(place, block, value)
        main = 3 * chan_own
        at_y = lax.axis_index("sy")
        for k, piece_ref in enumerate(piece_refs):
            near_ref[pl.ds((at_y ^ k) * main, main), :] = piece_ref[:main, :]
            far_ref[pl.ds((at_y ^ k) * chan_own, chan_own), :] = piece_ref[main:, : 3 * channels]
        near_weight = near_ref[...]
        far_weight = far_ref[...]
        blank = jnp.zeros((chan_own, LANES), f32)
        totals = [blank for _ in range(y_groups)]
        squares = [blank for _ in range(y_groups)]
        leasts = [blank + 1e30 for _ in range(y_groups)]
        mosts = [blank - 1e30 for _ in range(y_groups)]
        width = 2 * LANES
        for z in range(planes):
            for t in range(blocks // 2):
                window = [
                    cells_ref[z + dz, middle, (2 * t + dy) * LANES : (2 * t + dy) * LANES + width]
                    for dz in range(3)
                    for dy in range(3)
                    if dz + dy < 4
                ]
                taps = jnp.dot(
                    near_weight, jnp.concatenate(window, axis=0), preferred_element_type=f32
                )
                rest = jnp.dot(
                    far_weight,
                    cells_ref[z + 2, :, (2 * t + 2) * LANES : (2 * t + 2) * LANES + width],
                    preferred_element_type=f32,
                )
                for s in range(y_groups):
                    for half in range(2):
                        at = s * main
                        part = taps[at : at + main, at_block(half)]
                        out = tap_sum(
                            part[:chan_own],
                            part[chan_own : 2 * chan_own]
                            + rest[s * chan_own : (s + 1) * chan_own, at_block(half)],
                            part[2 * chan_own :],
                            row_len,
                        )
                        raw_ref[
                            z, s * chan_own : (s + 1) * chan_own, at_block(2 * t + half)
                        ] = out
                        totals[s] = totals[s] + out
                        squares[s] = squares[s] + out * out
                        leasts[s] = jnp.minimum(leasts[s], out)
                        mosts[s] = jnp.maximum(mosts[s], out)
        pairs = [
            affine(
                jnp.sum(totals[s], axis=1, keepdims=True),
                jnp.sum(squares[s], axis=1, keepdims=True),
                coarse_cells,
                column(rows[s, 0], chan_own, GAIN_AT),
                column(rows[s, 0], chan_own, SHIFT_AT),
            )
            for s in range(y_groups)
        ]
        scale = jnp.concatenate([one[0] for one in pairs], axis=0)
        offset = jnp.concatenate([one[1] for one in pairs], axis=0)
        lanes = lax.broadcasted_iota(jnp.int32, (chan_all, LANES), 1)
        next_ref[...] = jnp.where(lanes == 0, scale, jnp.where(lanes == 1, offset, 0.0))
        peak = jnp.zeros((chan_all, LANES), bf16)
        for extreme in (leasts, mosts):
            value = activated(jnp.concatenate(extreme, axis=0), scale, offset)
            peak = jnp.maximum(peak, jnp.abs(value))
        row = at_lane(tops[:, PEAK_AT : PEAK_AT + 1], 0)
        row = row + at_lane(tops[:, PEAK_AT + 1 : PEAK_AT + 2], 1)
        row = row + at_lane(peak_of(peak_pool), 2)
        row = row + at_lane(peak_of(peak), 3)
        peak_ref[...] = row[:, : peak_ref.shape[1]]

    return kernel


def fourth_kernel(coarse_cells):
    def kernel(
        raw_ref,
        weight_ref,
        param_ref,
        affine_ref,
        next_ref,
        fine_ref,
        out_ref,
        skip_ref,
        cells_ref,
        last_ref,
        narrow_ref,
        done,
    ):
        scale = affine_ref[:, 0:1]
        offset = affine_ref[:, 1:2]
        sends = []
        for z in range(fine_ref.shape[0]):
            act = jnp.stack(
                [activated(fine_ref[z, y], scale, offset) for y in range(fine_ref.shape[1])]
            )
            narrow_ref[:, z] = jnp.transpose(act, (1, 0, 2))
            sends.append(
                pltpu.make_async_copy(narrow_ref.at[:, z], skip_ref.at[0, :, z], done.at[z])
            )
            sends[-1].start()
        planes, chan_all, flat = cells_ref.shape
        chan_own, z_own = out_ref.shape[:2]
        row_len = LANES // 2
        blocks = flat // LANES
        weight = weight_ref[...]
        lower = lax.broadcasted_iota(jnp.int32, (chan_own, LANES), 1) < row_len
        blank = jnp.zeros((chan_own, LANES), f32)
        bound = clip_bound(param_ref, 3)
        scale = next_ref[:, 0:1]
        offset = next_ref[:, 1:2]

        def at_block(block):
            return slice(block * LANES, (block + 1) * LANES)

        def normed(z):
            for j in range(blocks):
                value = activated(raw_ref[z, :, at_block(j)], scale, offset)
                cells_ref[z, :, at_block(j)] = bounded(value, bound)

        def plane(z, sums):
            total, square = sums
            depths = [dz for dz in range(3) if 0 <= z + dz - 1 < planes]
            columns = slice(depths[0] * chan_all, (depths[-1] + 1) * chan_all)
            parts = []
            for t in range(blocks // 2):
                window = jnp.concatenate(
                    [
                        cells_ref[z + dz - 1, :, 2 * t * LANES : 2 * (t + 1) * LANES]
                        for dz in depths
                    ],
                    axis=0,
                )
                taps = jnp.dot(weight[:, columns], window, preferred_element_type=f32)
                parts.extend(taps[:, at_block(half)] for half in range(2))

            def tap(dy, dx, j):
                at = (3 * dy + dx) * chan_own
                return parts[j][at : at + chan_own]

            for j in range(blocks):
                three = []
                for dx in range(3):
                    if j > 0:
                        before = tap(0, dx, j - 1)
                    else:
                        before = jnp.where(lower, blank, turned(tap(0, dx, blocks - 1)))
                    if j + 1 < blocks:
                        after = tap(2, dx, j + 1)
                    else:
                        after = jnp.where(lower, turned(tap(2, dx, 0)), blank)
                    three.append(tap(1, dx, j) + before + after)
                out = tap_sum(*three, row_len)
                last_ref[z, :, at_block(j)] = out
                total = total + out
                square = square + out * out
            return total, square

        sums = (blank, blank)
        normed(0)
        for z in range(planes):
            if z + 1 < planes:
                normed(z + 1)
            sums = plane(z, sums)
        total, square = sums
        scale, offset = affine(
            jnp.sum(total, axis=1, keepdims=True),
            jnp.sum(square, axis=1, keepdims=True),
            coarse_cells,
            lane_of(param_ref, LAST_AT, chan_own),
            lane_of(param_ref, LAST_AT + 1, chan_own),
        )
        at_z = lax.axis_index("sz")
        own = []
        for i in range(z_own):
            cells = activated(last_ref[at_z * z_own + i], scale, offset).astype(f32)
            natural = []
            for p in range(blocks):
                row = (2 * p) % blocks
                first, second = cells[:, at_block(row)], cells[:, at_block(row + 1)]
                if 2 * p < blocks:
                    natural.append(jnp.where(lower, first, turned(second)))
                else:
                    natural.append(jnp.where(lower, turned(first), second))
            own.append(jnp.concatenate(natural, axis=1))
        for c in range(chan_own):
            out_ref[c] = jnp.concatenate([one[c : c + 1] for one in own], axis=0).astype(bf16)
        for send in sends:
            send.wait()

    return kernel


def final_kernel(*refs):
    cells_ref, peak_ref = refs[:2]
    out_ref, top_ref = refs[-2:]
    out_ref[0] = cells_ref[...]
    top = peak_ref[...]
    for ref in refs[2:-2]:
        top = jnp.maximum(top, ref[...])
    top_ref[...] = top


def shape(dims, dtype):
    return jax.ShapeDtypeStruct(dims, dtype)


def near_shape(dims, dtype):
    return pltpu.VMEM(dims, dtype)


def held(value):
    return pltpu.with_memory_space_constraint(value, pltpu.VMEM)


def per_device(
    volume,
    amax_history,
    conv_first,
    conv_second,
    conv_third,
    conv_fourth,
    gain_fine,
    shift_fine,
    gain_coarse,
    shift_coarse,
):
    channels, depth, height, width = volume.shape[1:]
    z_groups = lax.axis_size("sz")
    y_groups = lax.axis_size("sy")
    samples = lax.axis_size("sample")
    fine_cells = float(depth * z_groups * height * y_groups * width)
    coarse_cells = fine_cells / 8
    chan_own = conv_third.shape[1]
    chan_all = conv_fourth.shape[2]
    span = (height // 2) * (width // 2)
    planes = (depth // 2) * z_groups
    flat = span * y_groups
    group = z_groups * y_groups
    load_rows = (depth // 2) * channels + ROWS

    cells, first, second, peak = pl.pallas_call(
        prep_kernel,
        out_shape=(
            near_shape((depth, height, channels, width), bf16),
            near_shape((HALO, height, channels, width), bf16),
            near_shape((HALO, height, channels, width), bf16),
            near_shape((1, LANES), f32),
        ),
        name="prep",
    )(volume, amax_history)
    third_rows = 4 * chan_own
    m1, m2, m3, m4, params, gain_row = pl.pallas_call(
        matrix_kernel,
        out_shape=(
            near_shape((3 * channels, 9 * channels), bf16),
            near_shape((3 * channels, 9 * channels), bf16),
            near_shape((third_rows, 8 * channels), bf16),
            near_shape((9 * chan_own, 3 * chan_all), bf16),
            near_shape((channels, LANES), f32),
            near_shape((1, LANES), f32),
        ),
        name="matrices",
    )(
        held(peak),
        conv_first,
        conv_second,
        conv_third,
        conv_fourth,
        amax_history,
        gain_fine,
        shift_fine,
        gain_coarse,
        shift_coarse,
    )
    pieces = [m3]
    for k in range(1, y_groups):
        pieces.append(lax.ppermute(m3, "sy", [(i, i ^ k) for i in range(y_groups)]))
    pair_first, pair_second = pairings("sz")
    z_first = lax.ppermute(first, "sz", pair_first)
    z_second = lax.ppermute(second, "sz", pair_second)
    deep_depth = depth + 2 * HALO
    anywhere = pl.BlockSpec(memory_space=pl.ANY)
    levels = amax_history.shape[0]
    first, second = pl.pallas_call(
        deep_kernel,
        out_shape=(
            near_shape((deep_depth, HALO, channels, width), bf16),
            near_shape((deep_depth, HALO, channels, width), bf16),
        ),
        name="deep",
    )(held(cells), held(z_first), held(z_second), held(m1))
    pair_first, pair_second = pairings("sy")
    y_first = lax.ppermute(first, "sy", pair_first)
    y_second = lax.ppermute(second, "sy", pair_second)
    deep, raw_inner, sums = pl.pallas_call(
        first_inner_kernel,
        out_shape=(
            near_shape((deep_depth, height, channels, width), bf16),
            near_shape((depth + 2, height - 2, channels, width), f32),
            near_shape((2, channels, LANES), f32),
        ),
        name="first_inner",
    )(*(held(x) for x in (cells, z_first, z_second, m1)))
    raw_outer, row = pl.pallas_call(
        first_outer_kernel,
        out_shape=(
            near_shape((depth + 2, 2 * HALO, channels, width), f32),
            near_shape((group, 1, LANES), f32),
        ),
        scratch_shapes=[pltpu.VMEM((2, deep_depth, HALO, channels, width), bf16)],
        name="first_outer",
    )(*(held(x) for x in (deep, y_first, y_second, m1, peak, sums)))
    rows = lax.all_to_all(row, ("sy", "sz"), 0, 0, tiled=True)
    raw_second, load = pl.pallas_call(
        second_kernel(fine_cells),
        out_shape=(
            near_shape((depth, height, channels, width), f32),
            near_shape((load_rows, span), bf16),
        ),
        scratch_shapes=[
            pltpu.VMEM((depth + 2, height + 2, channels, width), bf16),
            pltpu.VMEM((depth // 2, height // 2, channels, width), f32),
        ],
        compiler_params=pltpu.CompilerParams(vmem_limit_bytes=KERNEL_BYTES),
        name="second",
    )(*(held(x) for x in (raw_inner, raw_outer, rows, m2, params, gain_row)))
    loads = [load]
    for k in range(1, z_groups):
        loads.append(lax.ppermute(load, "sz", [(i, i ^ k) for i in range(z_groups)]))
    gathered = lax.all_gather(jnp.concatenate(loads, axis=0), "sy", axis=0)
    raw_third, peaks, fine_affine, next_affine = pl.pallas_call(
        third_kernel(fine_cells, coarse_cells, load_rows, third_rows),
        out_shape=(
            near_shape((planes, chan_all, flat), f32),
            near_shape((1, levels), f32),
            near_shape((channels, LANES), f32),
            near_shape((chan_all, LANES), f32),
        ),
        scratch_shapes=[
            pltpu.VMEM((planes + 2, 3 * channels, flat + 2 * LANES), bf16),
            pltpu.VMEM((3 * chan_all, 8 * channels), bf16),
            pltpu.VMEM((chan_all, 3 * channels), bf16),
        ],
        compiler_params=pltpu.CompilerParams(vmem_limit_bytes=KERNEL_BYTES),
        name="third",
    )(*(held(x) for x in (gathered, params, *pieces)))
    if samples <= 4:
        others = [
            lax.ppermute(peaks, "sample", [(i, (i + k) % samples) for i in range(samples)])
            for k in range(1, samples)
        ]
    else:
        others = [lax.pmax(peaks, "sample")]
    near = pl.BlockSpec(memory_space=pltpu.VMEM)
    coarse, skip = pl.pallas_call(
        fourth_kernel(coarse_cells),
        out_shape=(
            near_shape((chan_own, depth // 2, flat), bf16),
            shape((1, channels, depth, height, width), bf16),
        ),
        out_specs=(near, anywhere),
        scratch_shapes=[
            pltpu.VMEM((planes, chan_all, flat), bf16),
            pltpu.VMEM((planes, chan_own, flat), f32),
            pltpu.VMEM((channels, depth, height, width), bf16),
            pltpu.SemaphoreType.DMA((depth,)),
        ],
        compiler_params=pltpu.CompilerParams(vmem_limit_bytes=KERNEL_BYTES),
        name="fourth",
    )(*(held(x) for x in (raw_third, m4, params, fine_affine, next_affine, raw_second)))
    coarse, peaks = pl.pallas_call(
        final_kernel,
        out_shape=(
            shape((1, chan_own, depth // 2, flat), bf16),
            shape((1, levels), f32),
        ),
        name="final",
    )(*(held(x) for x in (coarse, peaks, *others)))
    return skip, coarse, peaks.reshape(levels)


def solution(mesh):
    return jax.shard_map(
        per_device,
        mesh=mesh,
        in_specs=(
            P("sample", None, "sz", "sy", None),
            P(),
            P(),
            P(),
            P(None, "sy", None),
            P(None, "sy", None),
            P(),
            P(),
            P(None, "sy"),
            P(None, "sy"),
        ),
        out_specs=(P("sample", None, "sz", "sy", None), P("sample", "sy", "sz", None), P()),
        check_vma=False,
    )
```

```python
import jax
import jax.numpy as jnp
from jax import lax
from jax.experimental import pallas as pl
from jax.experimental.pallas import tpu as pltpu
from jax.sharding import PartitionSpec as P

norm_eps = 1e-05
leak_slope = 0.01
f32 = jnp.float32
bf16 = jnp.bfloat16
LANES = 128
HALO = 2
KERNEL_BYTES = 24 * 1024 * 1024
PEAK_AT = 64
CODE_AT = 66
GAIN_AT = 80
SHIFT_AT = 96
CODE_SPAN = 83.0
ROWS = 8


def pairings(axis):
    count = lax.axis_size(axis)
    first = [(i, i ^ 1) for i in range(count)]
    second = [(i, min(max(((i + 1) ^ 1) - 1, 0), count - 1)) for i in range(count)]
    return first, second


def column(row, channels, start):
    lanes = lax.broadcasted_iota(jnp.int32, (channels, row.shape[1]), 1)
    chans = lax.broadcasted_iota(jnp.int32, (channels, row.shape[1]), 0)
    return jnp.sum(jnp.where(lanes == chans + start, row, 0.0), axis=1, keepdims=True)


def as_row(col, start):
    channels = col.shape[0]
    lanes = lax.broadcasted_iota(jnp.int32, (channels, LANES), 1)
    chans = lax.broadcasted_iota(jnp.int32, (channels, LANES), 0)
    return jnp.sum(jnp.where(lanes == chans + start, col, 0.0), axis=0, keepdims=True)


def at_lane(value, lane):
    lanes = lax.broadcasted_iota(jnp.int32, (1, LANES), 1)
    return jnp.where(lanes == lane, value, 0.0)


def affine(total, square, cells, gains, offset):
    mean = total / cells
    spread = square / cells - mean * mean
    scale = lax.rsqrt(spread + norm_eps) * gains
    return scale, offset - mean * scale


def activated(values, scale, offset):
    normed = values * scale + offset
    return jnp.maximum(normed, leak_slope * normed).astype(bf16)


def peak_of(values):
    values = values.astype(f32)
    return jnp.max(jnp.max(values, axis=0, keepdims=True), axis=1, keepdims=True)


def bounded(values, bound):
    return jnp.minimum(jnp.maximum(values, -bound), bound)


BOUND_AT = 4
LAST_AT = 8


def bound_of(hist_ref, level):
    return jnp.max(hist_ref[level : level + 1, :], axis=1, keepdims=True)


def lane_of(param_ref, lane, channels):
    return param_ref[0:channels, lane : lane + 1]


def clip_bound(param_ref, level):
    return param_ref[0:1, BOUND_AT + level : BOUND_AT + level + 1].astype(bf16)


def matrix_of(weight, taps_ref, groups):
    out_chan = weight.shape[1]
    for dx in range(3):
        taps_ref[dx * out_chan : (dx + 1) * out_chan, :] = jnp.concatenate(
            [weight[3 * j + dx] for j in groups], axis=1
        )


def matrix_kernel(
    peak_ref,
    first_ref,
    second_ref,
    third_ref,
    fourth_ref,
    hist_ref,
    gain_ref,
    shift_ref,
    gain_coarse_ref,
    shift_coarse_ref,
    m1_ref,
    m2_ref,
    m3_ref,
    m4_ref,
    param_ref,
    gain_row_ref,
):
    taps = first_ref.shape[0]
    matrix_of(first_ref, m1_ref, range(taps // 3))
    matrix_of(second_ref, m2_ref, range(taps // 3))
    own = third_ref.shape[1]
    matrix_of(third_ref, m3_ref.at[0 : 3 * own], range(taps // 3 - 1))
    last = [third_ref[taps - 3 + dx] for dx in range(3)]
    rest = m3_ref.shape[1] - 3 * third_ref.shape[2]
    m3_ref[3 * own :, :] = jnp.concatenate(last + [jnp.zeros((own, rest), bf16)], axis=1)
    for dy in range(3):
        for dx in range(3):
            at = (3 * dy + dx) * own
            m4_ref[at : at + own, :] = jnp.concatenate(
                [fourth_ref[9 * dz + 3 * dy + dx] for dz in range(3)], axis=1
            )
    channels = param_ref.shape[0]
    lanes = lax.broadcasted_iota(jnp.int32, (channels, LANES), 1)
    params = jnp.zeros((channels, LANES), f32)
    columns = []
    for layer in range(2):
        columns.append((2 * layer, column(gain_ref[layer : layer + 1, :], channels, 0)))
        columns.append((2 * layer + 1, column(shift_ref[layer : layer + 1, :], channels, 0)))
    for level in range(hist_ref.shape[0]):
        columns.append((BOUND_AT + level, bound_of(hist_ref, level)))
    pad = jnp.zeros((channels - own, 1), f32)
    for place, ref in ((LAST_AT, gain_coarse_ref), (LAST_AT + 1, shift_coarse_ref)):
        columns.append((place, jnp.concatenate([column(ref[1:2, :], own, 0), pad], axis=0)))
    for lane, value in columns:
        params = jnp.where(lanes == lane, value, params)
    param_ref[...] = params
    gain_row_ref[...] = as_row(column(gain_coarse_ref[0:1, :], own, 0), GAIN_AT) + as_row(
        column(shift_coarse_ref[0:1, :], own, 0), SHIFT_AT
    )


def tap_sum(left, middle, right, period):
    lane = lax.broadcasted_iota(jnp.int32, middle.shape, 1) % period
    up = pltpu.roll(left, 1, 1)
    down = pltpu.roll(right, LANES - 1, 1)
    return middle + jnp.where(lane == 0, 0.0, up) + jnp.where(lane == period - 1, 0.0, down)


def slab_kernel(vol_ref, first_ref, second_ref, done):
    depth = vol_ref.shape[2]
    even = lax.axis_index("sz") % 2
    starts = ((1 - even) * (depth - HALO), even * (depth - HALO))
    copies = []
    for which, (start, target) in enumerate(zip(starts, (first_ref, second_ref))):
        source = vol_ref.at[0, :, pl.ds(start, HALO)]
        copies.append(pltpu.make_async_copy(source, target, done.at[which]))
        copies[-1].start()
    for copy in copies:
        copy.wait()


def prep_kernel(vol_ref, hist_ref, cells_ref, peak_ref):
    bound = bound_of(hist_ref, 0).astype(bf16)
    top = jnp.zeros(cells_ref.shape[2:], bf16)
    for z in range(vol_ref.shape[2]):
        rows = jnp.transpose(vol_ref[0, :, z], (1, 0, 2))
        for y in range(rows.shape[0]):
            top = jnp.maximum(top, jnp.abs(rows[y]))
            cells_ref[z, y] = bounded(rows[y], bound)
    peak_ref[...] = jnp.broadcast_to(peak_of(top), (1, LANES))


def sides(axis, first, second):
    at = lax.axis_index(axis)
    count = lax.axis_size(axis)
    even = at % 2 == 0
    blank = jnp.zeros_like(first)
    below = jnp.where(at == 0, blank, jnp.where(even, second, first))
    above = jnp.where(at == count - 1, blank, jnp.where(even, first, second))
    return below, above


def deep_kernel(
    cells_ref,
    got_first_ref,
    got_second_ref,
    param_ref,
    z_first_ref,
    z_second_ref,
    first_ref,
    second_ref,
):
    depth, height = cells_ref.shape[:2]
    bound = clip_bound(param_ref, 0)
    for source, target in ((got_first_ref, z_first_ref), (got_second_ref, z_second_ref)):
        for z in range(HALO):
            rows = jnp.transpose(source[:, z], (1, 0, 2))
            for y in range(height):
                target[z, y] = bounded(rows[y], bound)
    even = lax.axis_index("sy") % 2 == 0
    starts = (jnp.where(even, height - HALO, 0), jnp.where(even, 0, height - HALO))
    odd_z = lax.axis_index("sz") % 2
    far = HALO + depth
    for start, out_ref in zip(starts, (first_ref, second_ref)):
        rows = pl.ds(start, HALO)
        out_ref[pl.ds((1 - odd_z) * far, HALO)] = z_first_ref[:, rows]
        out_ref[pl.ds(odd_z * far, HALO)] = z_second_ref[:, rows]
        out_ref[HALO:far] = cells_ref[:, rows]


def conv_rows(cell, weight, z, rows, out_chan):
    window = jnp.concatenate(
        [
            jnp.concatenate([cell(z + dz, y + dy) for y in rows], axis=1)
            for dz in range(3)
            for dy in range(3)
        ],
        axis=0,
    )
    taps = jnp.dot(weight, window, preferred_element_type=f32)
    outs = []
    for half in range(2):
        part = taps[:, half * LANES : (half + 1) * LANES]
        outs.append(
            tap_sum(
                part[:out_chan], part[out_chan : 2 * out_chan], part[2 * out_chan :], LANES
            )
        )
    return outs


def first_inner_kernel(own_ref, got_first_ref, got_second_ref, weight_ref, deep_ref, raw_ref, sum_ref):
    depth, count, channels = raw_ref.shape[:3]
    own_depth = own_ref.shape[0]
    below, above = sides("sz", got_first_ref[...], got_second_ref[...])
    deep_ref[0:HALO] = below
    deep_ref[HALO : HALO + own_depth] = own_ref[...]
    deep_ref[HALO + own_depth :] = above
    weight = weight_ref[...]
    total = jnp.zeros((channels, LANES), f32)
    square = total
    for z in range(depth):
        for y in range(0, count, 2):
            outs = conv_rows(lambda z, y: deep_ref[z, y], weight, z, (y, y + 1), channels)
            for half in range(2):
                raw_ref[z, y + half] = outs[half]
                if 1 <= z < depth - 1:
                    total = total + outs[half]
                    square = square + outs[half] * outs[half]
    sum_ref[0] = total
    sum_ref[1] = square


def first_outer_kernel(
    deep_ref, got_first_ref, got_second_ref, weight_ref, peak_ref, sum_ref, raw_ref, row_ref, edge_ref
):
    depth, count, channels = raw_ref.shape[:3]
    planes, own_height = deep_ref.shape[:2]
    below, above = sides("sy", got_first_ref[...], got_second_ref[...])
    edge_ref[0] = below
    edge_ref[1] = above

    for at_end, end in (
        (lax.axis_index("sz") == 0, slice(0, HALO)),
        (lax.axis_index("sz") == lax.axis_size("sz") - 1, slice(planes - HALO, planes)),
    ):

        @pl.when(at_end)
        def _():
            edge_ref[:, end] = jnp.zeros((2, HALO) + edge_ref.shape[2:], bf16)

    def cell(z, y):
        if y < HALO:
            return edge_ref[0, z, y]
        if y < HALO + own_height:
            return deep_ref[z, y - HALO]
        return edge_ref[1, z, y - HALO - own_height]

    weight = weight_ref[...]
    total = sum_ref[0]
    square = sum_ref[1]
    last = own_height + 2 - 1
    for z in range(depth):
        for place, rows in ((0, (0, 1)), (2, (last - 1, last))):
            outs = conv_rows(cell, weight, z, rows, channels)
            for half in range(2):
                raw_ref[z, place + half] = outs[half]
                if 1 <= z < depth - 1 and 1 <= rows[half] < last:
                    total = total + outs[half]
                    square = square + outs[half] * outs[half]
    row = as_row(jnp.sum(total, axis=1, keepdims=True), 0)
    row = row + as_row(jnp.sum(square, axis=1, keepdims=True), channels)
    row = row + at_lane(peak_ref[...], PEAK_AT)
    row_ref[...] = jnp.broadcast_to(row[None], row_ref.shape)


def second_kernel(cell_count):
    def kernel(
        inner_ref,
        outer_ref,
        rows_ref,
        weight_ref,
        param_ref,
        gain_row_ref,
        raw_ref,
        load_ref,
        hidden_ref,
        pool_ref,
    ):
        depth, height, channels, width = raw_ref.shape
        wide_depth, wide_height = hidden_ref.shape[:2]
        rows = rows_ref[...]
        merged = jnp.sum(rows, axis=0)
        peak_vol = jnp.max(rows, axis=0)
        scale, offset = affine(
            column(merged, channels, 0),
            column(merged, channels, channels),
            cell_count,
            lane_of(param_ref, 0, channels),
            lane_of(param_ref, 1, channels),
        )
        bound = clip_bound(param_ref, 1)
        at_z = lax.axis_index("sz")
        at_y = lax.axis_index("sy")
        last_z = lax.axis_size("sz") - 1
        last_y = lax.axis_size("sy") - 1
        peak = jnp.zeros((channels, width), bf16)
        for z in range(wide_depth):
            for y in range(wide_height):
                if y < HALO:
                    raw = outer_ref[z, y]
                elif y < height:
                    raw = inner_ref[z, y - HALO]
                else:
                    raw = outer_ref[z, y - height + HALO]
                hidden = activated(raw, scale, offset)
                if 1 <= y < wide_height - 1 and 1 <= z < wide_depth - 1:
                    peak = jnp.maximum(peak, jnp.abs(hidden))
                hidden_ref[z, y] = bounded(hidden, bound)
        outside = (
            (at_z == 0, (slice(0, 1), slice(0, wide_height))),
            (at_z == last_z, (slice(wide_depth - 1, wide_depth), slice(0, wide_height))),
            (at_y == 0, (slice(0, wide_depth), slice(0, 1))),
            (at_y == last_y, (slice(0, wide_depth), slice(wide_height - 1, wide_height))),
        )
        for at_end, (zs, ys) in outside:

            @pl.when(at_end)
            def _():
                count = (zs.stop - zs.start, ys.stop - ys.start)
                hidden_ref[zs, ys] = jnp.zeros(count + (channels, width), bf16)

        blank = jnp.zeros((channels, width), f32)
        weight = weight_ref[...]
        sign = jnp.where(lane_of(param_ref, 2, channels) >= 0, 1.0, -1.0).astype(f32)
        half_height = height // 2
        total, square, least, most = blank, blank, blank + 1e30, blank - 1e30
        for zp in range(depth // 2):
            for yp in range(half_height):
                best = None
                for dz in range(2):
                    z = 2 * zp + dz
                    outs = conv_rows(
                        lambda z, y: hidden_ref[z, y], weight, z, (2 * yp, 2 * yp + 1), channels
                    )
                    for half in range(2):
                        raw_ref[z, 2 * yp + half] = outs[half]
                        total = total + outs[half]
                        square = square + outs[half] * outs[half]
                        signed = outs[half] * sign
                        best = signed if best is None else jnp.maximum(best, signed)
                best = jnp.maximum(best, pltpu.roll(best, LANES - 1, 1)) * sign
                pool_ref[zp, yp] = best
                least = jnp.minimum(least, best)
                most = jnp.maximum(most, best)
        most, least = peak_of(most), -peak_of(-least)
        center = 0.5 * (most + least)
        reach = jnp.maximum(0.5 * (most - least), 1e-30)
        rate = CODE_SPAN / reach
        pick = jnp.where(
            lax.broadcasted_iota(jnp.int32, (2 * LANES, LANES), 0)
            == 2 * lax.broadcasted_iota(jnp.int32, (2 * LANES, LANES), 1),
            1.0,
            0.0,
        ).astype(bf16)
        for zp in range(depth // 2):
            for yq in range(half_height // 2):
                both = jnp.concatenate([pool_ref[zp, 2 * yq], pool_ref[zp, 2 * yq + 1]], axis=1)
                both = jnp.exp((both - center) * rate).astype(bf16)
                load_ref[
                    zp * channels : (zp + 1) * channels, yq * LANES : (yq + 1) * LANES
                ] = jnp.dot(both, pick, preferred_element_type=f32).astype(bf16)
        row = as_row(jnp.sum(total, axis=1, keepdims=True), 0)
        row = row + as_row(jnp.sum(square, axis=1, keepdims=True), channels)
        row = row + at_lane(peak_vol, PEAK_AT)
        row = row + at_lane(peak_of(peak), PEAK_AT + 1)
        row = row + at_lane(center, CODE_AT)
        row = row + at_lane(reach / CODE_SPAN, CODE_AT + 1)
        row = row + gain_row_ref[...]
        high = row.astype(bf16).astype(f32)
        middle = (row - high).astype(bf16).astype(f32)
        low = row - high - middle
        level = lax.broadcasted_iota(jnp.int32, (ROWS, LANES), 0)
        parts = jnp.where(
            level == 0, high, jnp.where(level == 1, middle, jnp.where(level == 2, low, 0.0))
        )
        body = (depth // 2) * channels
        load_ref[body:, 0:LANES] = parts.astype(bf16)
        load_ref[body:, LANES:] = jnp.zeros((ROWS, load_ref.shape[1] - LANES), bf16)

    return kernel


def turned(cells):
    return pltpu.roll(cells, LANES // 2, 1)


def third_kernel(fine_cells, coarse_cells, load_rows, piece):
    def kernel(*refs):
        all_ref, param_ref = refs[:2]
        piece_refs = refs[2:-7]
        raw_ref, peak_ref, affine_ref, next_ref, cells_ref, near_ref, far_ref = refs[-7:]
        y_groups = all_ref.shape[0]
        z_groups = lax.axis_size("sz")
        span = all_ref.shape[2]
        planes, chan_all, flat = raw_ref.shape
        channels = cells_ref.shape[2] // 3
        chan_own = piece // 4
        row_len = LANES // 2
        blocks = flat // LANES
        body = load_rows - ROWS
        z_own = body // channels
        at_z = lax.axis_index("sz")
        totals = jnp.zeros((ROWS, LANES), f32)
        tops = jnp.zeros((1, LANES), f32)
        rows = {}
        for s in range(y_groups):
            for k in range(z_groups):
                parts = all_ref[s, k * load_rows + body : (k + 1) * load_rows, 0:LANES].astype(f32)
                totals = totals + parts
                rows[s, k] = jnp.sum(parts, axis=0, keepdims=True)
                tops = jnp.maximum(tops, rows[s, k])
        merged = jnp.sum(totals, axis=0, keepdims=True)
        scale, offset = affine(
            column(merged, channels, 0),
            column(merged, channels, channels),
            fine_cells,
            lane_of(param_ref, 2, channels),
            lane_of(param_ref, 3, channels),
        )
        lanes = lax.broadcasted_iota(jnp.int32, (channels, LANES), 1)
        affine_ref[...] = jnp.where(lanes == 0, scale, jnp.where(lanes == 1, offset, 0.0))
        bound = clip_bound(param_ref, 2)
        lower = lanes < row_len
        edge = lanes % row_len
        blank = jnp.zeros((channels, LANES), bf16)
        middle = slice(channels, 2 * channels)

        def at_block(block):
            return slice(block * LANES, (block + 1) * LANES)

        def keep(place, block, value):
            cells_ref[place, block, middle] = value
            if block >= 2:
                cells_ref[place, block, :channels] = jnp.where(
                    edge == 0, blank, pltpu.roll(value, 1, 1)
                )
                cells_ref[place, block, 2 * channels :] = jnp.where(
                    edge == row_len - 1, blank, pltpu.roll(value, LANES - 1, 1)
                )

        peak_pool = jnp.zeros((channels, span), bf16)
        half_groups = y_groups // 2
        for k in range(z_groups):
            for zp in range(z_own):
                place = (at_z ^ k) * z_own + zp
                at = k * load_rows + zp * channels
                ends = []
                for s in range(half_groups):
                    both = []
                    for own in (s, s + half_groups):
                        center = rows[own, k][:, CODE_AT : CODE_AT + 1]
                        reach = rows[own, k][:, CODE_AT + 1 : CODE_AT + 2]
                        code = jnp.log(all_ref[own, at : at + channels, :].astype(f32))
                        value = activated(code, scale * reach, scale * center + offset)
                        peak_pool = jnp.maximum(peak_pool, jnp.abs(value))
                        both.append(bounded(value, bound))
                    for q in range(span // LANES):
                        low, high = (one[:, at_block(q)] for one in both)
                        block = s * (span // row_len) + 2 * q
                        one = jnp.where(lower, low, turned(high))
                        two = jnp.where(lower, turned(low), high)
                        keep(place, block + 1, one)
                        keep(place, block + 2, two)
                        if block == 0:
                            ends.append((blocks + 1, jnp.where(lower, turned(one), blank)))
                        if block + 2 == blocks:
                            ends.append((0, jnp.where(lower, blank, turned(two))))
                for block, value in ends:
                    keep(place, block, value)
        main = 3 * chan_own
        at_y = lax.axis_index("sy")
        for k, piece_ref in enumerate(piece_refs):
            near_ref[pl.ds((at_y ^ k) * main, main), :] = piece_ref[:main, :]
            far_ref[pl.ds((at_y ^ k) * chan_own, chan_own), :] = piece_ref[main:, : 3 * channels]
        near_weight = near_ref[...]
        far_weight = far_ref[...]
        blank = jnp.zeros((chan_own, LANES), f32)
        totals = [blank for _ in range(y_groups)]
        squares = [blank for _ in range(y_groups)]
        leasts = [blank + 1e30 for _ in range(y_groups)]
        mosts = [blank - 1e30 for _ in range(y_groups)]
        for z in range(planes):
            for t in range(blocks // 2):
                depths = [dz for dz in range(3) if 0 <= z + dz - 1 < planes]

                def cells(dz, dy, which):
                    return jnp.concatenate(
                        [cells_ref[z + dz - 1, 2 * t + dy + half, which] for half in range(2)],
                        axis=1,
                    )

                window = [
                    cells(dz, dy, middle) for dz in depths for dy in range(3) if dz + dy < 4
                ]
                first = 3 * depths[0] * channels
                taps = jnp.dot(
                    near_weight[:, first : first + len(window) * channels],
                    jnp.concatenate(window, axis=0),
                    preferred_element_type=f32,
                )
                rest = None
                if depths[-1] == 2:
                    rest = jnp.dot(
                        far_weight, cells(2, 2, slice(None)), preferred_element_type=f32
                    )
                for s in range(y_groups):
                    for half in range(2):
                        at = s * main
                        part = taps[at : at + main, at_block(half)]
                        center = part[chan_own : 2 * chan_own]
                        if rest is not None:
                            own = slice(s * chan_own, (s + 1) * chan_own)
                            center = center + rest[own, at_block(half)]
                        out = tap_sum(part[:chan_own], center, part[2 * chan_own :], row_len)
                        raw_ref[
                            z, s * chan_own : (s + 1) * chan_own, at_block(2 * t + half)
                        ] = out
                        totals[s] = totals[s] + out
                        squares[s] = squares[s] + out * out
                        leasts[s] = jnp.minimum(leasts[s], out)
                        mosts[s] = jnp.maximum(mosts[s], out)
        pairs = [
            affine(
                jnp.sum(totals[s], axis=1, keepdims=True),
                jnp.sum(squares[s], axis=1, keepdims=True),
                coarse_cells,
                column(rows[s, 0], chan_own, GAIN_AT),
                column(rows[s, 0], chan_own, SHIFT_AT),
            )
            for s in range(y_groups)
        ]
        scale = jnp.concatenate([one[0] for one in pairs], axis=0)
        offset = jnp.concatenate([one[1] for one in pairs], axis=0)
        lanes = lax.broadcasted_iota(jnp.int32, (chan_all, LANES), 1)
        next_ref[...] = jnp.where(lanes == 0, scale, jnp.where(lanes == 1, offset, 0.0))
        peak = jnp.zeros((chan_all, LANES), bf16)
        for extreme in (leasts, mosts):
            value = activated(jnp.concatenate(extreme, axis=0), scale, offset)
            peak = jnp.maximum(peak, jnp.abs(value))
        row = at_lane(tops[:, PEAK_AT : PEAK_AT + 1], 0)
        row = row + at_lane(tops[:, PEAK_AT + 1 : PEAK_AT + 2], 1)
        row = row + at_lane(peak_of(peak_pool), 2)
        row = row + at_lane(peak_of(peak), 3)
        peak_ref[...] = row[:, : peak_ref.shape[1]]

    return kernel


def fourth_kernel(coarse_cells):
    def kernel(
        raw_ref,
        weight_ref,
        param_ref,
        affine_ref,
        next_ref,
        fine_ref,
        out_ref,
        skip_ref,
        cells_ref,
        last_ref,
        narrow_ref,
        done,
    ):
        scale = affine_ref[:, 0:1]
        offset = affine_ref[:, 1:2]
        sends = []
        for z in range(fine_ref.shape[0]):
            act = jnp.stack(
                [activated(fine_ref[z, y], scale, offset) for y in range(fine_ref.shape[1])]
            )
            narrow_ref[:, z] = jnp.transpose(act, (1, 0, 2))
            sends.append(
                pltpu.make_async_copy(narrow_ref.at[:, z], skip_ref.at[0, :, z], done.at[z])
            )
            sends[-1].start()
        planes, chan_all, flat = cells_ref.shape
        chan_own, z_own = out_ref.shape[:2]
        row_len = LANES // 2
        blocks = flat // LANES
        weight = weight_ref[...]
        lower = lax.broadcasted_iota(jnp.int32, (chan_own, LANES), 1) < row_len
        blank = jnp.zeros((chan_own, LANES), f32)
        bound = clip_bound(param_ref, 3)
        scale = next_ref[:, 0:1]
        offset = next_ref[:, 1:2]

        def at_block(block):
            return slice(block * LANES, (block + 1) * LANES)

        def normed(z):
            for j in range(blocks):
                value = activated(raw_ref[z, :, at_block(j)], scale, offset)
                cells_ref[z, :, at_block(j)] = bounded(value, bound)

        def plane(z, sums):
            total, square = sums
            depths = [dz for dz in range(3) if 0 <= z + dz - 1 < planes]
            columns = slice(depths[0] * chan_all, (depths[-1] + 1) * chan_all)
            parts = []
            for t in range(blocks // 2):
                window = jnp.concatenate(
                    [
                        cells_ref[z + dz - 1, :, 2 * t * LANES : 2 * (t + 1) * LANES]
                        for dz in depths
                    ],
                    axis=0,
                )
                taps = jnp.dot(weight[:, columns], window, preferred_element_type=f32)
                parts.extend(taps[:, at_block(half)] for half in range(2))

            def tap(dy, dx, j):
                at = (3 * dy + dx) * chan_own
                return parts[j][at : at + chan_own]

            for j in range(blocks):
                three = []
                for dx in range(3):
                    if j > 0:
                        before = tap(0, dx, j - 1)
                    else:
                        before = jnp.where(lower, blank, turned(tap(0, dx, blocks - 1)))
                    if j + 1 < blocks:
                        after = tap(2, dx, j + 1)
                    else:
                        after = jnp.where(lower, turned(tap(2, dx, 0)), blank)
                    three.append(tap(1, dx, j) + before + after)
                out = tap_sum(*three, row_len)
                last_ref[z, :, at_block(j)] = out
                total = total + out
                square = square + out * out
            return total, square

        sums = (blank, blank)
        normed(0)
        for z in range(planes):
            if z + 1 < planes:
                normed(z + 1)
            sums = plane(z, sums)
        total, square = sums
        scale, offset = affine(
            jnp.sum(total, axis=1, keepdims=True),
            jnp.sum(square, axis=1, keepdims=True),
            coarse_cells,
            lane_of(param_ref, LAST_AT, chan_own),
            lane_of(param_ref, LAST_AT + 1, chan_own),
        )
        at_z = lax.axis_index("sz")
        own = []
        for i in range(z_own):
            cells = activated(last_ref[at_z * z_own + i], scale, offset).astype(f32)
            natural = []
            for p in range(blocks):
                row = (2 * p) % blocks
                first, second = cells[:, at_block(row)], cells[:, at_block(row + 1)]
                if 2 * p < blocks:
                    natural.append(jnp.where(lower, first, turned(second)))
                else:
                    natural.append(jnp.where(lower, turned(first), second))
            own.append(jnp.concatenate(natural, axis=1))
        for c in range(chan_own):
            out_ref[c] = jnp.concatenate([one[c : c + 1] for one in own], axis=0).astype(bf16)
        for send in sends:
            send.wait()

    return kernel


def final_kernel(*refs):
    cells_ref, peak_ref = refs[:2]
    out_ref, top_ref = refs[-2:]
    out_ref[0] = cells_ref[...]
    top = peak_ref[...]
    for ref in refs[2:-2]:
        top = jnp.maximum(top, ref[...])
    top_ref[...] = top


def shape(dims, dtype):
    return jax.ShapeDtypeStruct(dims, dtype)


def near_shape(dims, dtype):
    return pltpu.VMEM(dims, dtype)


def held(value):
    return pltpu.with_memory_space_constraint(value, pltpu.VMEM)


def per_device(
    volume,
    amax_history,
    conv_first,
    conv_second,
    conv_third,
    conv_fourth,
    gain_fine,
    shift_fine,
    gain_coarse,
    shift_coarse,
):
    channels, depth, height, width = volume.shape[1:]
    z_groups = lax.axis_size("sz")
    y_groups = lax.axis_size("sy")
    samples = lax.axis_size("sample")
    fine_cells = float(depth * z_groups * height * y_groups * width)
    coarse_cells = fine_cells / 8
    chan_own = conv_third.shape[1]
    chan_all = conv_fourth.shape[2]
    span = (height // 2) * (width // 2)
    planes = (depth // 2) * z_groups
    flat = span * y_groups
    group = z_groups * y_groups
    load_rows = (depth // 2) * channels + ROWS

    anywhere = pl.BlockSpec(memory_space=pl.ANY)
    near = pl.BlockSpec(memory_space=pltpu.VMEM)
    z_first, z_second = pl.pallas_call(
        slab_kernel,
        in_specs=[anywhere],
        out_specs=(near, near),
        out_shape=(
            near_shape((channels, HALO, height, width), bf16),
            near_shape((channels, HALO, height, width), bf16),
        ),
        scratch_shapes=[pltpu.SemaphoreType.DMA((2,))],
        name="slabs",
    )(volume)
    cells, peak = pl.pallas_call(
        prep_kernel,
        out_shape=(
            near_shape((depth, height, channels, width), bf16),
            near_shape((1, LANES), f32),
        ),
        name="prep",
    )(volume, amax_history)
    third_rows = 4 * chan_own
    m1, m2, m3, m4, params, gain_row = pl.pallas_call(
        matrix_kernel,
        out_shape=(
            near_shape((3 * channels, 9 * channels), bf16),
            near_shape((3 * channels, 9 * channels), bf16),
            near_shape((third_rows, 8 * channels), bf16),
            near_shape((9 * chan_own, 3 * chan_all), bf16),
            near_shape((channels, LANES), f32),
            near_shape((1, LANES), f32),
        ),
        name="matrices",
    )(
        held(peak),
        conv_first,
        conv_second,
        conv_third,
        conv_fourth,
        amax_history,
        gain_fine,
        shift_fine,
        gain_coarse,
        shift_coarse,
    )
    pieces = [m3]
    for k in range(1, y_groups):
        pieces.append(lax.ppermute(m3, "sy", [(i, i ^ k) for i in range(y_groups)]))
    pair_first, pair_second = pairings("sz")
    z_first = lax.ppermute(z_first, "sz", pair_first)
    z_second = lax.ppermute(z_second, "sz", pair_second)
    deep_depth = depth + 2 * HALO
    levels = amax_history.shape[0]
    z_first, z_second, first, second = pl.pallas_call(
        deep_kernel,
        out_shape=(
            near_shape((HALO, height, channels, width), bf16),
            near_shape((HALO, height, channels, width), bf16),
            near_shape((deep_depth, HALO, channels, width), bf16),
            near_shape((deep_depth, HALO, channels, width), bf16),
        ),
        name="deep",
    )(*(held(x) for x in (cells, z_first, z_second, params)))
    pair_first, pair_second = pairings("sy")
    y_first = lax.ppermute(first, "sy", pair_first)
    y_second = lax.ppermute(second, "sy", pair_second)
    deep, raw_inner, sums = pl.pallas_call(
        first_inner_kernel,
        out_shape=(
            near_shape((deep_depth, height, channels, width), bf16),
            near_shape((depth + 2, height - 2, channels, width), f32),
            near_shape((2, channels, LANES), f32),
        ),
        name="first_inner",
    )(*(held(x) for x in (cells, z_first, z_second, m1)))
    raw_outer, row = pl.pallas_call(
        first_outer_kernel,
        out_shape=(
            near_shape((depth + 2, 2 * HALO, channels, width), f32),
            near_shape((group, 1, LANES), f32),
        ),
        scratch_shapes=[pltpu.VMEM((2, deep_depth, HALO, channels, width), bf16)],
        name="first_outer",
    )(*(held(x) for x in (deep, y_first, y_second, m1, peak, sums)))
    rows = lax.all_to_all(row, ("sy", "sz"), 0, 0, tiled=True)
    raw_second, load = pl.pallas_call(
        second_kernel(fine_cells),
        out_shape=(
            near_shape((depth, height, channels, width), f32),
            near_shape((load_rows, span), bf16),
        ),
        scratch_shapes=[
            pltpu.VMEM((depth + 2, height + 2, channels, width), bf16),
            pltpu.VMEM((depth // 2, height // 2, channels, width), f32),
        ],
        compiler_params=pltpu.CompilerParams(vmem_limit_bytes=KERNEL_BYTES),
        name="second",
    )(*(held(x) for x in (raw_inner, raw_outer, rows, m2, params, gain_row)))
    loads = [load]
    for k in range(1, z_groups):
        loads.append(lax.ppermute(load, "sz", [(i, i ^ k) for i in range(z_groups)]))
    gathered = lax.all_gather(jnp.concatenate(loads, axis=0), "sy", axis=0)
    raw_third, peaks, fine_affine, next_affine = pl.pallas_call(
        third_kernel(fine_cells, coarse_cells, load_rows, third_rows),
        out_shape=(
            near_shape((planes, chan_all, flat), f32),
            near_shape((1, levels), f32),
            near_shape((channels, LANES), f32),
            near_shape((chan_all, LANES), f32),
        ),
        scratch_shapes=[
            pltpu.VMEM((planes, flat // LANES + 2, 3 * channels, LANES), bf16),
            pltpu.VMEM((3 * chan_all, 8 * channels), bf16),
            pltpu.VMEM((chan_all, 3 * channels), bf16),
        ],
        compiler_params=pltpu.CompilerParams(vmem_limit_bytes=KERNEL_BYTES),
        name="third",
    )(*(held(x) for x in (gathered, params, *pieces)))
    if samples <= 4:
        others = [
            lax.ppermute(peaks, "sample", [(i, (i + k) % samples) for i in range(samples)])
            for k in range(1, samples)
        ]
    else:
        others = [lax.pmax(peaks, "sample")]
    coarse, skip = pl.pallas_call(
        fourth_kernel(coarse_cells),
        out_shape=(
            near_shape((chan_own, depth // 2, flat), bf16),
            shape((1, channels, depth, height, width), bf16),
        ),
        out_specs=(near, anywhere),
        scratch_shapes=[
            pltpu.VMEM((planes, chan_all, flat), bf16),
            pltpu.VMEM((planes, chan_own, flat), f32),
            pltpu.VMEM((channels, depth, height, width), bf16),
            pltpu.SemaphoreType.DMA((depth,)),
        ],
        compiler_params=pltpu.CompilerParams(vmem_limit_bytes=KERNEL_BYTES),
        name="fourth",
    )(*(held(x) for x in (raw_third, m4, params, fine_affine, next_affine, raw_second)))
    coarse, peaks = pl.pallas_call(
        final_kernel,
        out_shape=(
            shape((1, chan_own, depth // 2, flat), bf16),
            shape((1, levels), f32),
        ),
        name="final",
    )(*(held(x) for x in (coarse, peaks, *others)))
    return skip, coarse, peaks.reshape(levels)


def solution(mesh):
    return jax.shard_map(
        per_device,
        mesh=mesh,
        in_specs=(
            P("sample", None, "sz", "sy", None),
            P(),
            P(),
            P(),
            P(None, "sy", None),
            P(None, "sy", None),
            P(),
            P(),
            P(None, "sy"),
            P(None, "sy"),
        ),
        out_specs=(P("sample", None, "sz", "sy", None), P("sample", "sy", "sz", None), P()),
        check_vma=False,
    )
```

```python
import jax
import jax.numpy as jnp
from jax import lax
from jax.experimental import pallas as pl
from jax.experimental.pallas import tpu as pltpu
from jax.sharding import PartitionSpec as P

norm_eps = 1e-05
leak_slope = 0.01
f32 = jnp.float32
bf16 = jnp.bfloat16
LANES = 128
HALO = 2
SLAB_PARTS = 4
KERNEL_BYTES = 24 * 1024 * 1024
PEAK_AT = 64
CODE_AT = 66
GAIN_AT = 80
SHIFT_AT = 96
CODE_SPAN = 83.0
ROWS = 8


def pairings(axis):
    count = lax.axis_size(axis)
    first = [(i, i ^ 1) for i in range(count)]
    second = [(i, min(max(((i + 1) ^ 1) - 1, 0), count - 1)) for i in range(count)]
    return first, second


def column(row, channels, start):
    lanes = lax.broadcasted_iota(jnp.int32, (channels, row.shape[1]), 1)
    chans = lax.broadcasted_iota(jnp.int32, (channels, row.shape[1]), 0)
    return jnp.sum(jnp.where(lanes == chans + start, row, 0.0), axis=1, keepdims=True)


def as_row(col, start):
    channels = col.shape[0]
    lanes = lax.broadcasted_iota(jnp.int32, (channels, LANES), 1)
    chans = lax.broadcasted_iota(jnp.int32, (channels, LANES), 0)
    return jnp.sum(jnp.where(lanes == chans + start, col, 0.0), axis=0, keepdims=True)


def at_lane(value, lane):
    lanes = lax.broadcasted_iota(jnp.int32, (1, LANES), 1)
    return jnp.where(lanes == lane, value, 0.0)


def affine(total, square, cells, gains, offset):
    mean = total / cells
    spread = square / cells - mean * mean
    scale = lax.rsqrt(spread + norm_eps) * gains
    return scale, offset - mean * scale


def activated(values, scale, offset):
    normed = values * scale + offset
    return jnp.maximum(normed, leak_slope * normed).astype(bf16)


def peak_of(values):
    values = values.astype(f32)
    return jnp.max(jnp.max(values, axis=0, keepdims=True), axis=1, keepdims=True)


def bounded(values, bound):
    return jnp.minimum(jnp.maximum(values, -bound), bound)


BOUND_AT = 4
LAST_AT = 8


def bound_of(hist_ref, level):
    return jnp.max(hist_ref[level : level + 1, :], axis=1, keepdims=True)


def lane_of(param_ref, lane, channels):
    return param_ref[0:channels, lane : lane + 1]


def clip_bound(param_ref, level):
    return param_ref[0:1, BOUND_AT + level : BOUND_AT + level + 1].astype(bf16)


def matrix_of(weight, taps_ref, groups):
    out_chan = weight.shape[1]
    for dx in range(3):
        taps_ref[dx * out_chan : (dx + 1) * out_chan, :] = jnp.concatenate(
            [weight[3 * j + dx] for j in groups], axis=1
        )


def matrix_kernel(
    peak_ref,
    first_ref,
    second_ref,
    third_ref,
    fourth_ref,
    hist_ref,
    gain_ref,
    shift_ref,
    gain_coarse_ref,
    shift_coarse_ref,
    m1_ref,
    m2_ref,
    m3_ref,
    m4_ref,
    param_ref,
    gain_row_ref,
):
    taps = first_ref.shape[0]
    matrix_of(first_ref, m1_ref, range(taps // 3))
    matrix_of(second_ref, m2_ref, range(taps // 3))
    own = third_ref.shape[1]
    matrix_of(third_ref, m3_ref.at[0 : 3 * own], range(taps // 3 - 1))
    last = [third_ref[taps - 3 + dx] for dx in range(3)]
    rest = m3_ref.shape[1] - 3 * third_ref.shape[2]
    m3_ref[3 * own :, :] = jnp.concatenate(last + [jnp.zeros((own, rest), bf16)], axis=1)
    for dy in range(3):
        for dx in range(3):
            at = (3 * dy + dx) * own
            m4_ref[at : at + own, :] = jnp.concatenate(
                [fourth_ref[9 * dz + 3 * dy + dx] for dz in range(3)], axis=1
            )
    channels = param_ref.shape[0]
    lanes = lax.broadcasted_iota(jnp.int32, (channels, LANES), 1)
    params = jnp.zeros((channels, LANES), f32)
    columns = []
    for layer in range(2):
        columns.append((2 * layer, column(gain_ref[layer : layer + 1, :], channels, 0)))
        columns.append((2 * layer + 1, column(shift_ref[layer : layer + 1, :], channels, 0)))
    for level in range(hist_ref.shape[0]):
        columns.append((BOUND_AT + level, bound_of(hist_ref, level)))
    pad = jnp.zeros((channels - own, 1), f32)
    for place, ref in ((LAST_AT, gain_coarse_ref), (LAST_AT + 1, shift_coarse_ref)):
        columns.append((place, jnp.concatenate([column(ref[1:2, :], own, 0), pad], axis=0)))
    for lane, value in columns:
        params = jnp.where(lanes == lane, value, params)
    param_ref[...] = params
    gain_row_ref[...] = as_row(column(gain_coarse_ref[0:1, :], own, 0), GAIN_AT) + as_row(
        column(shift_coarse_ref[0:1, :], own, 0), SHIFT_AT
    )


def tap_sum(left, middle, right, period):
    lane = lax.broadcasted_iota(jnp.int32, middle.shape, 1) % period
    up = pltpu.roll(left, 1, 1)
    down = pltpu.roll(right, LANES - 1, 1)
    return middle + jnp.where(lane == 0, 0.0, up) + jnp.where(lane == period - 1, 0.0, down)


def slab_kernel(vol_ref, first_ref, second_ref, done):
    depth = vol_ref.shape[2]
    even = lax.axis_index("sz") % 2
    starts = ((1 - even) * (depth - HALO), even * (depth - HALO))
    copies = []
    group = first_ref.shape[0] // SLAB_PARTS
    for start, target in zip(starts, (first_ref, second_ref)):
        for part in range(SLAB_PARTS):
            own = slice(part * group, (part + 1) * group)
            source = vol_ref.at[0, own, pl.ds(start, HALO)]
            copies.append(pltpu.make_async_copy(source, target.at[own], done.at[len(copies)]))
            copies[-1].start()
    for copy in copies:
        copy.wait()


def prep_kernel(vol_ref, hist_ref, cells_ref, peak_ref):
    bound = bound_of(hist_ref, 0).astype(bf16)
    top = jnp.zeros(cells_ref.shape[2:], bf16)
    for z in range(vol_ref.shape[2]):
        rows = jnp.transpose(vol_ref[0, :, z], (1, 0, 2))
        for y in range(rows.shape[0]):
            top = jnp.maximum(top, jnp.abs(rows[y]))
            cells_ref[z, y] = bounded(rows[y], bound)
    peak_ref[...] = jnp.broadcast_to(peak_of(top), (1, LANES))


def sides(axis, first, second):
    at = lax.axis_index(axis)
    count = lax.axis_size(axis)
    even = at % 2 == 0
    blank = jnp.zeros_like(first)
    below = jnp.where(at == 0, blank, jnp.where(even, second, first))
    above = jnp.where(at == count - 1, blank, jnp.where(even, first, second))
    return below, above


def deep_kernel(
    cells_ref,
    got_first_ref,
    got_second_ref,
    param_ref,
    z_first_ref,
    z_second_ref,
    first_ref,
    second_ref,
):
    depth, height = cells_ref.shape[:2]
    bound = clip_bound(param_ref, 0)
    for source, target in ((got_first_ref, z_first_ref), (got_second_ref, z_second_ref)):
        for z in range(HALO):
            rows = jnp.transpose(source[:, z], (1, 0, 2))
            for y in range(height):
                target[z, y] = bounded(rows[y], bound)
    even = lax.axis_index("sy") % 2 == 0
    starts = (jnp.where(even, height - HALO, 0), jnp.where(even, 0, height - HALO))
    odd_z = lax.axis_index("sz") % 2
    far = HALO + depth
    for start, out_ref in zip(starts, (first_ref, second_ref)):
        rows = pl.ds(start, HALO)
        out_ref[pl.ds((1 - odd_z) * far, HALO)] = z_first_ref[:, rows]
        out_ref[pl.ds(odd_z * far, HALO)] = z_second_ref[:, rows]
        out_ref[HALO:far] = cells_ref[:, rows]


def conv_rows(cell, weight, z, rows, out_chan):
    window = jnp.concatenate(
        [
            jnp.concatenate([cell(z + dz, y + dy) for y in rows], axis=1)
            for dz in range(3)
            for dy in range(3)
        ],
        axis=0,
    )
    taps = jnp.dot(weight, window, preferred_element_type=f32)
    outs = []
    for half in range(2):
        part = taps[:, half * LANES : (half + 1) * LANES]
        outs.append(
            tap_sum(
                part[:out_chan], part[out_chan : 2 * out_chan], part[2 * out_chan :], LANES
            )
        )
    return outs


def first_inner_kernel(own_ref, got_first_ref, got_second_ref, weight_ref, deep_ref, raw_ref, sum_ref):
    depth, count, channels = raw_ref.shape[:3]
    own_depth = own_ref.shape[0]
    below, above = sides("sz", got_first_ref[...], got_second_ref[...])
    deep_ref[0:HALO] = below
    deep_ref[HALO : HALO + own_depth] = own_ref[...]
    deep_ref[HALO + own_depth :] = above
    weight = weight_ref[...]
    total = jnp.zeros((channels, LANES), f32)
    square = total
    for z in range(depth):
        for y in range(0, count, 2):
            outs = conv_rows(lambda z, y: deep_ref[z, y], weight, z, (y, y + 1), channels)
            for half in range(2):
                raw_ref[z, y + half] = outs[half]
                if 1 <= z < depth - 1:
                    total = total + outs[half]
                    square = square + outs[half] * outs[half]
    sum_ref[0] = total
    sum_ref[1] = square


def first_outer_kernel(
    deep_ref, got_first_ref, got_second_ref, weight_ref, peak_ref, sum_ref, raw_ref, row_ref, edge_ref
):
    depth, count, channels = raw_ref.shape[:3]
    planes, own_height = deep_ref.shape[:2]
    below, above = sides("sy", got_first_ref[...], got_second_ref[...])
    at_z = lax.axis_index("sz")
    lowest = jnp.where(at_z > 0, 1.0, 0.0).astype(bf16)
    highest = jnp.where(at_z < lax.axis_size("sz") - 1, 1.0, 0.0).astype(bf16)
    for side, cells in enumerate((below, above)):
        edge_ref[side, :HALO] = cells[:HALO] * lowest
        edge_ref[side, HALO : planes - HALO] = cells[HALO : planes - HALO]
        edge_ref[side, planes - HALO :] = cells[planes - HALO :] * highest

    def cell(z, y):
        if y < HALO:
            return edge_ref[0, z, y]
        if y < HALO + own_height:
            return deep_ref[z, y - HALO]
        return edge_ref[1, z, y - HALO - own_height]

    weight = weight_ref[...]
    total = sum_ref[0]
    square = sum_ref[1]
    last = own_height + 2 - 1
    for z in range(depth):
        for place, rows in ((0, (0, 1)), (2, (last - 1, last))):
            outs = conv_rows(cell, weight, z, rows, channels)
            for half in range(2):
                raw_ref[z, place + half] = outs[half]
                if 1 <= z < depth - 1 and 1 <= rows[half] < last:
                    total = total + outs[half]
                    square = square + outs[half] * outs[half]
    row = as_row(jnp.sum(total, axis=1, keepdims=True), 0)
    row = row + as_row(jnp.sum(square, axis=1, keepdims=True), channels)
    row = row + at_lane(peak_ref[...], PEAK_AT)
    row_ref[...] = jnp.broadcast_to(row[None], row_ref.shape)


def second_kernel(cell_count):
    def kernel(
        inner_ref,
        outer_ref,
        rows_ref,
        weight_ref,
        param_ref,
        gain_row_ref,
        raw_ref,
        load_ref,
        hidden_ref,
        pool_ref,
    ):
        depth, height, channels, width = raw_ref.shape
        wide_depth, wide_height = hidden_ref.shape[:2]
        rows = rows_ref[...]
        merged = jnp.sum(rows, axis=0)
        peak_vol = jnp.max(rows, axis=0)
        scale, offset = affine(
            column(merged, channels, 0),
            column(merged, channels, channels),
            cell_count,
            lane_of(param_ref, 0, channels),
            lane_of(param_ref, 1, channels),
        )
        bound = clip_bound(param_ref, 1)
        at_z = lax.axis_index("sz")
        at_y = lax.axis_index("sy")
        last_z = lax.axis_size("sz") - 1
        last_y = lax.axis_size("sy") - 1

        def one_if(inside):
            return jnp.where(inside, 1.0, 0.0).astype(bf16)

        edges_z = (one_if(at_z > 0), one_if(at_z < last_z))
        edges_y = (one_if(at_y > 0), one_if(at_y < last_y))
        peak = jnp.zeros((channels, width), bf16)
        for z in range(wide_depth):
            for y in range(wide_height):
                if y < HALO:
                    raw = outer_ref[z, y]
                elif y < height:
                    raw = inner_ref[z, y - HALO]
                else:
                    raw = outer_ref[z, y - height + HALO]
                hidden = activated(raw, scale, offset)
                if 1 <= y < wide_height - 1 and 1 <= z < wide_depth - 1:
                    peak = jnp.maximum(peak, jnp.abs(hidden))
                hidden = bounded(hidden, bound)
                for place, last, edges in ((z, wide_depth - 1, edges_z), (y, wide_height - 1, edges_y)):
                    if place in (0, last):
                        hidden = hidden * edges[place == last]
                hidden_ref[z, y] = hidden
        blank = jnp.zeros((channels, width), f32)
        weight = weight_ref[...]
        sign = jnp.where(lane_of(param_ref, 2, channels) >= 0, 1.0, -1.0).astype(f32)
        half_height = height // 2
        total, square, least, most = blank, blank, blank + 1e30, blank - 1e30
        for zp in range(depth // 2):
            for yp in range(half_height):
                best = None
                for dz in range(2):
                    z = 2 * zp + dz
                    outs = conv_rows(
                        lambda z, y: hidden_ref[z, y], weight, z, (2 * yp, 2 * yp + 1), channels
                    )
                    for half in range(2):
                        raw_ref[z, 2 * yp + half] = outs[half]
                        total = total + outs[half]
                        square = square + outs[half] * outs[half]
                        signed = outs[half] * sign
                        best = signed if best is None else jnp.maximum(best, signed)
                best = jnp.maximum(best, pltpu.roll(best, LANES - 1, 1)) * sign
                pool_ref[zp, yp] = best
                least = jnp.minimum(least, best)
                most = jnp.maximum(most, best)
        most, least = peak_of(most), -peak_of(-least)
        center = 0.5 * (most + least)
        reach = jnp.maximum(0.5 * (most - least), 1e-30)
        rate = CODE_SPAN / reach
        pick = jnp.where(
            lax.broadcasted_iota(jnp.int32, (2 * LANES, LANES), 0)
            == 2 * lax.broadcasted_iota(jnp.int32, (2 * LANES, LANES), 1),
            1.0,
            0.0,
        ).astype(bf16)
        for zp in range(depth // 2):
            for yq in range(half_height // 2):
                both = jnp.concatenate([pool_ref[zp, 2 * yq], pool_ref[zp, 2 * yq + 1]], axis=1)
                both = jnp.exp((both - center) * rate).astype(bf16)
                load_ref[
                    zp * channels : (zp + 1) * channels, yq * LANES : (yq + 1) * LANES
                ] = jnp.dot(both, pick, preferred_element_type=f32).astype(bf16)
        row = as_row(jnp.sum(total, axis=1, keepdims=True), 0)
        row = row + as_row(jnp.sum(square, axis=1, keepdims=True), channels)
        row = row + at_lane(peak_vol, PEAK_AT)
        row = row + at_lane(peak_of(peak), PEAK_AT + 1)
        row = row + at_lane(center, CODE_AT)
        row = row + at_lane(reach / CODE_SPAN, CODE_AT + 1)
        row = row + gain_row_ref[...]
        high = row.astype(bf16).astype(f32)
        middle = (row - high).astype(bf16).astype(f32)
        low = row - high - middle
        level = lax.broadcasted_iota(jnp.int32, (ROWS, LANES), 0)
        parts = jnp.where(
            level == 0, high, jnp.where(level == 1, middle, jnp.where(level == 2, low, 0.0))
        )
        body = (depth // 2) * channels
        load_ref[body:, 0:LANES] = parts.astype(bf16)
        load_ref[body:, LANES:] = jnp.zeros((ROWS, load_ref.shape[1] - LANES), bf16)

    return kernel


def turned(cells):
    return pltpu.roll(cells, LANES // 2, 1)


def third_kernel(fine_cells, coarse_cells, load_rows, piece):
    def kernel(*refs):
        all_ref, param_ref = refs[:2]
        piece_refs = refs[2:-7]
        raw_ref, peak_ref, affine_ref, next_ref, cells_ref, near_ref, far_ref = refs[-7:]
        y_groups = all_ref.shape[0]
        z_groups = lax.axis_size("sz")
        span = all_ref.shape[2]
        planes, chan_all, flat = raw_ref.shape
        channels = cells_ref.shape[2] // 3
        chan_own = piece // 4
        row_len = LANES // 2
        blocks = flat // LANES
        body = load_rows - ROWS
        z_own = body // channels
        at_z = lax.axis_index("sz")
        totals = jnp.zeros((ROWS, LANES), f32)
        tops = jnp.zeros((1, LANES), f32)
        rows = {}
        for s in range(y_groups):
            for k in range(z_groups):
                parts = all_ref[s, k * load_rows + body : (k + 1) * load_rows, 0:LANES].astype(f32)
                totals = totals + parts
                rows[s, k] = jnp.sum(parts, axis=0, keepdims=True)
                tops = jnp.maximum(tops, rows[s, k])
        merged = jnp.sum(totals, axis=0, keepdims=True)
        scale, offset = affine(
            column(merged, channels, 0),
            column(merged, channels, channels),
            fine_cells,
            lane_of(param_ref, 2, channels),
            lane_of(param_ref, 3, channels),
        )
        lanes = lax.broadcasted_iota(jnp.int32, (channels, LANES), 1)
        affine_ref[...] = jnp.where(lanes == 0, scale, jnp.where(lanes == 1, offset, 0.0))
        bound = clip_bound(param_ref, 2)
        lower = lanes < row_len
        edge = lanes % row_len
        blank = jnp.zeros((channels, LANES), bf16)
        middle = slice(channels, 2 * channels)

        def at_block(block):
            return slice(block * LANES, (block + 1) * LANES)

        def keep(place, block, value):
            cells_ref[place, block, middle] = value
            if block >= 2:
                cells_ref[place, block, :channels] = jnp.where(
                    edge == 0, blank, pltpu.roll(value, 1, 1)
                )
                cells_ref[place, block, 2 * channels :] = jnp.where(
                    edge == row_len - 1, blank, pltpu.roll(value, LANES - 1, 1)
                )

        peak_pool = jnp.zeros((channels, span), bf16)
        half_groups = y_groups // 2
        for k in range(z_groups):
            for zp in range(z_own):
                place = (at_z ^ k) * z_own + zp
                at = k * load_rows + zp * channels
                ends = []
                for s in range(half_groups):
                    both = []
                    for own in (s, s + half_groups):
                        center = rows[own, k][:, CODE_AT : CODE_AT + 1]
                        reach = rows[own, k][:, CODE_AT + 1 : CODE_AT + 2]
                        code = jnp.log(all_ref[own, at : at + channels, :].astype(f32))
                        value = activated(code, scale * reach, scale * center + offset)
                        peak_pool = jnp.maximum(peak_pool, jnp.abs(value))
                        both.append(bounded(value, bound))
                    for q in range(span // LANES):
                        low, high = (one[:, at_block(q)] for one in both)
                        block = s * (span // row_len) + 2 * q
                        one = jnp.where(lower, low, turned(high))
                        two = jnp.where(lower, turned(low), high)
                        keep(place, block + 1, one)
                        keep(place, block + 2, two)
                        if block == 0:
                            ends.append((blocks + 1, jnp.where(lower, turned(one), blank)))
                        if block + 2 == blocks:
                            ends.append((0, jnp.where(lower, blank, turned(two))))
                for block, value in ends:
                    keep(place, block, value)
        main = 3 * chan_own
        at_y = lax.axis_index("sy")
        for k, piece_ref in enumerate(piece_refs):
            near_ref[pl.ds((at_y ^ k) * main, main), :] = piece_ref[:main, :]
            far_ref[pl.ds((at_y ^ k) * chan_own, chan_own), :] = piece_ref[main:, : 3 * channels]
        near_weight = near_ref[...]
        far_weight = far_ref[...]
        blank = jnp.zeros((chan_own, LANES), f32)
        totals = [blank for _ in range(y_groups)]
        squares = [blank for _ in range(y_groups)]
        leasts = [blank + 1e30 for _ in range(y_groups)]
        mosts = [blank - 1e30 for _ in range(y_groups)]
        for z in range(planes):
            for t in range(blocks // 2):
                depths = [dz for dz in range(3) if 0 <= z + dz - 1 < planes]

                def cells(dz, dy, which):
                    return jnp.concatenate(
                        [cells_ref[z + dz - 1, 2 * t + dy + half, which] for half in range(2)],
                        axis=1,
                    )

                window = [
                    cells(dz, dy, middle) for dz in depths for dy in range(3) if dz + dy < 4
                ]
                first = 3 * depths[0] * channels
                taps = jnp.dot(
                    near_weight[:, first : first + len(window) * channels],
                    jnp.concatenate(window, axis=0),
                    preferred_element_type=f32,
                )
                rest = None
                if depths[-1] == 2:
                    rest = jnp.dot(
                        far_weight, cells(2, 2, slice(None)), preferred_element_type=f32
                    )
                for s in range(y_groups):
                    for half in range(2):
                        at = s * main
                        part = taps[at : at + main, at_block(half)]
                        center = part[chan_own : 2 * chan_own]
                        if rest is not None:
                            own = slice(s * chan_own, (s + 1) * chan_own)
                            center = center + rest[own, at_block(half)]
                        out = tap_sum(part[:chan_own], center, part[2 * chan_own :], row_len)
                        raw_ref[
                            z, s * chan_own : (s + 1) * chan_own, at_block(2 * t + half)
                        ] = out
                        totals[s] = totals[s] + out
                        squares[s] = squares[s] + out * out
                        leasts[s] = jnp.minimum(leasts[s], out)
                        mosts[s] = jnp.maximum(mosts[s], out)
        pairs = [
            affine(
                jnp.sum(totals[s], axis=1, keepdims=True),
                jnp.sum(squares[s], axis=1, keepdims=True),
                coarse_cells,
                column(rows[s, 0], chan_own, GAIN_AT),
                column(rows[s, 0], chan_own, SHIFT_AT),
            )
            for s in range(y_groups)
        ]
        scale = jnp.concatenate([one[0] for one in pairs], axis=0)
        offset = jnp.concatenate([one[1] for one in pairs], axis=0)
        lanes = lax.broadcasted_iota(jnp.int32, (chan_all, LANES), 1)
        next_ref[...] = jnp.where(lanes == 0, scale, jnp.where(lanes == 1, offset, 0.0))
        peak = jnp.zeros((chan_all, LANES), bf16)
        for extreme in (leasts, mosts):
            value = activated(jnp.concatenate(extreme, axis=0), scale, offset)
            peak = jnp.maximum(peak, jnp.abs(value))
        row = at_lane(tops[:, PEAK_AT : PEAK_AT + 1], 0)
        row = row + at_lane(tops[:, PEAK_AT + 1 : PEAK_AT + 2], 1)
        row = row + at_lane(peak_of(peak_pool), 2)
        row = row + at_lane(peak_of(peak), 3)
        peak_ref[...] = row[:, : peak_ref.shape[1]]

    return kernel


def fourth_kernel(coarse_cells):
    def kernel(
        raw_ref,
        weight_ref,
        param_ref,
        affine_ref,
        next_ref,
        fine_ref,
        out_ref,
        skip_ref,
        cells_ref,
        last_ref,
        narrow_ref,
        done,
    ):
        scale = affine_ref[:, 0:1]
        offset = affine_ref[:, 1:2]
        sends = []
        for z in range(fine_ref.shape[0]):
            act = jnp.stack(
                [activated(fine_ref[z, y], scale, offset) for y in range(fine_ref.shape[1])]
            )
            narrow_ref[:, z] = jnp.transpose(act, (1, 0, 2))
            sends.append(
                pltpu.make_async_copy(narrow_ref.at[:, z], skip_ref.at[0, :, z], done.at[z])
            )
            sends[-1].start()
        planes, chan_all, flat = cells_ref.shape
        chan_own, z_own = out_ref.shape[:2]
        row_len = LANES // 2
        blocks = flat // LANES
        weight = weight_ref[...]
        lower = lax.broadcasted_iota(jnp.int32, (chan_own, LANES), 1) < row_len
        blank = jnp.zeros((chan_own, LANES), f32)
        bound = clip_bound(param_ref, 3)
        scale = next_ref[:, 0:1]
        offset = next_ref[:, 1:2]

        def at_block(block):
            return slice(block * LANES, (block + 1) * LANES)

        def normed(z):
            for j in range(blocks):
                value = activated(raw_ref[z, :, at_block(j)], scale, offset)
                cells_ref[z, :, at_block(j)] = bounded(value, bound)

        def plane(z, sums):
            total, square = sums
            depths = [dz for dz in range(3) if 0 <= z + dz - 1 < planes]
            columns = slice(depths[0] * chan_all, (depths[-1] + 1) * chan_all)
            parts = []
            for t in range(blocks // 2):
                window = jnp.concatenate(
                    [
                        cells_ref[z + dz - 1, :, 2 * t * LANES : 2 * (t + 1) * LANES]
                        for dz in depths
                    ],
                    axis=0,
                )
                taps = jnp.dot(weight[:, columns], window, preferred_element_type=f32)
                parts.extend(taps[:, at_block(half)] for half in range(2))

            def tap(dy, dx, j):
                at = (3 * dy + dx) * chan_own
                return parts[j][at : at + chan_own]

            for j in range(blocks):
                three = []
                for dx in range(3):
                    if j > 0:
                        before = tap(0, dx, j - 1)
                    else:
                        before = jnp.where(lower, blank, turned(tap(0, dx, blocks - 1)))
                    if j + 1 < blocks:
                        after = tap(2, dx, j + 1)
                    else:
                        after = jnp.where(lower, turned(tap(2, dx, 0)), blank)
                    three.append(tap(1, dx, j) + before + after)
                out = tap_sum(*three, row_len)
                last_ref[z, :, at_block(j)] = out
                total = total + out
                square = square + out * out
            return total, square

        sums = (blank, blank)
        normed(0)
        for z in range(planes):
            if z + 1 < planes:
                normed(z + 1)
            sums = plane(z, sums)
        total, square = sums
        scale, offset = affine(
            jnp.sum(total, axis=1, keepdims=True),
            jnp.sum(square, axis=1, keepdims=True),
            coarse_cells,
            lane_of(param_ref, LAST_AT, chan_own),
            lane_of(param_ref, LAST_AT + 1, chan_own),
        )
        at_z = lax.axis_index("sz")
        own = []
        for i in range(z_own):
            cells = activated(last_ref[at_z * z_own + i], scale, offset).astype(f32)
            natural = []
            for p in range(blocks):
                row = (2 * p) % blocks
                first, second = cells[:, at_block(row)], cells[:, at_block(row + 1)]
                if 2 * p < blocks:
                    natural.append(jnp.where(lower, first, turned(second)))
                else:
                    natural.append(jnp.where(lower, turned(first), second))
            own.append(jnp.concatenate(natural, axis=1))
        for c in range(chan_own):
            out_ref[c] = jnp.concatenate([one[c : c + 1] for one in own], axis=0).astype(bf16)
        for send in sends:
            send.wait()

    return kernel


def final_kernel(*refs):
    cells_ref, peak_ref = refs[:2]
    out_ref, top_ref = refs[-2:]
    out_ref[0] = cells_ref[...]
    top = peak_ref[...]
    for ref in refs[2:-2]:
        top = jnp.maximum(top, ref[...])
    top_ref[...] = top


def shape(dims, dtype):
    return jax.ShapeDtypeStruct(dims, dtype)


def near_shape(dims, dtype):
    return pltpu.VMEM(dims, dtype)


def held(value):
    return pltpu.with_memory_space_constraint(value, pltpu.VMEM)


def per_device(
    volume,
    amax_history,
    conv_first,
    conv_second,
    conv_third,
    conv_fourth,
    gain_fine,
    shift_fine,
    gain_coarse,
    shift_coarse,
):
    channels, depth, height, width = volume.shape[1:]
    z_groups = lax.axis_size("sz")
    y_groups = lax.axis_size("sy")
    samples = lax.axis_size("sample")
    fine_cells = float(depth * z_groups * height * y_groups * width)
    coarse_cells = fine_cells / 8
    chan_own = conv_third.shape[1]
    chan_all = conv_fourth.shape[2]
    span = (height // 2) * (width // 2)
    planes = (depth // 2) * z_groups
    flat = span * y_groups
    group = z_groups * y_groups
    load_rows = (depth // 2) * channels + ROWS

    anywhere = pl.BlockSpec(memory_space=pl.ANY)
    near = pl.BlockSpec(memory_space=pltpu.VMEM)
    z_first, z_second = pl.pallas_call(
        slab_kernel,
        in_specs=[anywhere],
        out_specs=(near, near),
        out_shape=(
            near_shape((channels, HALO, height, width), bf16),
            near_shape((channels, HALO, height, width), bf16),
        ),
        scratch_shapes=[pltpu.SemaphoreType.DMA((2 * SLAB_PARTS,))],
        name="slabs",
    )(volume)
    cells, peak = pl.pallas_call(
        prep_kernel,
        out_shape=(
            near_shape((depth, height, channels, width), bf16),
            near_shape((1, LANES), f32),
        ),
        name="prep",
    )(volume, amax_history)
    third_rows = 4 * chan_own
    m1, m2, m3, m4, params, gain_row = pl.pallas_call(
        matrix_kernel,
        out_shape=(
            near_shape((3 * channels, 9 * channels), bf16),
            near_shape((3 * channels, 9 * channels), bf16),
            near_shape((third_rows, 8 * channels), bf16),
            near_shape((9 * chan_own, 3 * chan_all), bf16),
            near_shape((channels, LANES), f32),
            near_shape((1, LANES), f32),
        ),
        name="matrices",
    )(
        held(peak),
        conv_first,
        conv_second,
        conv_third,
        conv_fourth,
        amax_history,
        gain_fine,
        shift_fine,
        gain_coarse,
        shift_coarse,
    )
    pieces = [m3]
    for k in range(1, y_groups):
        pieces.append(lax.ppermute(m3, "sy", [(i, i ^ k) for i in range(y_groups)]))
    pair_first, pair_second = pairings("sz")
    z_first = lax.ppermute(z_first, "sz", pair_first)
    z_second = lax.ppermute(z_second, "sz", pair_second)
    deep_depth = depth + 2 * HALO
    levels = amax_history.shape[0]
    z_first, z_second, first, second = pl.pallas_call(
        deep_kernel,
        out_shape=(
            near_shape((HALO, height, channels, width), bf16),
            near_shape((HALO, height, channels, width), bf16),
            near_shape((deep_depth, HALO, channels, width), bf16),
            near_shape((deep_depth, HALO, channels, width), bf16),
        ),
        name="deep",
    )(*(held(x) for x in (cells, z_first, z_second, params)))
    pair_first, pair_second = pairings("sy")
    y_first = lax.ppermute(first, "sy", pair_first)
    y_second = lax.ppermute(second, "sy", pair_second)
    deep, raw_inner, sums = pl.pallas_call(
        first_inner_kernel,
        out_shape=(
            near_shape((deep_depth, height, channels, width), bf16),
            near_shape((depth + 2, height - 2, channels, width), f32),
            near_shape((2, channels, LANES), f32),
        ),
        name="first_inner",
    )(*(held(x) for x in (cells, z_first, z_second, m1)))
    raw_outer, row = pl.pallas_call(
        first_outer_kernel,
        out_shape=(
            near_shape((depth + 2, 2 * HALO, channels, width), f32),
            near_shape((group, 1, LANES), f32),
        ),
        scratch_shapes=[pltpu.VMEM((2, deep_depth, HALO, channels, width), bf16)],
        name="first_outer",
    )(*(held(x) for x in (deep, y_first, y_second, m1, peak, sums)))
    rows = lax.all_to_all(row, ("sy", "sz"), 0, 0, tiled=True)
    raw_second, load = pl.pallas_call(
        second_kernel(fine_cells),
        out_shape=(
            near_shape((depth, height, channels, width), f32),
            near_shape((load_rows, span), bf16),
        ),
        scratch_shapes=[
            pltpu.VMEM((depth + 2, height + 2, channels, width), bf16),
            pltpu.VMEM((depth // 2, height // 2, channels, width), f32),
        ],
        compiler_params=pltpu.CompilerParams(vmem_limit_bytes=KERNEL_BYTES),
        name="second",
    )(*(held(x) for x in (raw_inner, raw_outer, rows, m2, params, gain_row)))
    loads = [load]
    for k in range(1, z_groups):
        loads.append(lax.ppermute(load, "sz", [(i, i ^ k) for i in range(z_groups)]))
    gathered = lax.all_gather(jnp.concatenate(loads, axis=0), "sy", axis=0)
    raw_third, peaks, fine_affine, next_affine = pl.pallas_call(
        third_kernel(fine_cells, coarse_cells, load_rows, third_rows),
        out_shape=(
            near_shape((planes, chan_all, flat), f32),
            near_shape((1, levels), f32),
            near_shape((channels, LANES), f32),
            near_shape((chan_all, LANES), f32),
        ),
        scratch_shapes=[
            pltpu.VMEM((planes, flat // LANES + 2, 3 * channels, LANES), bf16),
            pltpu.VMEM((3 * chan_all, 8 * channels), bf16),
            pltpu.VMEM((chan_all, 3 * channels), bf16),
        ],
        compiler_params=pltpu.CompilerParams(vmem_limit_bytes=KERNEL_BYTES),
        name="third",
    )(*(held(x) for x in (gathered, params, *pieces)))
    if samples <= 4:
        others = [
            lax.ppermute(peaks, "sample", [(i, (i + k) % samples) for i in range(samples)])
            for k in range(1, samples)
        ]
    else:
        others = [lax.pmax(peaks, "sample")]
    coarse, skip = pl.pallas_call(
        fourth_kernel(coarse_cells),
        out_shape=(
            near_shape((chan_own, depth // 2, flat), bf16),
            shape((1, channels, depth, height, width), bf16),
        ),
        out_specs=(near, anywhere),
        scratch_shapes=[
            pltpu.VMEM((planes, chan_all, flat), bf16),
            pltpu.VMEM((planes, chan_own, flat), f32),
            pltpu.VMEM((channels, depth, height, width), bf16),
            pltpu.SemaphoreType.DMA((depth,)),
        ],
        compiler_params=pltpu.CompilerParams(vmem_limit_bytes=KERNEL_BYTES),
        name="fourth",
    )(*(held(x) for x in (raw_third, m4, params, fine_affine, next_affine, raw_second)))
    coarse, peaks = pl.pallas_call(
        final_kernel,
        out_shape=(
            shape((1, chan_own, depth // 2, flat), bf16),
            shape((1, levels), f32),
        ),
        name="final",
    )(*(held(x) for x in (coarse, peaks, *others)))
    return skip, coarse, peaks.reshape(levels)


def solution(mesh):
    return jax.shard_map(
        per_device,
        mesh=mesh,
        in_specs=(
            P("sample", None, "sz", "sy", None),
            P(),
            P(),
            P(),
            P(None, "sy", None),
            P(None, "sy", None),
            P(),
            P(),
            P(None, "sy"),
            P(None, "sy"),
        ),
        out_specs=(P("sample", None, "sz", "sy", None), P("sample", "sy", "sz", None), P()),
        check_vma=False,
    )
```

```python
import jax
import jax.numpy as jnp
from jax import lax
from jax.experimental import pallas as pl
from jax.experimental.pallas import tpu as pltpu
from jax.sharding import PartitionSpec as P

norm_eps = 1e-05
leak_slope = 0.01
f32 = jnp.float32
bf16 = jnp.bfloat16
LANES = 128
HALO = 2
SLAB_PARTS = 4
KERNEL_BYTES = 24 * 1024 * 1024
PEAK_AT = 64
CODE_AT = 66
GAIN_AT = 80
SHIFT_AT = 96
CODE_SPAN = 83.0
ROWS = 8


def pairings(axis):
    count = lax.axis_size(axis)
    first = [(i, i ^ 1) for i in range(count)]
    second = [(i, min(max(((i + 1) ^ 1) - 1, 0), count - 1)) for i in range(count)]
    return first, second


def column(row, channels, start):
    lanes = lax.broadcasted_iota(jnp.int32, (channels, row.shape[1]), 1)
    chans = lax.broadcasted_iota(jnp.int32, (channels, row.shape[1]), 0)
    return jnp.sum(jnp.where(lanes == chans + start, row, 0.0), axis=1, keepdims=True)


def as_row(col, start):
    channels = col.shape[0]
    lanes = lax.broadcasted_iota(jnp.int32, (channels, LANES), 1)
    chans = lax.broadcasted_iota(jnp.int32, (channels, LANES), 0)
    return jnp.sum(jnp.where(lanes == chans + start, col, 0.0), axis=0, keepdims=True)


def at_lane(value, lane):
    lanes = lax.broadcasted_iota(jnp.int32, (1, LANES), 1)
    return jnp.where(lanes == lane, value, 0.0)


def affine(total, square, cells, gains, offset):
    mean = total / cells
    spread = square / cells - mean * mean
    scale = lax.rsqrt(spread + norm_eps) * gains
    return scale, offset - mean * scale


def activated(values, scale, offset):
    normed = values * scale + offset
    return jnp.maximum(normed, leak_slope * normed).astype(bf16)


def peak_of(values):
    values = values.astype(f32)
    return jnp.max(jnp.max(values, axis=0, keepdims=True), axis=1, keepdims=True)


def bounded(values, bound):
    return jnp.minimum(jnp.maximum(values, -bound), bound)


BOUND_AT = 4
LAST_AT = 8


def bound_of(hist_ref, level):
    return jnp.max(hist_ref[level : level + 1, :], axis=1, keepdims=True)


def lane_of(param_ref, lane, channels):
    return param_ref[0:channels, lane : lane + 1]


def clip_bound(param_ref, level):
    return param_ref[0:1, BOUND_AT + level : BOUND_AT + level + 1].astype(bf16)


def matrix_of(weight, taps_ref, groups):
    out_chan = weight.shape[1]
    for dx in range(3):
        taps_ref[dx * out_chan : (dx + 1) * out_chan, :] = jnp.concatenate(
            [weight[3 * j + dx] for j in groups], axis=1
        )


def matrix_kernel(
    peak_ref,
    first_ref,
    second_ref,
    third_ref,
    fourth_ref,
    hist_ref,
    gain_ref,
    shift_ref,
    gain_coarse_ref,
    shift_coarse_ref,
    m1_ref,
    m2_ref,
    m3_ref,
    m4_ref,
    param_ref,
    gain_row_ref,
):
    taps = first_ref.shape[0]
    matrix_of(first_ref, m1_ref, range(taps // 3))
    matrix_of(second_ref, m2_ref, range(taps // 3))
    own = third_ref.shape[1]
    matrix_of(third_ref, m3_ref.at[0 : 3 * own], range(taps // 3 - 1))
    last = [third_ref[taps - 3 + dx] for dx in range(3)]
    rest = m3_ref.shape[1] - 3 * third_ref.shape[2]
    m3_ref[3 * own :, :] = jnp.concatenate(last + [jnp.zeros((own, rest), bf16)], axis=1)
    for dy in range(3):
        for dx in range(3):
            at = (3 * dy + dx) * own
            m4_ref[at : at + own, :] = jnp.concatenate(
                [fourth_ref[9 * dz + 3 * dy + dx] for dz in range(3)], axis=1
            )
    channels = param_ref.shape[0]
    lanes = lax.broadcasted_iota(jnp.int32, (channels, LANES), 1)
    params = jnp.zeros((channels, LANES), f32)
    columns = []
    for layer in range(2):
        columns.append((2 * layer, column(gain_ref[layer : layer + 1, :], channels, 0)))
        columns.append((2 * layer + 1, column(shift_ref[layer : layer + 1, :], channels, 0)))
    for level in range(hist_ref.shape[0]):
        columns.append((BOUND_AT + level, bound_of(hist_ref, level)))
    pad = jnp.zeros((channels - own, 1), f32)
    for place, ref in ((LAST_AT, gain_coarse_ref), (LAST_AT + 1, shift_coarse_ref)):
        columns.append((place, jnp.concatenate([column(ref[1:2, :], own, 0), pad], axis=0)))
    for lane, value in columns:
        params = jnp.where(lanes == lane, value, params)
    param_ref[...] = params
    gain_row_ref[...] = as_row(column(gain_coarse_ref[0:1, :], own, 0), GAIN_AT) + as_row(
        column(shift_coarse_ref[0:1, :], own, 0), SHIFT_AT
    )


def tap_sum(left, middle, right, period):
    lane = lax.broadcasted_iota(jnp.int32, middle.shape, 1) % period
    up = pltpu.roll(left, 1, 1)
    down = pltpu.roll(right, LANES - 1, 1)
    return middle + jnp.where(lane == 0, 0.0, up) + jnp.where(lane == period - 1, 0.0, down)


def slab_kernel(vol_ref, first_ref, second_ref, done):
    depth = vol_ref.shape[2]
    even = lax.axis_index("sz") % 2
    starts = ((1 - even) * (depth - HALO), even * (depth - HALO))
    copies = []
    group = first_ref.shape[0] // SLAB_PARTS
    for start, target in zip(starts, (first_ref, second_ref)):
        for part in range(SLAB_PARTS):
            own = slice(part * group, (part + 1) * group)
            source = vol_ref.at[0, own, pl.ds(start, HALO)]
            copies.append(pltpu.make_async_copy(source, target.at[own], done.at[len(copies)]))
            copies[-1].start()
    for copy in copies:
        copy.wait()


def prep_kernel(vol_ref, hist_ref, cells_ref, peak_ref):
    bound = bound_of(hist_ref, 0).astype(bf16)
    top = jnp.zeros(cells_ref.shape[2:], bf16)
    for z in range(vol_ref.shape[2]):
        rows = jnp.transpose(vol_ref[0, :, z], (1, 0, 2))
        for y in range(rows.shape[0]):
            top = jnp.maximum(top, jnp.abs(rows[y]))
            cells_ref[z, y] = bounded(rows[y], bound)
    peak_ref[...] = jnp.broadcast_to(peak_of(top), (1, LANES))


def sides(axis, first, second):
    at = lax.axis_index(axis)
    count = lax.axis_size(axis)
    even = at % 2 == 0
    blank = jnp.zeros_like(first)
    below = jnp.where(at == 0, blank, jnp.where(even, second, first))
    above = jnp.where(at == count - 1, blank, jnp.where(even, first, second))
    return below, above


def deep_kernel(
    cells_ref,
    got_first_ref,
    got_second_ref,
    param_ref,
    z_first_ref,
    z_second_ref,
    first_ref,
    second_ref,
):
    depth, height = cells_ref.shape[:2]
    bound = clip_bound(param_ref, 0)
    for source, target in ((got_first_ref, z_first_ref), (got_second_ref, z_second_ref)):
        for z in range(HALO):
            rows = jnp.transpose(source[:, z], (1, 0, 2))
            for y in range(height):
                target[z, y] = bounded(rows[y], bound)
    even = lax.axis_index("sy") % 2 == 0
    starts = (jnp.where(even, height - HALO, 0), jnp.where(even, 0, height - HALO))
    odd_z = lax.axis_index("sz") % 2
    far = HALO + depth
    for start, out_ref in zip(starts, (first_ref, second_ref)):
        rows = pl.ds(start, HALO)
        out_ref[pl.ds((1 - odd_z) * far, HALO)] = z_first_ref[:, rows]
        out_ref[pl.ds(odd_z * far, HALO)] = z_second_ref[:, rows]
        out_ref[HALO:far] = cells_ref[:, rows]


def conv_rows(cell, weight, z, rows, out_chan):
    window = jnp.concatenate(
        [
            jnp.concatenate([cell(z + dz, y + dy) for y in rows], axis=1)
            for dz in range(3)
            for dy in range(3)
        ],
        axis=0,
    )
    taps = jnp.dot(weight, window, preferred_element_type=f32)
    outs = []
    for half in range(2):
        part = taps[:, half * LANES : (half + 1) * LANES]
        outs.append(
            tap_sum(
                part[:out_chan], part[out_chan : 2 * out_chan], part[2 * out_chan :], LANES
            )
        )
    return outs


def first_inner_kernel(own_ref, got_first_ref, got_second_ref, weight_ref, deep_ref, raw_ref, sum_ref):
    depth, count, channels = raw_ref.shape[:3]
    own_depth = own_ref.shape[0]
    below, above = sides("sz", got_first_ref[...], got_second_ref[...])
    deep_ref[0:HALO] = below
    deep_ref[HALO : HALO + own_depth] = own_ref[...]
    deep_ref[HALO + own_depth :] = above
    weight = weight_ref[...]
    total = jnp.zeros((channels, LANES), f32)
    square = total
    for z in range(depth):
        for y in range(0, count, 2):
            outs = conv_rows(lambda z, y: deep_ref[z, y], weight, z, (y, y + 1), channels)
            for half in range(2):
                raw_ref[z, y + half] = outs[half]
                if 1 <= z < depth - 1:
                    total = total + outs[half]
                    square = square + outs[half] * outs[half]
    sum_ref[0] = total
    sum_ref[1] = square


def first_outer_kernel(
    deep_ref, got_first_ref, got_second_ref, weight_ref, peak_ref, sum_ref, raw_ref, row_ref, edge_ref
):
    depth, count, channels = raw_ref.shape[:3]
    planes, own_height = deep_ref.shape[:2]
    below, above = sides("sy", got_first_ref[...], got_second_ref[...])
    at_z = lax.axis_index("sz")
    lowest = jnp.where(at_z > 0, 1.0, 0.0).astype(bf16)
    highest = jnp.where(at_z < lax.axis_size("sz") - 1, 1.0, 0.0).astype(bf16)
    for side, cells in enumerate((below, above)):
        edge_ref[side, :HALO] = cells[:HALO] * lowest
        edge_ref[side, HALO : planes - HALO] = cells[HALO : planes - HALO]
        edge_ref[side, planes - HALO :] = cells[planes - HALO :] * highest

    def cell(z, y):
        if y < HALO:
            return edge_ref[0, z, y]
        if y < HALO + own_height:
            return deep_ref[z, y - HALO]
        return edge_ref[1, z, y - HALO - own_height]

    weight = weight_ref[...]
    total = sum_ref[0]
    square = sum_ref[1]
    last = own_height + 2 - 1
    for z in range(depth):
        for place, rows in ((0, (0, 1)), (2, (last - 1, last))):
            outs = conv_rows(cell, weight, z, rows, channels)
            for half in range(2):
                raw_ref[z, place + half] = outs[half]
                if 1 <= z < depth - 1 and 1 <= rows[half] < last:
                    total = total + outs[half]
                    square = square + outs[half] * outs[half]
    row = as_row(jnp.sum(total, axis=1, keepdims=True), 0)
    row = row + as_row(jnp.sum(square, axis=1, keepdims=True), channels)
    row = row + at_lane(peak_ref[...], PEAK_AT)
    row_ref[...] = jnp.broadcast_to(row[None], row_ref.shape)


def second_kernel(cell_count):
    def kernel(
        inner_ref,
        outer_ref,
        rows_ref,
        weight_ref,
        param_ref,
        gain_row_ref,
        raw_ref,
        load_ref,
        hidden_ref,
        pool_ref,
    ):
        depth, height, channels, width = raw_ref.shape
        wide_depth, wide_height = hidden_ref.shape[:2]
        rows = rows_ref[...]
        merged = jnp.sum(rows, axis=0)
        peak_vol = jnp.max(rows, axis=0)
        scale, offset = affine(
            column(merged, channels, 0),
            column(merged, channels, channels),
            cell_count,
            lane_of(param_ref, 0, channels),
            lane_of(param_ref, 1, channels),
        )
        bound = clip_bound(param_ref, 1)
        at_z = lax.axis_index("sz")
        at_y = lax.axis_index("sy")
        last_z = lax.axis_size("sz") - 1
        last_y = lax.axis_size("sy") - 1

        def one_if(inside):
            return jnp.where(inside, 1.0, 0.0).astype(bf16)

        edges_z = (one_if(at_z > 0), one_if(at_z < last_z))
        edges_y = (one_if(at_y > 0), one_if(at_y < last_y))
        peak = jnp.zeros((channels, width), bf16)
        for z in range(wide_depth):
            for y in range(wide_height):
                if y < HALO:
                    raw = outer_ref[z, y]
                elif y < height:
                    raw = inner_ref[z, y - HALO]
                else:
                    raw = outer_ref[z, y - height + HALO]
                hidden = activated(raw, scale, offset)
                if 1 <= y < wide_height - 1 and 1 <= z < wide_depth - 1:
                    peak = jnp.maximum(peak, jnp.abs(hidden))
                hidden = bounded(hidden, bound)
                for place, last, edges in ((z, wide_depth - 1, edges_z), (y, wide_height - 1, edges_y)):
                    if place in (0, last):
                        hidden = hidden * edges[place == last]
                hidden_ref[z, y] = hidden
        blank = jnp.zeros((channels, width), f32)
        weight = weight_ref[...]
        sign = jnp.where(lane_of(param_ref, 2, channels) >= 0, 1.0, -1.0).astype(f32)
        half_height = height // 2
        total, square, least, most = blank, blank, blank + 1e30, blank - 1e30
        for zp in range(depth // 2):
            for yp in range(half_height):
                best = None
                for dz in range(2):
                    z = 2 * zp + dz
                    outs = conv_rows(
                        lambda z, y: hidden_ref[z, y], weight, z, (2 * yp, 2 * yp + 1), channels
                    )
                    for half in range(2):
                        raw_ref[z, 2 * yp + half] = outs[half]
                        total = total + outs[half]
                        square = square + outs[half] * outs[half]
                        signed = outs[half] * sign
                        best = signed if best is None else jnp.maximum(best, signed)
                best = jnp.maximum(best, pltpu.roll(best, LANES - 1, 1)) * sign
                pool_ref[zp, yp] = best
                least = jnp.minimum(least, best)
                most = jnp.maximum(most, best)
        most, least = peak_of(most), -peak_of(-least)
        center = 0.5 * (most + least)
        reach = jnp.maximum(0.5 * (most - least), 1e-30)
        rate = CODE_SPAN / reach
        pick = jnp.where(
            lax.broadcasted_iota(jnp.int32, (2 * LANES, LANES), 0)
            == 2 * lax.broadcasted_iota(jnp.int32, (2 * LANES, LANES), 1),
            1.0,
            0.0,
        ).astype(bf16)
        for zp in range(depth // 2):
            for yq in range(half_height // 2):
                both = jnp.concatenate([pool_ref[zp, 2 * yq], pool_ref[zp, 2 * yq + 1]], axis=1)
                both = jnp.exp((both - center) * rate).astype(bf16)
                load_ref[
                    zp * channels : (zp + 1) * channels, yq * LANES : (yq + 1) * LANES
                ] = jnp.dot(both, pick, preferred_element_type=f32).astype(bf16)
        row = as_row(jnp.sum(total, axis=1, keepdims=True), 0)
        row = row + as_row(jnp.sum(square, axis=1, keepdims=True), channels)
        row = row + at_lane(peak_vol, PEAK_AT)
        row = row + at_lane(peak_of(peak), PEAK_AT + 1)
        row = row + at_lane(center, CODE_AT)
        row = row + at_lane(reach / CODE_SPAN, CODE_AT + 1)
        row = row + gain_row_ref[...]
        high = row.astype(bf16).astype(f32)
        middle = (row - high).astype(bf16).astype(f32)
        low = row - high - middle
        level = lax.broadcasted_iota(jnp.int32, (ROWS, LANES), 0)
        parts = jnp.where(
            level == 0, high, jnp.where(level == 1, middle, jnp.where(level == 2, low, 0.0))
        )
        body = (depth // 2) * channels
        load_ref[body:, 0:LANES] = parts.astype(bf16)
        load_ref[body:, LANES:] = jnp.zeros((ROWS, load_ref.shape[1] - LANES), bf16)

    return kernel


def turned(cells):
    return pltpu.roll(cells, LANES // 2, 1)


def third_kernel(fine_cells, coarse_cells, load_rows, piece):
    def kernel(*refs):
        all_ref, param_ref = refs[:2]
        piece_refs = refs[2:-7]
        raw_ref, peak_ref, affine_ref, next_ref, cells_ref, near_ref, far_ref = refs[-7:]
        y_groups = all_ref.shape[0]
        z_groups = lax.axis_size("sz")
        span = all_ref.shape[2]
        planes, chan_all, flat = raw_ref.shape
        channels = cells_ref.shape[2] // 3
        chan_own = piece // 4
        row_len = LANES // 2
        blocks = flat // LANES
        body = load_rows - ROWS
        z_own = body // channels
        at_z = lax.axis_index("sz")
        totals = jnp.zeros((ROWS, LANES), f32)
        tops = jnp.zeros((1, LANES), f32)
        rows = {}
        for s in range(y_groups):
            for k in range(z_groups):
                parts = all_ref[s, k * load_rows + body : (k + 1) * load_rows, 0:LANES].astype(f32)
                totals = totals + parts
                rows[s, k] = jnp.sum(parts, axis=0, keepdims=True)
                tops = jnp.maximum(tops, rows[s, k])
        merged = jnp.sum(totals, axis=0, keepdims=True)
        scale, offset = affine(
            column(merged, channels, 0),
            column(merged, channels, channels),
            fine_cells,
            lane_of(param_ref, 2, channels),
            lane_of(param_ref, 3, channels),
        )
        lanes = lax.broadcasted_iota(jnp.int32, (channels, LANES), 1)
        affine_ref[...] = jnp.where(lanes == 0, scale, jnp.where(lanes == 1, offset, 0.0))
        bound = clip_bound(param_ref, 2)
        lower = lanes < row_len
        edge = lanes % row_len
        blank = jnp.zeros((channels, LANES), bf16)
        middle = slice(channels, 2 * channels)

        def at_block(block):
            return slice(block * LANES, (block + 1) * LANES)

        def keep(place, block, value):
            cells_ref[place, block, middle] = value
            if block >= 2:
                cells_ref[place, block, :channels] = jnp.where(
                    edge == 0, blank, pltpu.roll(value, 1, 1)
                )
                cells_ref[place, block, 2 * channels :] = jnp.where(
                    edge == row_len - 1, blank, pltpu.roll(value, LANES - 1, 1)
                )

        peak_pool = jnp.zeros((channels, span), bf16)
        half_groups = y_groups // 2
        for s in range(half_groups):
            for k, zp in [(k, zp) for k in range(z_groups) for zp in range(z_own)]:
                place = (at_z ^ k) * z_own + zp
                at = k * load_rows + zp * channels
                ends = []
                both = []
                for own in (s, s + half_groups):
                    center = rows[own, k][:, CODE_AT : CODE_AT + 1]
                    reach = rows[own, k][:, CODE_AT + 1 : CODE_AT + 2]
                    code = jnp.log(all_ref[own, at : at + channels, :].astype(f32))
                    value = activated(code, scale * reach, scale * center + offset)
                    peak_pool = jnp.maximum(peak_pool, jnp.abs(value))
                    both.append(bounded(value, bound))
                for q in range(span // LANES):
                    low, high = (one[:, at_block(q)] for one in both)
                    block = s * (span // row_len) + 2 * q
                    one = jnp.where(lower, low, turned(high))
                    two = jnp.where(lower, turned(low), high)
                    keep(place, block + 1, one)
                    keep(place, block + 2, two)
                    if block == 0:
                        ends.append((blocks + 1, jnp.where(lower, turned(one), blank)))
                    if block + 2 == blocks:
                        ends.append((0, jnp.where(lower, blank, turned(two))))
                for block, value in ends:
                    keep(place, block, value)
        main = 3 * chan_own
        at_y = lax.axis_index("sy")
        for k, piece_ref in enumerate(piece_refs):
            near_ref[pl.ds((at_y ^ k) * main, main), :] = piece_ref[:main, :]
            far_ref[pl.ds((at_y ^ k) * chan_own, chan_own), :] = piece_ref[main:, : 3 * channels]
        near_weight = near_ref[...]
        far_weight = far_ref[...]
        blank = jnp.zeros((chan_own, LANES), f32)
        totals = [blank for _ in range(y_groups)]
        squares = [blank for _ in range(y_groups)]
        leasts = [blank + 1e30 for _ in range(y_groups)]
        mosts = [blank - 1e30 for _ in range(y_groups)]
        for t in range(blocks // 2):
            for z in range(planes):
                depths = [dz for dz in range(3) if 0 <= z + dz - 1 < planes]

                def cells(dz, dy, which):
                    return jnp.concatenate(
                        [cells_ref[z + dz - 1, 2 * t + dy + half, which] for half in range(2)],
                        axis=1,
                    )

                window = [
                    cells(dz, dy, middle) for dz in depths for dy in range(3) if dz + dy < 4
                ]
                first = 3 * depths[0] * channels
                taps = jnp.dot(
                    near_weight[:, first : first + len(window) * channels],
                    jnp.concatenate(window, axis=0),
                    preferred_element_type=f32,
                )
                rest = None
                if depths[-1] == 2:
                    rest = jnp.dot(
                        far_weight, cells(2, 2, slice(None)), preferred_element_type=f32
                    )
                for s in range(y_groups):
                    for half in range(2):
                        at = s * main
                        part = taps[at : at + main, at_block(half)]
                        center = part[chan_own : 2 * chan_own]
                        if rest is not None:
                            own = slice(s * chan_own, (s + 1) * chan_own)
                            center = center + rest[own, at_block(half)]
                        out = tap_sum(part[:chan_own], center, part[2 * chan_own :], row_len)
                        raw_ref[
                            z, s * chan_own : (s + 1) * chan_own, at_block(2 * t + half)
                        ] = out
                        totals[s] = totals[s] + out
                        squares[s] = squares[s] + out * out
                        leasts[s] = jnp.minimum(leasts[s], out)
                        mosts[s] = jnp.maximum(mosts[s], out)
        pairs = [
            affine(
                jnp.sum(totals[s], axis=1, keepdims=True),
                jnp.sum(squares[s], axis=1, keepdims=True),
                coarse_cells,
                column(rows[s, 0], chan_own, GAIN_AT),
                column(rows[s, 0], chan_own, SHIFT_AT),
            )
            for s in range(y_groups)
        ]
        scale = jnp.concatenate([one[0] for one in pairs], axis=0)
        offset = jnp.concatenate([one[1] for one in pairs], axis=0)
        lanes = lax.broadcasted_iota(jnp.int32, (chan_all, LANES), 1)
        next_ref[...] = jnp.where(lanes == 0, scale, jnp.where(lanes == 1, offset, 0.0))
        peak = jnp.zeros((chan_all, LANES), bf16)
        for extreme in (leasts, mosts):
            value = activated(jnp.concatenate(extreme, axis=0), scale, offset)
            peak = jnp.maximum(peak, jnp.abs(value))
        row = at_lane(tops[:, PEAK_AT : PEAK_AT + 1], 0)
        row = row + at_lane(tops[:, PEAK_AT + 1 : PEAK_AT + 2], 1)
        row = row + at_lane(peak_of(peak_pool), 2)
        row = row + at_lane(peak_of(peak), 3)
        peak_ref[...] = row[:, : peak_ref.shape[1]]

    return kernel


def fourth_kernel(coarse_cells):
    def kernel(
        raw_ref,
        weight_ref,
        param_ref,
        affine_ref,
        next_ref,
        fine_ref,
        out_ref,
        skip_ref,
        cells_ref,
        last_ref,
        narrow_ref,
        done,
    ):
        scale = affine_ref[:, 0:1]
        offset = affine_ref[:, 1:2]
        sends = []
        for z in range(fine_ref.shape[0]):
            act = jnp.stack(
                [activated(fine_ref[z, y], scale, offset) for y in range(fine_ref.shape[1])]
            )
            narrow_ref[:, z] = jnp.transpose(act, (1, 0, 2))
            sends.append(
                pltpu.make_async_copy(narrow_ref.at[:, z], skip_ref.at[0, :, z], done.at[z])
            )
            sends[-1].start()
        planes, chan_all, flat = cells_ref.shape
        chan_own, z_own = out_ref.shape[:2]
        row_len = LANES // 2
        blocks = flat // LANES
        weight = weight_ref[...]
        lower = lax.broadcasted_iota(jnp.int32, (chan_own, LANES), 1) < row_len
        blank = jnp.zeros((chan_own, LANES), f32)
        bound = clip_bound(param_ref, 3)
        scale = next_ref[:, 0:1]
        offset = next_ref[:, 1:2]

        def at_block(block):
            return slice(block * LANES, (block + 1) * LANES)

        def normed(z):
            for j in range(blocks):
                value = activated(raw_ref[z, :, at_block(j)], scale, offset)
                cells_ref[z, :, at_block(j)] = bounded(value, bound)

        def plane(z, sums):
            total, square = sums
            depths = [dz for dz in range(3) if 0 <= z + dz - 1 < planes]
            columns = slice(depths[0] * chan_all, (depths[-1] + 1) * chan_all)
            parts = []
            for t in range(blocks // 2):
                window = jnp.concatenate(
                    [
                        cells_ref[z + dz - 1, :, 2 * t * LANES : 2 * (t + 1) * LANES]
                        for dz in depths
                    ],
                    axis=0,
                )
                taps = jnp.dot(weight[:, columns], window, preferred_element_type=f32)
                parts.extend(taps[:, at_block(half)] for half in range(2))

            def tap(dy, dx, j):
                at = (3 * dy + dx) * chan_own
                return parts[j][at : at + chan_own]

            for j in range(blocks):
                three = []
                for dx in range(3):
                    if j > 0:
                        before = tap(0, dx, j - 1)
                    else:
                        before = jnp.where(lower, blank, turned(tap(0, dx, blocks - 1)))
                    if j + 1 < blocks:
                        after = tap(2, dx, j + 1)
                    else:
                        after = jnp.where(lower, turned(tap(2, dx, 0)), blank)
                    three.append(tap(1, dx, j) + before + after)
                out = tap_sum(*three, row_len)
                last_ref[z, :, at_block(j)] = out
                total = total + out
                square = square + out * out
            return total, square

        sums = (blank, blank)
        normed(0)
        for z in range(planes):
            if z + 1 < planes:
                normed(z + 1)
            sums = plane(z, sums)
        total, square = sums
        scale, offset = affine(
            jnp.sum(total, axis=1, keepdims=True),
            jnp.sum(square, axis=1, keepdims=True),
            coarse_cells,
            lane_of(param_ref, LAST_AT, chan_own),
            lane_of(param_ref, LAST_AT + 1, chan_own),
        )
        at_z = lax.axis_index("sz")
        own = []
        for i in range(z_own):
            cells = activated(last_ref[at_z * z_own + i], scale, offset).astype(f32)
            natural = []
            for p in range(blocks):
                row = (2 * p) % blocks
                first, second = cells[:, at_block(row)], cells[:, at_block(row + 1)]
                if 2 * p < blocks:
                    natural.append(jnp.where(lower, first, turned(second)))
                else:
                    natural.append(jnp.where(lower, turned(first), second))
            own.append(jnp.concatenate(natural, axis=1))
        for c in range(chan_own):
            out_ref[c] = jnp.concatenate([one[c : c + 1] for one in own], axis=0).astype(bf16)
        for send in sends:
            send.wait()

    return kernel


def final_kernel(*refs):
    cells_ref, peak_ref = refs[:2]
    out_ref, top_ref = refs[-2:]
    out_ref[0] = cells_ref[...]
    top = peak_ref[...]
    for ref in refs[2:-2]:
        top = jnp.maximum(top, ref[...])
    top_ref[...] = top


def shape(dims, dtype):
    return jax.ShapeDtypeStruct(dims, dtype)


def near_shape(dims, dtype):
    return pltpu.VMEM(dims, dtype)


def held(value):
    return pltpu.with_memory_space_constraint(value, pltpu.VMEM)


def per_device(
    volume,
    amax_history,
    conv_first,
    conv_second,
    conv_third,
    conv_fourth,
    gain_fine,
    shift_fine,
    gain_coarse,
    shift_coarse,
):
    channels, depth, height, width = volume.shape[1:]
    z_groups = lax.axis_size("sz")
    y_groups = lax.axis_size("sy")
    samples = lax.axis_size("sample")
    fine_cells = float(depth * z_groups * height * y_groups * width)
    coarse_cells = fine_cells / 8
    chan_own = conv_third.shape[1]
    chan_all = conv_fourth.shape[2]
    span = (height // 2) * (width // 2)
    planes = (depth // 2) * z_groups
    flat = span * y_groups
    group = z_groups * y_groups
    load_rows = (depth // 2) * channels + ROWS

    anywhere = pl.BlockSpec(memory_space=pl.ANY)
    near = pl.BlockSpec(memory_space=pltpu.VMEM)
    z_first, z_second = pl.pallas_call(
        slab_kernel,
        in_specs=[anywhere],
        out_specs=(near, near),
        out_shape=(
            near_shape((channels, HALO, height, width), bf16),
            near_shape((channels, HALO, height, width), bf16),
        ),
        scratch_shapes=[pltpu.SemaphoreType.DMA((2 * SLAB_PARTS,))],
        name="slabs",
    )(volume)
    cells, peak = pl.pallas_call(
        prep_kernel,
        out_shape=(
            near_shape((depth, height, channels, width), bf16),
            near_shape((1, LANES), f32),
        ),
        name="prep",
    )(volume, amax_history)
    third_rows = 4 * chan_own
    m1, m2, m3, m4, params, gain_row = pl.pallas_call(
        matrix_kernel,
        out_shape=(
            near_shape((3 * channels, 9 * channels), bf16),
            near_shape((3 * channels, 9 * channels), bf16),
            near_shape((third_rows, 8 * channels), bf16),
            near_shape((9 * chan_own, 3 * chan_all), bf16),
            near_shape((channels, LANES), f32),
            near_shape((1, LANES), f32),
        ),
        name="matrices",
    )(
        held(peak),
        conv_first,
        conv_second,
        conv_third,
        conv_fourth,
        amax_history,
        gain_fine,
        shift_fine,
        gain_coarse,
        shift_coarse,
    )
    pieces = [m3]
    for k in range(1, y_groups):
        pieces.append(lax.ppermute(m3, "sy", [(i, i ^ k) for i in range(y_groups)]))
    pair_first, pair_second = pairings("sz")
    z_first = lax.ppermute(z_first, "sz", pair_first)
    z_second = lax.ppermute(z_second, "sz", pair_second)
    deep_depth = depth + 2 * HALO
    levels = amax_history.shape[0]
    z_first, z_second, first, second = pl.pallas_call(
        deep_kernel,
        out_shape=(
            near_shape((HALO, height, channels, width), bf16),
            near_shape((HALO, height, channels, width), bf16),
            near_shape((deep_depth, HALO, channels, width), bf16),
            near_shape((deep_depth, HALO, channels, width), bf16),
        ),
        name="deep",
    )(*(held(x) for x in (cells, z_first, z_second, params)))
    pair_first, pair_second = pairings("sy")
    y_first = lax.ppermute(first, "sy", pair_first)
    y_second = lax.ppermute(second, "sy", pair_second)
    deep, raw_inner, sums = pl.pallas_call(
        first_inner_kernel,
        out_shape=(
            near_shape((deep_depth, height, channels, width), bf16),
            near_shape((depth + 2, height - 2, channels, width), f32),
            near_shape((2, channels, LANES), f32),
        ),
        name="first_inner",
    )(*(held(x) for x in (cells, z_first, z_second, m1)))
    raw_outer, row = pl.pallas_call(
        first_outer_kernel,
        out_shape=(
            near_shape((depth + 2, 2 * HALO, channels, width), f32),
            near_shape((group, 1, LANES), f32),
        ),
        scratch_shapes=[pltpu.VMEM((2, deep_depth, HALO, channels, width), bf16)],
        name="first_outer",
    )(*(held(x) for x in (deep, y_first, y_second, m1, peak, sums)))
    rows = lax.all_to_all(row, ("sy", "sz"), 0, 0, tiled=True)
    raw_second, load = pl.pallas_call(
        second_kernel(fine_cells),
        out_shape=(
            near_shape((depth, height, channels, width), f32),
            near_shape((load_rows, span), bf16),
        ),
        scratch_shapes=[
            pltpu.VMEM((depth + 2, height + 2, channels, width), bf16),
            pltpu.VMEM((depth // 2, height // 2, channels, width), f32),
        ],
        compiler_params=pltpu.CompilerParams(vmem_limit_bytes=KERNEL_BYTES),
        name="second",
    )(*(held(x) for x in (raw_inner, raw_outer, rows, m2, params, gain_row)))
    loads = [load]
    for k in range(1, z_groups):
        loads.append(lax.ppermute(load, "sz", [(i, i ^ k) for i in range(z_groups)]))
    gathered = lax.all_gather(jnp.concatenate(loads, axis=0), "sy", axis=0)
    raw_third, peaks, fine_affine, next_affine = pl.pallas_call(
        third_kernel(fine_cells, coarse_cells, load_rows, third_rows),
        out_shape=(
            near_shape((planes, chan_all, flat), f32),
            near_shape((1, levels), f32),
            near_shape((channels, LANES), f32),
            near_shape((chan_all, LANES), f32),
        ),
        scratch_shapes=[
            pltpu.VMEM((planes, flat // LANES + 2, 3 * channels, LANES), bf16),
            pltpu.VMEM((3 * chan_all, 8 * channels), bf16),
            pltpu.VMEM((chan_all, 3 * channels), bf16),
        ],
        compiler_params=pltpu.CompilerParams(vmem_limit_bytes=KERNEL_BYTES),
        name="third",
    )(*(held(x) for x in (gathered, params, *pieces)))
    if samples <= 4:
        others = [
            lax.ppermute(peaks, "sample", [(i, (i + k) % samples) for i in range(samples)])
            for k in range(1, samples)
        ]
    else:
        others = [lax.pmax(peaks, "sample")]
    coarse, skip = pl.pallas_call(
        fourth_kernel(coarse_cells),
        out_shape=(
            near_shape((chan_own, depth // 2, flat), bf16),
            shape((1, channels, depth, height, width), bf16),
        ),
        out_specs=(near, anywhere),
        scratch_shapes=[
            pltpu.VMEM((planes, chan_all, flat), bf16),
            pltpu.VMEM((planes, chan_own, flat), f32),
            pltpu.VMEM((channels, depth, height, width), bf16),
            pltpu.SemaphoreType.DMA((depth,)),
        ],
        compiler_params=pltpu.CompilerParams(vmem_limit_bytes=KERNEL_BYTES),
        name="fourth",
    )(*(held(x) for x in (raw_third, m4, params, fine_affine, next_affine, raw_second)))
    coarse, peaks = pl.pallas_call(
        final_kernel,
        out_shape=(
            shape((1, chan_own, depth // 2, flat), bf16),
            shape((1, levels), f32),
        ),
        name="final",
    )(*(held(x) for x in (coarse, peaks, *others)))
    return skip, coarse, peaks.reshape(levels)


def solution(mesh):
    return jax.shard_map(
        per_device,
        mesh=mesh,
        in_specs=(
            P("sample", None, "sz", "sy", None),
            P(),
            P(),
            P(),
            P(None, "sy", None),
            P(None, "sy", None),
            P(),
            P(),
            P(None, "sy"),
            P(None, "sy"),
        ),
        out_specs=(P("sample", None, "sz", "sy", None), P("sample", "sy", "sz", None), P()),
        check_vma=False,
    )
```

```python
import jax
import jax.numpy as jnp
from jax import lax
from jax.experimental import pallas as pl
from jax.experimental.pallas import tpu as pltpu
from jax.sharding import PartitionSpec as P

norm_eps = 1e-05
leak_slope = 0.01
f32 = jnp.float32
bf16 = jnp.bfloat16
LANES = 128
HALO = 2
SLAB_PARTS = 4
KERNEL_BYTES = 24 * 1024 * 1024
PEAK_AT = 64
GAIN_AT = 80
SHIFT_AT = 96
CODE_SPAN = 83.0
ROWS = 8


def pairings(axis):
    count = lax.axis_size(axis)
    first = [(i, i ^ 1) for i in range(count)]
    second = [(i, min(max(((i + 1) ^ 1) - 1, 0), count - 1)) for i in range(count)]
    return first, second


def column(row, channels, start):
    lanes = lax.broadcasted_iota(jnp.int32, (channels, row.shape[1]), 1)
    chans = lax.broadcasted_iota(jnp.int32, (channels, row.shape[1]), 0)
    return jnp.sum(jnp.where(lanes == chans + start, row, 0.0), axis=1, keepdims=True)


def as_row(col, start):
    channels = col.shape[0]
    lanes = lax.broadcasted_iota(jnp.int32, (channels, LANES), 1)
    chans = lax.broadcasted_iota(jnp.int32, (channels, LANES), 0)
    return jnp.sum(jnp.where(lanes == chans + start, col, 0.0), axis=0, keepdims=True)


def at_lane(value, lane):
    lanes = lax.broadcasted_iota(jnp.int32, (1, LANES), 1)
    return jnp.where(lanes == lane, value, 0.0)


def affine(total, square, cells, gains, offset):
    mean = total / cells
    spread = square / cells - mean * mean
    scale = lax.rsqrt(spread + norm_eps) * gains
    return scale, offset - mean * scale


def activated(values, scale, offset):
    normed = values * scale + offset
    return jnp.maximum(normed, leak_slope * normed).astype(bf16)


def peak_of(values):
    values = values.astype(f32)
    return jnp.max(jnp.max(values, axis=0, keepdims=True), axis=1, keepdims=True)


def bounded(values, bound):
    return jnp.minimum(jnp.maximum(values, -bound), bound)


BOUND_AT = 4
LAST_AT = 8


def bound_of(hist_ref, level):
    return jnp.max(hist_ref[level : level + 1, :], axis=1, keepdims=True)


def lane_of(param_ref, lane, channels):
    return param_ref[0:channels, lane : lane + 1]


def clip_bound(param_ref, level):
    return param_ref[0:1, BOUND_AT + level : BOUND_AT + level + 1].astype(bf16)


def matrix_of(weight, taps_ref, groups):
    out_chan = weight.shape[1]
    for dx in range(3):
        taps_ref[dx * out_chan : (dx + 1) * out_chan, :] = jnp.concatenate(
            [weight[3 * j + dx] for j in groups], axis=1
        )


def matrix_kernel(
    peak_ref,
    first_ref,
    second_ref,
    third_ref,
    fourth_ref,
    hist_ref,
    gain_ref,
    shift_ref,
    gain_coarse_ref,
    shift_coarse_ref,
    m1_ref,
    m2_ref,
    m3_ref,
    m4_ref,
    param_ref,
    gain_row_ref,
):
    taps = first_ref.shape[0]
    matrix_of(first_ref, m1_ref, range(taps // 3))
    matrix_of(second_ref, m2_ref, range(taps // 3))
    own = third_ref.shape[1]
    matrix_of(third_ref, m3_ref.at[0 : 3 * own], range(taps // 3 - 1))
    last = [third_ref[taps - 3 + dx] for dx in range(3)]
    rest = m3_ref.shape[1] - 3 * third_ref.shape[2]
    m3_ref[3 * own :, :] = jnp.concatenate(last + [jnp.zeros((own, rest), bf16)], axis=1)
    for dy in range(3):
        for dx in range(3):
            at = (3 * dy + dx) * own
            m4_ref[at : at + own, :] = jnp.concatenate(
                [fourth_ref[9 * dz + 3 * dy + dx] for dz in range(3)], axis=1
            )
    channels = param_ref.shape[0]
    lanes = lax.broadcasted_iota(jnp.int32, (channels, LANES), 1)
    params = jnp.zeros((channels, LANES), f32)
    columns = []
    for layer in range(2):
        columns.append((2 * layer, column(gain_ref[layer : layer + 1, :], channels, 0)))
        columns.append((2 * layer + 1, column(shift_ref[layer : layer + 1, :], channels, 0)))
    for level in range(hist_ref.shape[0]):
        columns.append((BOUND_AT + level, bound_of(hist_ref, level)))
    pad = jnp.zeros((channels - own, 1), f32)
    for place, ref in ((LAST_AT, gain_coarse_ref), (LAST_AT + 1, shift_coarse_ref)):
        columns.append((place, jnp.concatenate([column(ref[1:2, :], own, 0), pad], axis=0)))
    for lane, value in columns:
        params = jnp.where(lanes == lane, value, params)
    param_ref[...] = params
    gain_row_ref[...] = as_row(column(gain_coarse_ref[0:1, :], own, 0), GAIN_AT) + as_row(
        column(shift_coarse_ref[0:1, :], own, 0), SHIFT_AT
    )


def tap_sum(left, middle, right, period):
    lane = lax.broadcasted_iota(jnp.int32, middle.shape, 1) % period
    up = pltpu.roll(left, 1, 1)
    down = pltpu.roll(right, LANES - 1, 1)
    return middle + jnp.where(lane == 0, 0.0, up) + jnp.where(lane == period - 1, 0.0, down)


def slab_kernel(vol_ref, first_ref, second_ref, done):
    depth = vol_ref.shape[2]
    even = lax.axis_index("sz") % 2
    starts = ((1 - even) * (depth - HALO), even * (depth - HALO))
    copies = []
    group = first_ref.shape[0] // SLAB_PARTS
    for start, target in zip(starts, (first_ref, second_ref)):
        for part in range(SLAB_PARTS):
            own = slice(part * group, (part + 1) * group)
            source = vol_ref.at[0, own, pl.ds(start, HALO)]
            copies.append(pltpu.make_async_copy(source, target.at[own], done.at[len(copies)]))
            copies[-1].start()
    for copy in copies:
        copy.wait()


def prep_kernel(vol_ref, hist_ref, cells_ref, peak_ref):
    bound = bound_of(hist_ref, 0).astype(bf16)
    top = jnp.zeros(cells_ref.shape[2:], bf16)
    for z in range(vol_ref.shape[2]):
        rows = jnp.transpose(vol_ref[0, :, z], (1, 0, 2))
        for y in range(rows.shape[0]):
            top = jnp.maximum(top, jnp.abs(rows[y]))
            cells_ref[z, y] = bounded(rows[y], bound)
    peak_ref[...] = jnp.broadcast_to(peak_of(top), (1, LANES))


def sides(axis, first, second):
    at = lax.axis_index(axis)
    count = lax.axis_size(axis)
    even = at % 2 == 0
    blank = jnp.zeros_like(first)
    below = jnp.where(at == 0, blank, jnp.where(even, second, first))
    above = jnp.where(at == count - 1, blank, jnp.where(even, first, second))
    return below, above


def deep_kernel(
    cells_ref,
    got_first_ref,
    got_second_ref,
    param_ref,
    z_first_ref,
    z_second_ref,
    first_ref,
    second_ref,
):
    depth, height = cells_ref.shape[:2]
    bound = clip_bound(param_ref, 0)
    for source, target in ((got_first_ref, z_first_ref), (got_second_ref, z_second_ref)):
        for z in range(HALO):
            rows = jnp.transpose(source[:, z], (1, 0, 2))
            for y in range(height):
                target[z, y] = bounded(rows[y], bound)
    even = lax.axis_index("sy") % 2 == 0
    starts = (jnp.where(even, height - HALO, 0), jnp.where(even, 0, height - HALO))
    odd_z = lax.axis_index("sz") % 2
    far = HALO + depth
    for start, out_ref in zip(starts, (first_ref, second_ref)):
        rows = pl.ds(start, HALO)
        out_ref[pl.ds((1 - odd_z) * far, HALO)] = z_first_ref[:, rows]
        out_ref[pl.ds(odd_z * far, HALO)] = z_second_ref[:, rows]
        out_ref[HALO:far] = cells_ref[:, rows]


def conv_rows(cell, weight, z, rows, out_chan):
    window = jnp.concatenate(
        [
            jnp.concatenate([cell(z + dz, y + dy) for y in rows], axis=1)
            for dz in range(3)
            for dy in range(3)
        ],
        axis=0,
    )
    taps = jnp.dot(weight, window, preferred_element_type=f32)
    outs = []
    for half in range(2):
        part = taps[:, half * LANES : (half + 1) * LANES]
        outs.append(
            tap_sum(
                part[:out_chan], part[out_chan : 2 * out_chan], part[2 * out_chan :], LANES
            )
        )
    return outs


def first_inner_kernel(own_ref, got_first_ref, got_second_ref, weight_ref, deep_ref, raw_ref, sum_ref):
    depth, count, channels = raw_ref.shape[:3]
    own_depth = own_ref.shape[0]
    below, above = sides("sz", got_first_ref[...], got_second_ref[...])
    deep_ref[0:HALO] = below
    deep_ref[HALO : HALO + own_depth] = own_ref[...]
    deep_ref[HALO + own_depth :] = above
    weight = weight_ref[...]
    total = jnp.zeros((channels, LANES), f32)
    square = total
    for z in range(depth):
        for y in range(0, count, 2):
            outs = conv_rows(lambda z, y: deep_ref[z, y], weight, z, (y, y + 1), channels)
            for half in range(2):
                raw_ref[z, y + half] = outs[half]
                if 1 <= z < depth - 1:
                    total = total + outs[half]
                    square = square + outs[half] * outs[half]
    sum_ref[0] = total
    sum_ref[1] = square


def first_outer_kernel(
    deep_ref, got_first_ref, got_second_ref, weight_ref, peak_ref, sum_ref, raw_ref, row_ref, edge_ref
):
    depth, count, channels = raw_ref.shape[:3]
    planes, own_height = deep_ref.shape[:2]
    below, above = sides("sy", got_first_ref[...], got_second_ref[...])
    at_z = lax.axis_index("sz")
    lowest = jnp.where(at_z > 0, 1.0, 0.0).astype(bf16)
    highest = jnp.where(at_z < lax.axis_size("sz") - 1, 1.0, 0.0).astype(bf16)
    for side, cells in enumerate((below, above)):
        edge_ref[side, :HALO] = cells[:HALO] * lowest
        edge_ref[side, HALO : planes - HALO] = cells[HALO : planes - HALO]
        edge_ref[side, planes - HALO :] = cells[planes - HALO :] * highest

    def cell(z, y):
        if y < HALO:
            return edge_ref[0, z, y]
        if y < HALO + own_height:
            return deep_ref[z, y - HALO]
        return edge_ref[1, z, y - HALO - own_height]

    weight = weight_ref[...]
    total = sum_ref[0]
    square = sum_ref[1]
    last = own_height + 2 - 1
    for z in range(depth):
        for place, rows in ((0, (0, 1)), (2, (last - 1, last))):
            outs = conv_rows(cell, weight, z, rows, channels)
            for half in range(2):
                raw_ref[z, place + half] = outs[half]
                if 1 <= z < depth - 1 and 1 <= rows[half] < last:
                    total = total + outs[half]
                    square = square + outs[half] * outs[half]
    row = as_row(jnp.sum(total, axis=1, keepdims=True), 0)
    row = row + as_row(jnp.sum(square, axis=1, keepdims=True), channels)
    row = row + at_lane(peak_ref[...], PEAK_AT)
    row_ref[...] = jnp.broadcast_to(row[None], row_ref.shape)


def second_kernel(cell_count):
    def kernel(
        inner_ref,
        outer_ref,
        rows_ref,
        weight_ref,
        param_ref,
        gain_row_ref,
        raw_ref,
        load_ref,
        hidden_ref,
        pool_ref,
    ):
        depth, height, channels, width = raw_ref.shape
        wide_depth, wide_height = hidden_ref.shape[:2]
        rows = rows_ref[...]
        merged = jnp.sum(rows, axis=0)
        peak_vol = jnp.max(rows, axis=0)
        scale, offset = affine(
            column(merged, channels, 0),
            column(merged, channels, channels),
            cell_count,
            lane_of(param_ref, 0, channels),
            lane_of(param_ref, 1, channels),
        )
        bound = clip_bound(param_ref, 1)
        at_z = lax.axis_index("sz")
        at_y = lax.axis_index("sy")
        last_z = lax.axis_size("sz") - 1
        last_y = lax.axis_size("sy") - 1

        def one_if(inside):
            return jnp.where(inside, 1.0, 0.0).astype(bf16)

        edges_z = (one_if(at_z > 0), one_if(at_z < last_z))
        edges_y = (one_if(at_y > 0), one_if(at_y < last_y))
        peak = jnp.zeros((channels, width), bf16)
        for z in range(wide_depth):
            for y in range(wide_height):
                if y < HALO:
                    raw = outer_ref[z, y]
                elif y < height:
                    raw = inner_ref[z, y - HALO]
                else:
                    raw = outer_ref[z, y - height + HALO]
                hidden = activated(raw, scale, offset)
                if 1 <= y < wide_height - 1 and 1 <= z < wide_depth - 1:
                    peak = jnp.maximum(peak, jnp.abs(hidden))
                hidden = bounded(hidden, bound)
                for place, last, edges in ((z, wide_depth - 1, edges_z), (y, wide_height - 1, edges_y)):
                    if place in (0, last):
                        hidden = hidden * edges[place == last]
                hidden_ref[z, y] = hidden
        blank = jnp.zeros((channels, width), f32)
        weight = weight_ref[...]
        sign = jnp.where(lane_of(param_ref, 2, channels) >= 0, 1.0, -1.0).astype(f32)
        half_height = height // 2
        total, square, least, most = blank, blank, blank + 1e30, blank - 1e30
        for zp in range(depth // 2):
            for yp in range(half_height):
                best = None
                for dz in range(2):
                    z = 2 * zp + dz
                    outs = conv_rows(
                        lambda z, y: hidden_ref[z, y], weight, z, (2 * yp, 2 * yp + 1), channels
                    )
                    for half in range(2):
                        raw_ref[z, 2 * yp + half] = outs[half]
                        total = total + outs[half]
                        square = square + outs[half] * outs[half]
                        signed = outs[half] * sign
                        best = signed if best is None else jnp.maximum(best, signed)
                best = jnp.maximum(best, pltpu.roll(best, LANES - 1, 1)) * sign
                pool_ref[zp, yp] = best
                least = jnp.minimum(least, best)
                most = jnp.maximum(most, best)
        most = jnp.max(most, axis=1, keepdims=True)
        least = jnp.min(least, axis=1, keepdims=True)
        center = 0.5 * (most + least)
        reach = jnp.maximum(0.5 * (most - least), 1e-30)
        rate = CODE_SPAN / reach
        pick = jnp.where(
            lax.broadcasted_iota(jnp.int32, (2 * LANES, LANES), 0)
            == 2 * lax.broadcasted_iota(jnp.int32, (2 * LANES, LANES), 1),
            1.0,
            0.0,
        ).astype(bf16)
        for zp in range(depth // 2):
            for yq in range(half_height // 2):
                both = jnp.concatenate([pool_ref[zp, 2 * yq], pool_ref[zp, 2 * yq + 1]], axis=1)
                both = jnp.exp((both - center) * rate).astype(bf16)
                load_ref[
                    zp * channels : (zp + 1) * channels, yq * LANES : (yq + 1) * LANES
                ] = jnp.dot(both, pick, preferred_element_type=f32).astype(bf16)
        row = as_row(jnp.sum(total, axis=1, keepdims=True), 0)
        row = row + as_row(jnp.sum(square, axis=1, keepdims=True), channels)
        row = row + at_lane(peak_vol, PEAK_AT)
        row = row + at_lane(peak_of(peak), PEAK_AT + 1)
        row = row + gain_row_ref[...]
        code_row = as_row(center, 0) + as_row(reach / CODE_SPAN, channels)
        level = lax.broadcasted_iota(jnp.int32, (ROWS, LANES), 0)
        body = (depth // 2) * channels
        for place, one in ((0, row), (LANES, code_row)):
            high = one.astype(bf16).astype(f32)
            middle = (one - high).astype(bf16).astype(f32)
            low = one - high - middle
            parts = jnp.where(
                level == 0, high, jnp.where(level == 1, middle, jnp.where(level == 2, low, 0.0))
            )
            load_ref[body:, place : place + LANES] = parts.astype(bf16)

    return kernel


def turned(cells):
    return pltpu.roll(cells, LANES // 2, 1)


def third_kernel(fine_cells, coarse_cells, load_rows, piece):
    def kernel(*refs):
        all_ref, param_ref = refs[:2]
        piece_refs = refs[2:-7]
        raw_ref, peak_ref, affine_ref, next_ref, cells_ref, near_ref, far_ref = refs[-7:]
        y_groups = all_ref.shape[0]
        z_groups = lax.axis_size("sz")
        span = all_ref.shape[2]
        planes, chan_all, flat = raw_ref.shape
        channels = cells_ref.shape[2] // 3
        chan_own = piece // 4
        row_len = LANES // 2
        blocks = flat // LANES
        body = load_rows - ROWS
        z_own = body // channels
        at_z = lax.axis_index("sz")
        totals = jnp.zeros((ROWS, LANES), f32)
        tops = jnp.zeros((1, LANES), f32)
        rows = {}
        for s in range(y_groups):
            for k in range(z_groups):
                parts = all_ref[s, k * load_rows + body : (k + 1) * load_rows, 0:LANES].astype(f32)
                totals = totals + parts
                rows[s, k] = jnp.sum(parts, axis=0, keepdims=True)
                tops = jnp.maximum(tops, rows[s, k])
        merged = jnp.sum(totals, axis=0, keepdims=True)
        scale, offset = affine(
            column(merged, channels, 0),
            column(merged, channels, channels),
            fine_cells,
            lane_of(param_ref, 2, channels),
            lane_of(param_ref, 3, channels),
        )
        lanes = lax.broadcasted_iota(jnp.int32, (channels, LANES), 1)
        affine_ref[...] = jnp.where(lanes == 0, scale, jnp.where(lanes == 1, offset, 0.0))
        bound = clip_bound(param_ref, 2)
        lower = lanes < row_len
        edge = lanes % row_len
        blank = jnp.zeros((channels, LANES), bf16)
        middle = slice(channels, 2 * channels)

        def at_block(block):
            return slice(block * LANES, (block + 1) * LANES)

        def keep(place, block, value):
            cells_ref[place, block, middle] = value
            if block >= 2:
                cells_ref[place, block, :channels] = jnp.where(
                    edge == 0, blank, pltpu.roll(value, 1, 1)
                )
                cells_ref[place, block, 2 * channels :] = jnp.where(
                    edge == row_len - 1, blank, pltpu.roll(value, LANES - 1, 1)
                )

        peak_pool = jnp.zeros((channels, span), bf16)
        half_groups = y_groups // 2
        codes = {}
        for s in range(half_groups):
            for k, zp in [(k, zp) for k in range(z_groups) for zp in range(z_own)]:
                place = (at_z ^ k) * z_own + zp
                at = k * load_rows + zp * channels
                ends = []
                both = []
                for own in (s, s + half_groups):
                    if zp == 0:
                        first = k * load_rows + body
                        code_row = all_ref[own, first : first + ROWS, LANES : 2 * LANES]
                        code_row = jnp.sum(code_row.astype(f32), axis=0, keepdims=True)
                        center = column(code_row, channels, 0)
                        reach = column(code_row, channels, channels)
                        codes[own, k] = (scale * reach, scale * center + offset)
                    code = jnp.log(all_ref[own, at : at + channels, :].astype(f32))
                    value = activated(code, *codes[own, k])
                    peak_pool = jnp.maximum(peak_pool, jnp.abs(value))
                    both.append(bounded(value, bound))
                for q in range(span // LANES):
                    low, high = (one[:, at_block(q)] for one in both)
                    block = s * (span // row_len) + 2 * q
                    one = jnp.where(lower, low, turned(high))
                    two = jnp.where(lower, turned(low), high)
                    keep(place, block + 1, one)
                    keep(place, block + 2, two)
                    if block == 0:
                        ends.append((blocks + 1, jnp.where(lower, turned(one), blank)))
                    if block + 2 == blocks:
                        ends.append((0, jnp.where(lower, blank, turned(two))))
                for block, value in ends:
                    keep(place, block, value)
        main = 3 * chan_own
        at_y = lax.axis_index("sy")
        for k, piece_ref in enumerate(piece_refs):
            near_ref[pl.ds((at_y ^ k) * main, main), :] = piece_ref[:main, :]
            far_ref[pl.ds((at_y ^ k) * chan_own, chan_own), :] = piece_ref[main:, : 3 * channels]
        near_weight = near_ref[...]
        far_weight = far_ref[...]
        blank = jnp.zeros((chan_own, LANES), f32)
        totals = [blank for _ in range(y_groups)]
        squares = [blank for _ in range(y_groups)]
        leasts = [blank + 1e30 for _ in range(y_groups)]
        mosts = [blank - 1e30 for _ in range(y_groups)]
        for t in range(blocks // 2):
            for z in range(planes):
                depths = [dz for dz in range(3) if 0 <= z + dz - 1 < planes]

                def cells(dz, dy, which):
                    return jnp.concatenate(
                        [cells_ref[z + dz - 1, 2 * t + dy + half, which] for half in range(2)],
                        axis=1,
                    )

                window = [
                    cells(dz, dy, middle) for dz in depths for dy in range(3) if dz + dy < 4
                ]
                first = 3 * depths[0] * channels
                taps = jnp.dot(
                    near_weight[:, first : first + len(window) * channels],
                    jnp.concatenate(window, axis=0),
                    preferred_element_type=f32,
                )
                rest = None
                if depths[-1] == 2:
                    rest = jnp.dot(
                        far_weight, cells(2, 2, slice(None)), preferred_element_type=f32
                    )
                for s in range(y_groups):
                    for half in range(2):
                        at = s * main
                        part = taps[at : at + main, at_block(half)]
                        center = part[chan_own : 2 * chan_own]
                        if rest is not None:
                            own = slice(s * chan_own, (s + 1) * chan_own)
                            center = center + rest[own, at_block(half)]
                        out = tap_sum(part[:chan_own], center, part[2 * chan_own :], row_len)
                        raw_ref[
                            z, s * chan_own : (s + 1) * chan_own, at_block(2 * t + half)
                        ] = out
                        totals[s] = totals[s] + out
                        squares[s] = squares[s] + out * out
                        leasts[s] = jnp.minimum(leasts[s], out)
                        mosts[s] = jnp.maximum(mosts[s], out)
        pairs = [
            affine(
                jnp.sum(totals[s], axis=1, keepdims=True),
                jnp.sum(squares[s], axis=1, keepdims=True),
                coarse_cells,
                column(rows[s, 0], chan_own, GAIN_AT),
                column(rows[s, 0], chan_own, SHIFT_AT),
            )
            for s in range(y_groups)
        ]
        scale = jnp.concatenate([one[0] for one in pairs], axis=0)
        offset = jnp.concatenate([one[1] for one in pairs], axis=0)
        lanes = lax.broadcasted_iota(jnp.int32, (chan_all, LANES), 1)
        next_ref[...] = jnp.where(lanes == 0, scale, jnp.where(lanes == 1, offset, 0.0))
        peak = jnp.zeros((chan_all, LANES), bf16)
        for extreme in (leasts, mosts):
            value = activated(jnp.concatenate(extreme, axis=0), scale, offset)
            peak = jnp.maximum(peak, jnp.abs(value))
        row = at_lane(tops[:, PEAK_AT : PEAK_AT + 1], 0)
        row = row + at_lane(tops[:, PEAK_AT + 1 : PEAK_AT + 2], 1)
        row = row + at_lane(peak_of(peak_pool), 2)
        row = row + at_lane(peak_of(peak), 3)
        peak_ref[...] = row[:, : peak_ref.shape[1]]

    return kernel


def fourth_kernel(coarse_cells):
    def kernel(
        raw_ref,
        weight_ref,
        param_ref,
        affine_ref,
        next_ref,
        fine_ref,
        out_ref,
        skip_ref,
        cells_ref,
        last_ref,
        narrow_ref,
        done,
    ):
        scale = affine_ref[:, 0:1]
        offset = affine_ref[:, 1:2]
        sends = []
        for z in range(fine_ref.shape[0]):
            act = jnp.stack(
                [activated(fine_ref[z, y], scale, offset) for y in range(fine_ref.shape[1])]
            )
            narrow_ref[:, z] = jnp.transpose(act, (1, 0, 2))
            sends.append(
                pltpu.make_async_copy(narrow_ref.at[:, z], skip_ref.at[0, :, z], done.at[z])
            )
            sends[-1].start()
        planes, chan_all, flat = cells_ref.shape
        chan_own, z_own = out_ref.shape[:2]
        row_len = LANES // 2
        blocks = flat // LANES
        weight = weight_ref[...]
        lower = lax.broadcasted_iota(jnp.int32, (chan_own, LANES), 1) < row_len
        blank = jnp.zeros((chan_own, LANES), f32)
        bound = clip_bound(param_ref, 3)
        scale = next_ref[:, 0:1]
        offset = next_ref[:, 1:2]

        def at_block(block):
            return slice(block * LANES, (block + 1) * LANES)

        def normed(z):
            for j in range(blocks):
                value = activated(raw_ref[z, :, at_block(j)], scale, offset)
                cells_ref[z, :, at_block(j)] = bounded(value, bound)

        def plane(z, sums):
            total, square = sums
            depths = [dz for dz in range(3) if 0 <= z + dz - 1 < planes]
            columns = slice(depths[0] * chan_all, (depths[-1] + 1) * chan_all)
            parts = []
            for t in range(blocks // 2):
                window = jnp.concatenate(
                    [
                        cells_ref[z + dz - 1, :, 2 * t * LANES : 2 * (t + 1) * LANES]
                        for dz in depths
                    ],
                    axis=0,
                )
                taps = jnp.dot(weight[:, columns], window, preferred_element_type=f32)
                parts.extend(taps[:, at_block(half)] for half in range(2))

            def tap(dy, dx, j):
                at = (3 * dy + dx) * chan_own
                return parts[j][at : at + chan_own]

            for j in range(blocks):
                three = []
                for dx in range(3):
                    if j > 0:
                        before = tap(0, dx, j - 1)
                    else:
                        before = jnp.where(lower, blank, turned(tap(0, dx, blocks - 1)))
                    if j + 1 < blocks:
                        after = tap(2, dx, j + 1)
                    else:
                        after = jnp.where(lower, turned(tap(2, dx, 0)), blank)
                    three.append(tap(1, dx, j) + before + after)
                out = tap_sum(*three, row_len)
                last_ref[z, :, at_block(j)] = out
                total = total + out
                square = square + out * out
            return total, square

        sums = (blank, blank)
        normed(0)
        for z in range(planes):
            if z + 1 < planes:
                normed(z + 1)
            sums = plane(z, sums)
        total, square = sums
        scale, offset = affine(
            jnp.sum(total, axis=1, keepdims=True),
            jnp.sum(square, axis=1, keepdims=True),
            coarse_cells,
            lane_of(param_ref, LAST_AT, chan_own),
            lane_of(param_ref, LAST_AT + 1, chan_own),
        )
        at_z = lax.axis_index("sz")
        own = []
        for i in range(z_own):
            cells = activated(last_ref[at_z * z_own + i], scale, offset).astype(f32)
            natural = []
            for p in range(blocks):
                row = (2 * p) % blocks
                first, second = cells[:, at_block(row)], cells[:, at_block(row + 1)]
                if 2 * p < blocks:
                    natural.append(jnp.where(lower, first, turned(second)))
                else:
                    natural.append(jnp.where(lower, turned(first), second))
            own.append(jnp.concatenate(natural, axis=1))
        for c in range(chan_own):
            out_ref[c] = jnp.concatenate([one[c : c + 1] for one in own], axis=0).astype(bf16)
        for send in sends:
            send.wait()

    return kernel


def final_kernel(*refs):
    cells_ref, peak_ref = refs[:2]
    out_ref, top_ref = refs[-2:]
    out_ref[0] = cells_ref[...]
    top = peak_ref[...]
    for ref in refs[2:-2]:
        top = jnp.maximum(top, ref[...])
    top_ref[...] = top


def shape(dims, dtype):
    return jax.ShapeDtypeStruct(dims, dtype)


def near_shape(dims, dtype):
    return pltpu.VMEM(dims, dtype)


def held(value):
    return pltpu.with_memory_space_constraint(value, pltpu.VMEM)


def per_device(
    volume,
    amax_history,
    conv_first,
    conv_second,
    conv_third,
    conv_fourth,
    gain_fine,
    shift_fine,
    gain_coarse,
    shift_coarse,
):
    channels, depth, height, width = volume.shape[1:]
    z_groups = lax.axis_size("sz")
    y_groups = lax.axis_size("sy")
    samples = lax.axis_size("sample")
    fine_cells = float(depth * z_groups * height * y_groups * width)
    coarse_cells = fine_cells / 8
    chan_own = conv_third.shape[1]
    chan_all = conv_fourth.shape[2]
    span = (height // 2) * (width // 2)
    planes = (depth // 2) * z_groups
    flat = span * y_groups
    group = z_groups * y_groups
    load_rows = (depth // 2) * channels + ROWS

    anywhere = pl.BlockSpec(memory_space=pl.ANY)
    near = pl.BlockSpec(memory_space=pltpu.VMEM)
    z_first, z_second = pl.pallas_call(
        slab_kernel,
        in_specs=[anywhere],
        out_specs=(near, near),
        out_shape=(
            near_shape((channels, HALO, height, width), bf16),
            near_shape((channels, HALO, height, width), bf16),
        ),
        scratch_shapes=[pltpu.SemaphoreType.DMA((2 * SLAB_PARTS,))],
        name="slabs",
    )(volume)
    cells, peak = pl.pallas_call(
        prep_kernel,
        out_shape=(
            near_shape((depth, height, channels, width), bf16),
            near_shape((1, LANES), f32),
        ),
        name="prep",
    )(volume, amax_history)
    third_rows = 4 * chan_own
    m1, m2, m3, m4, params, gain_row = pl.pallas_call(
        matrix_kernel,
        out_shape=(
            near_shape((3 * channels, 9 * channels), bf16),
            near_shape((3 * channels, 9 * channels), bf16),
            near_shape((third_rows, 8 * channels), bf16),
            near_shape((9 * chan_own, 3 * chan_all), bf16),
            near_shape((channels, LANES), f32),
            near_shape((1, LANES), f32),
        ),
        name="matrices",
    )(
        held(peak),
        conv_first,
        conv_second,
        conv_third,
        conv_fourth,
        amax_history,
        gain_fine,
        shift_fine,
        gain_coarse,
        shift_coarse,
    )
    pieces = [m3]
    for k in range(1, y_groups):
        pieces.append(lax.ppermute(m3, "sy", [(i, i ^ k) for i in range(y_groups)]))
    pair_first, pair_second = pairings("sz")
    z_first = lax.ppermute(z_first, "sz", pair_first)
    z_second = lax.ppermute(z_second, "sz", pair_second)
    deep_depth = depth + 2 * HALO
    levels = amax_history.shape[0]
    z_first, z_second, first, second = pl.pallas_call(
        deep_kernel,
        out_shape=(
            near_shape((HALO, height, channels, width), bf16),
            near_shape((HALO, height, channels, width), bf16),
            near_shape((deep_depth, HALO, channels, width), bf16),
            near_shape((deep_depth, HALO, channels, width), bf16),
        ),
        name="deep",
    )(*(held(x) for x in (cells, z_first, z_second, params)))
    pair_first, pair_second = pairings("sy")
    y_first = lax.ppermute(first, "sy", pair_first)
    y_second = lax.ppermute(second, "sy", pair_second)
    deep, raw_inner, sums = pl.pallas_call(
        first_inner_kernel,
        out_shape=(
            near_shape((deep_depth, height, channels, width), bf16),
            near_shape((depth + 2, height - 2, channels, width), f32),
            near_shape((2, channels, LANES), f32),
        ),
        name="first_inner",
    )(*(held(x) for x in (cells, z_first, z_second, m1)))
    raw_outer, row = pl.pallas_call(
        first_outer_kernel,
        out_shape=(
            near_shape((depth + 2, 2 * HALO, channels, width), f32),
            near_shape((group, 1, LANES), f32),
        ),
        scratch_shapes=[pltpu.VMEM((2, deep_depth, HALO, channels, width), bf16)],
        name="first_outer",
    )(*(held(x) for x in (deep, y_first, y_second, m1, peak, sums)))
    rows = lax.all_to_all(row, ("sy", "sz"), 0, 0, tiled=True)
    raw_second, load = pl.pallas_call(
        second_kernel(fine_cells),
        out_shape=(
            near_shape((depth, height, channels, width), f32),
            near_shape((load_rows, span), bf16),
        ),
        scratch_shapes=[
            pltpu.VMEM((depth + 2, height + 2, channels, width), bf16),
            pltpu.VMEM((depth // 2, height // 2, channels, width), f32),
        ],
        compiler_params=pltpu.CompilerParams(vmem_limit_bytes=KERNEL_BYTES),
        name="second",
    )(*(held(x) for x in (raw_inner, raw_outer, rows, m2, params, gain_row)))
    loads = [load]
    for k in range(1, z_groups):
        loads.append(lax.ppermute(load, "sz", [(i, i ^ k) for i in range(z_groups)]))
    gathered = lax.all_gather(jnp.concatenate(loads, axis=0), "sy", axis=0)
    raw_third, peaks, fine_affine, next_affine = pl.pallas_call(
        third_kernel(fine_cells, coarse_cells, load_rows, third_rows),
        out_shape=(
            near_shape((planes, chan_all, flat), f32),
            near_shape((1, levels), f32),
            near_shape((channels, LANES), f32),
            near_shape((chan_all, LANES), f32),
        ),
        scratch_shapes=[
            pltpu.VMEM((planes, flat // LANES + 2, 3 * channels, LANES), bf16),
            pltpu.VMEM((3 * chan_all, 8 * channels), bf16),
            pltpu.VMEM((chan_all, 3 * channels), bf16),
        ],
        compiler_params=pltpu.CompilerParams(vmem_limit_bytes=KERNEL_BYTES),
        name="third",
    )(*(held(x) for x in (gathered, params, *pieces)))
    if samples <= 4:
        others = [
            lax.ppermute(peaks, "sample", [(i, (i + k) % samples) for i in range(samples)])
            for k in range(1, samples)
        ]
    else:
        others = [lax.pmax(peaks, "sample")]
    coarse, skip = pl.pallas_call(
        fourth_kernel(coarse_cells),
        out_shape=(
            near_shape((chan_own, depth // 2, flat), bf16),
            shape((1, channels, depth, height, width), bf16),
        ),
        out_specs=(near, anywhere),
        scratch_shapes=[
            pltpu.VMEM((planes, chan_all, flat), bf16),
            pltpu.VMEM((planes, chan_own, flat), f32),
            pltpu.VMEM((channels, depth, height, width), bf16),
            pltpu.SemaphoreType.DMA((depth,)),
        ],
        compiler_params=pltpu.CompilerParams(vmem_limit_bytes=KERNEL_BYTES),
        name="fourth",
    )(*(held(x) for x in (raw_third, m4, params, fine_affine, next_affine, raw_second)))
    coarse, peaks = pl.pallas_call(
        final_kernel,
        out_shape=(
            shape((1, chan_own, depth // 2, flat), bf16),
            shape((1, levels), f32),
        ),
        name="final",
    )(*(held(x) for x in (coarse, peaks, *others)))
    return skip, coarse, peaks.reshape(levels)


def solution(mesh):
    return jax.shard_map(
        per_device,
        mesh=mesh,
        in_specs=(
            P("sample", None, "sz", "sy", None),
            P(),
            P(),
            P(),
            P(None, "sy", None),
            P(None, "sy", None),
            P(),
            P(),
            P(None, "sy"),
            P(None, "sy"),
        ),
        out_specs=(P("sample", None, "sz", "sy", None), P("sample", "sy", "sz", None), P()),
        check_vma=False,
    )
```
